32 devices in a mesh: gx: 8 (over z, y), gy: 4 (over x, core).
Axes of the slice: x: 2, y: 2, z: 4, core: 2. Of those that a mesh axis runs over, the one named last changes fastest.
Arguments:
- modes: float32 [2, 3, 96, 64, 128], P(None, None, 'gx', 'gy'), may hold values from -6 to 6
- moduli: float32 [96, 64, 128], P('gx', 'gy'), may hold values from 0.5 to 2
- pinned: int32 [96, 64, 128], P('gx', 'gy'), may hold values 0 or 1
- spectrum: float32 [3, 2], replicated, may hold values from 0.175 to 5, as said below
Outputs:
- correction: float32 [2, 3, 96, 64, 128], P(None, None, 'gx', 'gy')
The draws below stay inside these ranges and needn't reach their ends.
Inputs may be any that keep to these rules, and one draw needn't show every extreme that they name: spectrum[l] = (lower, upper) with upper from 3.5 to 5 and lower 0.05 to 0.15 times upper.
All inputs are finite; a program needn't handle non-finite values. No bound on the sum of `pinned` on one device may be relied on, other than what follows from the above.
Results may differ from the reference program's by a relative error of at most 0.0003.
Values sent between devices are 32-bit elements; how exact they have to be, the bound alone decides.
A program may use at most 128 MiB of HBM per device.

```python
import math
import jax
import jax.numpy as jnp
import numpy as np
from jax import lax

VECS = 2
DEG = 3
COARSE_DEG = 4
X = 96
Y = 64
Z = 128


def draw_spectrum(key, part):
    upper_key = jax.random.fold_in(key, 11)
    ratio_key = jax.random.fold_in(key, 23)
    top_end = jax.random.uniform(upper_key, (3,), jnp.float32, 3.5, 5.0)
    fraction = jax.random.uniform(ratio_key, (3,), jnp.float32, 0.05, 0.15)
    return jnp.stack([top_end * fraction, top_end], 1)


def place_ends(values, key, low, top_value):
    longest = values.shape.index(max(values.shape))
    spots = []
    for shift in (0, 1):
        where = [jax.random.randint(jax.random.fold_in(key, axis), (), 0, length) for axis, length in enumerate(values.shape)]
        where[longest] = (where[longest] + shift) % values.shape[longest]
        spots.append(tuple(where))
    return values.at[spots[0]].set(low).at[spots[1]].set(top_value)


def steps_of(stream_key, extent, cuts, least, high):
    def one(axis_at, parts):
        heights = jax.random.uniform(jax.random.fold_in(jax.random.fold_in(stream_key, 6), axis_at), (parts,), jnp.float32, least / len(cuts), high / len(cuts))
        return jnp.repeat(jnp.exp(heights), extent[axis_at] // parts).reshape((-1,) + (1,) * (len(extent) - axis_at - 1))

    factor_of = one(*cuts[0])
    for cut in cuts[1:]:
        factor_of = factor_of * one(*cut)
    return factor_of


def scatter_about(own_key, extent, spread, limit, split=(), kind=jnp.bfloat16):
    entries = spread * jax.random.normal(own_key, extent, jnp.float32)
    if split:
        entries = entries * steps_of(own_key, extent, split, -0.22, 0.18)
    return jnp.clip(entries, -limit, limit).astype(kind)


def setup_inputs(seed: int = 0) -> dict:
    streams_of = jax.random.split(jax.random.key(seed), 5)
    modes = scatter_about(streams_of[0], (VECS, 3, X, Y, Z), 1.0, 6.0, ((2, 8), (3, 4)), jnp.float32)
    moduli = jnp.clip(jnp.exp(math.log(2.0) - 1.3862944 * jax.random.uniform(streams_of[1], (X, Y, Z), jnp.float32) ** steps_of(streams_of[1], (X, Y, Z), ((0, 8), (1, 4)), -0.2, 0.2)), 0.5, 2.0)
    pinned = place_ends((jax.random.randint(streams_of[2], (X, Y, Z), 0, 8) < 1).astype(jnp.int32), jax.random.fold_in(streams_of[2], 1), 0, 1)
    spectrum = draw_spectrum(jax.random.fold_in(streams_of[4], 71), 0)
    return {"modes": modes, "moduli": moduli, "pinned": pinned, "spectrum": spectrum}


MU_SHEAR = 1.0
LAMBDA_BULK = 1.5
PROLONG_TABLES = {4: np.array([[1.0, 0.0, 0.0], [0.375, 0.75, -0.125], [0.0, 1.0, 0.0], [-0.125, 0.75, 0.375]], dtype=np.float32), 2: np.array([[1.0, 0.0], [0.5, 0.5]], dtype=np.float32)}
GAUSS_POINTS = [-0.9602898564975363, -0.7966664774136267, -0.5255324099163290, -0.1834346424956498, 0.1834346424956498, 0.5255324099163290, 0.7966664774136267, 0.9602898564975363]
GAUSS_WEIGHTS = [0.1012285362903763, 0.2223810344533745, 0.3137066458778873, 0.3626837833783620, 0.3626837833783620, 0.3137066458778873, 0.2223810344533745, 0.1012285362903763]


def assemble(element, degree):
    coef_table = np.zeros((degree, 2 * degree + 1))
    for residue in range(degree):
        for offset in range(-degree, degree + 1):
            target = residue + offset
            if 0 <= target <= degree:
                coef_table[residue, offset + degree] += element[residue, target]
            if residue == 0 and offset <= 0:
                coef_table[residue, offset + degree] += element[degree, degree + offset]
    return coef_table.astype(np.float32)


def basis_tables(degree):
    nodes = [float(place) / degree for place in range(degree + 1)]
    points = 0.5 * (np.array(GAUSS_POINTS) + 1.0)
    weights = 0.5 * np.array(GAUSS_WEIGHTS)
    values = np.zeros((degree + 1, points.size))
    slopes = np.zeros((degree + 1, points.size))
    for column in range(degree + 1):
        product = np.ones(points.size)
        for other in range(degree + 1):
            if other != column:
                product = product * (points - nodes[other]) / (nodes[column] - nodes[other])
        values[column] = product
        slope_sum = np.zeros(points.size)
        for skipped in range(degree + 1):
            if skipped != column:
                partial_prod = np.ones(points.size) / (nodes[column] - nodes[skipped])
                for other in range(degree + 1):
                    if other != column and other != skipped:
                        partial_prod = partial_prod * (points - nodes[other]) / (nodes[column] - nodes[other])
                slope_sum = slope_sum + partial_prod
        slopes[column] = slope_sum
    mass_el = (values * weights) @ values.T
    stiff_el = (slopes * weights) @ slopes.T
    mixed_el = (slopes * weights) @ values.T
    return [assemble(mass_el, degree), assemble(stiff_el, degree), assemble(mixed_el, degree), assemble(mixed_el.T, degree)]


def coupling():
    return MU_SHEAR + (LAMBDA_BULK + MU_SHEAR) * np.eye(3, dtype=np.float32)


def line_apply(field, along, coef_table, margin):
    degree = coef_table.shape[0]
    length = field.shape[along] - 2 * degree
    residue = (np.arange(length) + degree - margin) % degree
    coef_rows = coef_table[residue]
    shape_out = [1] * field.ndim
    shape_out[along] = length
    summed = None
    for offset in range(2 * degree + 1):
        window = lax.slice_in_dim(field, offset, offset + length, 1, along)
        weighted = window * jnp.asarray(coef_rows[:, offset].reshape(shape_out))
        summed = weighted if summed is None else summed + weighted
    return summed


def z_line(field, coef_table):
    degree = coef_table.shape[0]
    widths = [(0, 0)] * (field.ndim - 1) + [(degree, degree)]
    return line_apply(jnp.pad(field, widths), field.ndim - 1, coef_table, degree)


def elastic(padded, tables, margin):
    mass_tab, stiff_tab, mixed_tab, trans_tab = tables
    weights = coupling()
    z_mass = z_line(padded, mass_tab)
    z_stiff = z_line(padded, stiff_tab)
    along_x = line_apply(line_apply(z_mass, 3, mass_tab, margin), 2, stiff_tab, margin)
    along_y = line_apply(line_apply(z_mass, 3, stiff_tab, margin), 2, mass_tab, margin)
    along_z = line_apply(line_apply(z_stiff, 3, mass_tab, margin), 2, mass_tab, margin)
    outputs = []
    for target in range(3):
        result = weights[target, 0] * along_x[:, target] + weights[target, 1] * along_y[:, target] + weights[target, 2] * along_z[:, target]
        for source in range(3):
            if source != target:
                chosen = [mass_tab, mass_tab, mass_tab]
                chosen[target] = mixed_tab
                chosen[source] = trans_tab
                coupled = z_line(padded[:, source], chosen[2])
                coupled = line_apply(coupled, 2, chosen[1], margin)
                coupled = line_apply(coupled, 1, chosen[0], margin)
                result = result + (LAMBDA_BULK + MU_SHEAR) * coupled
        outputs.append(result)
    return jnp.stack(outputs, 1)


def level_fields(moduli, pinned, stride):
    sampled = moduli[::stride, ::stride, ::stride]
    pinned_f = pinned[::stride, ::stride, ::stride].astype(jnp.float32)
    return sampled * (1.0 - pinned_f), pinned_f


def inverse_diag(scaling, pinned_f, tables):
    mass_tab, stiff_tab = tables[0], tables[1]
    degree = mass_tab.shape[0]
    weights = coupling()
    centers = []
    for along in range(3):
        residue = np.arange(scaling.shape[along]) % degree
        shape_out = [1, 1, 1]
        shape_out[along] = scaling.shape[along]
        centers.append((mass_tab[residue, degree].reshape(shape_out), stiff_tab[residue, degree].reshape(shape_out)))
    rows_out = []
    for target in range(3):
        diagonal = weights[target, 0] * centers[0][1] * centers[1][0] * centers[2][0]
        diagonal = diagonal + weights[target, 1] * centers[0][0] * centers[1][1] * centers[2][0]
        diagonal = diagonal + weights[target, 2] * centers[0][0] * centers[1][0] * centers[2][1]
        rows_out.append(scaling * scaling * jnp.asarray(diagonal) + pinned_f)
    return 1.0 / jnp.stack(rows_out, 0)


def operate(field, scaling, pinned_f, tables, padder):
    degree = tables[0].shape[0]
    padded = padder(scaling * field, degree)
    return scaling * elastic(padded, tables, degree) + pinned_f * field


def chebyshev(source, initial, n_steps, bounds, inverse, apply_op):
    low_end = bounds[0]
    top_end = bounds[1]
    center = 0.5 * (top_end + low_end)
    radius = 0.5 * (top_end - low_end)
    ratio_cs = center / radius
    rho_now = 1.0 / ratio_cs
    residual = source if initial is None else source - apply_op(initial)
    update = inverse * residual / center
    solution = update if initial is None else initial + update
    for sweep_at in range(n_steps - 1):
        residual = residual - apply_op(update)
        rho_next = 1.0 / (2.0 * ratio_cs - rho_now)
        update = rho_next * rho_now * update + (2.0 * rho_next / radius) * inverse * residual
        solution = solution + update
        rho_now = rho_next
    return solution


def alternate(pieces, along):
    stacked = jnp.stack(pieces, along + 1)
    dims_now = list(stacked.shape)
    merged = dims_now[:along] + [dims_now[along] * dims_now[along + 1]] + dims_now[along + 2:]
    return stacked.reshape(merged)


def restrict_line(field, along, table, margin):
    period, tap_count = table.shape
    half_per = period // 2
    owned_n = field.shape[along] - 2 * margin
    if margin < period:
        widths = [(0, 0)] * field.ndim
        widths[along] = (period - margin, 0)
        field = jnp.pad(field, widths)
        start_at = 0
    else:
        start_at = margin - period
    blocks = lax.slice_in_dim(field, start_at, start_at + owned_n + period, 1, along)
    dims_now = list(blocks.shape)
    elems = owned_n // period
    blocks = blocks.reshape(dims_now[:along] + [elems + 1, period] + dims_now[along + 1:])
    tap_sums = []
    for tap_at in range(tap_count):
        running = None
        for residue in range(period):
            if table[residue, tap_at] != 0.0:
                portion = float(table[residue, tap_at]) * lax.index_in_dim(blocks, residue, along + 1, False)
                running = portion if running is None else running + portion
        tap_sums.append(running)
    leading = lax.slice_in_dim(tap_sums[0], 1, elems + 1, 1, along) + lax.slice_in_dim(tap_sums[half_per], 0, elems, 1, along)
    pieces = [leading] + [lax.slice_in_dim(tap_sums[tap_at], 1, elems + 1, 1, along) for tap_at in range(1, half_per)]
    return alternate(pieces, along)


def restrict_all(field, margin, degree):
    table = PROLONG_TABLES[degree]
    coarse = restrict_line(field, 2, table, margin)
    coarse = restrict_line(coarse, 3, table, margin)
    return restrict_line(coarse, 4, table, 0)


def prolong_line(field, along, table, margin):
    period, tap_count = table.shape
    half_per = period // 2
    elems = (field.shape[along] - 2 * margin) // half_per
    columns = [lax.slice_in_dim(field, margin + tap_at, margin + tap_at + half_per * (elems - 1) + 1, half_per, along) for tap_at in range(tap_count)]
    pieces = []
    for residue in range(period):
        running = None
        for tap_at in range(tap_count):
            if table[residue, tap_at] != 0.0:
                portion = float(table[residue, tap_at]) * columns[tap_at]
                running = portion if running is None else running + portion
        pieces.append(running)
    return alternate(pieces, along)


def prolong_all(field, degree):
    table = PROLONG_TABLES[degree]
    fine = prolong_line(field, 2, table, 1)
    fine = prolong_line(fine, 3, table, 1)
    fine = jnp.pad(fine, [(0, 0)] * 4 + [(1, 1)])
    return prolong_line(fine, 4, table, 1)


def zero_pad(field, width):
    widths = [(0, 0)] * field.ndim
    widths[-3] = (width, width)
    widths[-2] = (width, width)
    return jnp.pad(field, widths)


def reference(modes, moduli, pinned, spectrum):
    degrees = [4, 2, 1]
    tables = [basis_tables(degree) for degree in degrees]
    fields = [level_fields(moduli, pinned, stride) for stride in (1, 2, 4)]

    def v_cycle(level_at, source):
        scaling, pinned_f = fields[level_at]
        inverse = inverse_diag(scaling, pinned_f, tables[level_at])[None]

        def apply_op(field):
            return operate(field, scaling, pinned_f, tables[level_at], zero_pad)

        if level_at == 2:
            return chebyshev(source, None, COARSE_DEG, spectrum[2], inverse, apply_op)
        degree = degrees[level_at]
        solution = chebyshev(source, None, DEG, spectrum[level_at], inverse, apply_op)
        residual = (1.0 - pinned_f) * source - scaling * elastic(zero_pad(scaling * solution, degree), tables[level_at], degree)
        coarse_fixed = fields[level_at + 1][1]
        coarse_src = (1.0 - coarse_fixed) * restrict_all(zero_pad(residual, degree - 1), degree - 1, degree)
        lifted = v_cycle(level_at + 1, coarse_src)
        solution = solution + (1.0 - pinned_f) * prolong_all(zero_pad(lifted, 1), degree)
        return chebyshev(source, solution, DEG, spectrum[level_at], inverse, apply_op)

    return v_cycle(0, modes)
```

```python
import functools

import jax
import jax.numpy as jnp
import numpy as np
from jax import lax
from jax.experimental import pallas as pl
from jax.experimental.pallas import tpu as pltpu
from jax.sharding import PartitionSpec as P

DEG = 3
COARSE_DEG = 4
DEGREES = (4, 2, 1)
MU_SHEAR = 1.0
LAMBDA_BULK = 1.5
PROLONG_TABLES = {
    4: np.array(
        [[1.0, 0.0, 0.0], [0.375, 0.75, -0.125], [0.0, 1.0, 0.0], [-0.125, 0.75, 0.375]]
    ),
    2: np.array([[1.0, 0.0], [0.5, 0.5]]),
}
DIRS = ((-1, 0), (1, 0), (0, -1), (0, 1), (-1, -1), (-1, 1), (1, -1), (1, 1))
F32 = jnp.float32
BF16 = jnp.bfloat16
M_, K_, G_, T_ = range(4)


def element_matrices(degree):
    nodes = [float(place) / degree for place in range(degree + 1)]
    gauss_x, gauss_w = np.polynomial.legendre.leggauss(8)
    points = 0.5 * (gauss_x + 1.0)
    weights = 0.5 * gauss_w
    values = np.zeros((degree + 1, points.size))
    slopes = np.zeros((degree + 1, points.size))
    for column in range(degree + 1):
        product = np.ones(points.size)
        for other in range(degree + 1):
            if other != column:
                product = product * (points - nodes[other]) / (nodes[column] - nodes[other])
        values[column] = product
        for skipped in range(degree + 1):
            if skipped != column:
                part = np.ones(points.size) / (nodes[column] - nodes[skipped])
                for other in range(degree + 1):
                    if other != column and other != skipped:
                        part = part * (points - nodes[other]) / (nodes[column] - nodes[other])
                slopes[column] += part
    mass = (values * weights) @ values.T
    stiff = (slopes * weights) @ slopes.T
    mixed = (slopes * weights) @ values.T
    return [mass, stiff, mixed, mixed.T]


def assembled(element, count, ghost):
    p = element.shape[0] - 1
    out = np.zeros((count + 1, count + 1))
    for e in range(count // p):
        out[e * p : e * p + p + 1, e * p : e * p + p + 1] += element
    if ghost:
        out[0, 0] += element[p, p]
    return out


def up(n, m):
    return -(-n // m) * m


def bf16_parts(mat, count):
    rest = np.asarray(mat, np.float64)
    parts = []
    for _ in range(count):
        part = rest.astype(np.float32).astype(BF16)
        parts.append(part)
        rest = rest - part.astype(np.float64)
    return parts


def exact_bf16(mat):
    out = np.asarray(mat, np.float32).astype(BF16)
    assert np.array_equal(out.astype(np.float64), mat)
    return out


class Level:
    def __init__(self, degree, nx, ny, nz, vecs):
        self.p, self.nx, self.ny, self.nz, self.vecs = degree, nx, ny, nz, vecs
        self.ys = up(nx + 1, 8)
        self.run = up(ny, 8)
        self.base = 2 * self.ys + self.run
        self.rows = up(self.base + nx * self.run, 16)
        self.nb = self.base + self.run
        assert self.nb % 16 == 0
        self.lanes = up(vecs * nz, 128)
        tight = up(self.rows, 16)
        if 3 * tight <= 256:
            self.kp, self.kb = tight, 256
        else:
            self.kp = up(self.rows, 128)
            self.kb = 3 * self.kp
        self.packed = self.kb == 256
        self.seg = 256 if self.packed else self.kp
        self.where = {(x, y): self.row(x, y) for x in range(nx + 1) for y in range(ny + 1)}

    def row(self, x, y):
        if y == 0:
            return x
        if y == self.ny:
            return self.ys + x
        if x == self.nx:
            return 2 * self.ys + y
        return self.base + self.run * x + y

    def factors(self):
        out = []
        for axis, n in ((0, self.nx), (1, self.ny)):
            expand = np.zeros((self.rows, 32))
            spread = np.zeros((128, self.seg))
            for at, row in self.where.items():
                expand[row, at[axis]] = 1
                for copy in range(3 if self.packed else 1):
                    for part in range(3):
                        spread[32 * part + at[axis], copy * self.kp + row] = 1
            table = np.zeros((2, 32, 512), BF16)
            for ghost in range(2):
                for i, element in enumerate(element_matrices(self.p)):
                    parts = bf16_parts(assembled(element, n, ghost), 3)
                    for part, mat in enumerate(parts):
                        at = 128 * i + 32 * part
                        table[ghost, : n + 1, at : at + n + 1] = mat
            out.append((exact_bf16(expand), table, exact_bf16(spread)))
        return out

    def lines(self):
        p, n = self.p, self.nz
        mats = []
        for e in element_matrices(p):
            full = assembled(e, n, True)[:n, :n].T
            if n % 128:
                lifted = np.zeros((self.lanes, self.lanes))
                size = self.vecs * n
                lifted[:size, :size] = np.kron(np.eye(self.vecs), full)
                full = lifted
            mats.append(np.stack(bf16_parts(full, 2)))
        return np.stack(mats)

    def diagonal(self):
        def center(which, count):
            p = self.p
            e = element_matrices(p)[which]
            line = np.array([e[a, a] + (e[p, p] if a == 0 else 0.0) for a in range(p)])
            return line[np.arange(count) % p]

        rows = np.zeros((self.rows, 128), np.float32)
        m_x, m_y, m_z = [center(0, n) for n in (self.nx + self.p, self.ny + self.p, self.nz)]
        k_x, k_y, k_z = [center(1, n) for n in (self.nx + self.p, self.ny + self.p, self.nz)]
        for c in range(3):
            coef = [MU_SHEAR + (LAMBDA_BULK + MU_SHEAR) * (c == e) for e in range(3)]
            for (x, y), row in self.where.items():
                rows[row, c] = coef[0] * k_x[x] * m_y[y] + coef[1] * m_x[x] * k_y[y]
                rows[row, 3 + c] = coef[2] * m_x[x] * m_y[y]
        lanes = np.zeros((8, self.lanes), np.float32)
        lanes[0, : self.vecs * self.nz] = np.tile(m_z, self.vecs)
        lanes[1, : self.vecs * self.nz] = np.tile(k_z, self.vecs)
        return rows, lanes

    def sample(self, top):
        step = top.p // self.p
        sel_x = np.zeros((self.rows, top.rows))
        for (x, y), row in self.where.items():
            sel_x[row, top.where[x * step, y * step]] = 1
        sel_z = np.zeros((top.lanes, self.lanes))
        for v in range(self.vecs):
            for z in range(self.nz):
                sel_z[v * top.nz + z * step, v * self.nz + z] = 1
        return exact_bf16(sel_x), exact_bf16(sel_z)


def interpolation(table, count):
    q = table.shape[0]
    half = q // 2
    out = np.zeros((count + 1, count // 2 + 1))
    for i in range(count + 1):
        for t in range(half + 1):
            j = half * (i // q) + t
            if table[i % q, t] != 0.0:
                out[i, j] += table[i % q, t]
    return out


def transfer(fine, coarse):
    table = PROLONG_TABLES[fine.p]
    px, py = interpolation(table, fine.nx), interpolation(table, fine.ny)
    pz = interpolation(table, fine.nz)[: fine.nz, : coarse.nz]
    plane = np.zeros((fine.rows, coarse.rows))
    for (x, y), row in fine.where.items():
        for (cx, cy), col in coarse.where.items():
            plane[row, col] = px[x, cx] * py[y, cy]
    line = np.zeros((coarse.lanes, fine.lanes))
    size = (fine.vecs * coarse.nz, fine.vecs * fine.nz)
    line[: size[0], : size[1]] = np.kron(np.eye(fine.vecs), pz.T)
    down = (np.tile(plane.T, (1, 2)), np.tile(line.T, (2, 1)))
    upward = (np.tile(plane, (1, 2)), np.tile(line, (2, 1)))
    return [exact_bf16(m) for m in down + upward]


def halves(value):
    hi = value.astype(BF16)
    return hi, (value - hi.astype(F32)).astype(BF16)


def mm(a, b):
    return lax.dot_general(a, b, (((1,), (0,)), ((), ())), preferred_element_type=F32)


def wide3(value):
    hi, lo = halves(value)
    return jnp.concatenate([hi, lo, hi], axis=1)


def wide2(value):
    hi, lo = halves(value)
    return jnp.concatenate([hi, lo], axis=1)


def tall2(value):
    hi, lo = halves(value)
    return jnp.concatenate([hi, lo], axis=0)


def kernel(levels, names, *refs):
    R = dict(zip(names, refs))
    gx_n, gy_n = lax.axis_size("gx"), lax.axis_size("gy")
    me_x, me_y = lax.axis_index("gx"), lax.axis_index("gy")

    def reach(dx, dy):
        ok = None
        for d, me, n in ((dx, me_x, gx_n), (dy, me_y, gy_n)):
            if d:
                here = me + d < n if d > 0 else me + d >= 0
                ok = here if ok is None else jnp.logical_and(ok, here)
        return ok

    def device(dx, dy):
        return (jnp.clip(me_x + dx, 0, gx_n - 1), jnp.clip(me_y + dy, 0, gy_n - 1))

    top = levels[0]
    vecs, nz = top.vecs, top.nz
    body_rows = pl.ds(top.base, top.nx * top.run)

    moves = []

    def load(src, dst):
        moves.append(pltpu.make_async_copy(src, dst, R["lsem"].at[len(moves)]))
        moves[-1].start()

    load(R["moduli_in"], R["moduli"])
    load(R["pinned_in"], R["pinned"])
    for v in range(vecs):
        load(R["modes"].at[v], R["r0"].at[:, body_rows, pl.ds(v * nz, nz)])
    first_moves = len(moves)
    for l, lev in enumerate(levels):
        if lev.nz % 128 == 0:
            R[f"z{l}"][...] = jnp.zeros_like(R[f"z{l}"])
        load(R[f"tx{l}_in"].at[jnp.where(me_x == 0, 1, 0)], R[f"tx{l}"])
        load(R[f"ty{l}_in"].at[jnp.where(me_y == 0, 1, 0)], R[f"ty{l}"])
    for name in names:
        if name.endswith("_in") and name[:2] not in ("mo", "pi", "tx", "ty"):
            if name[0] == "z":
                lev = levels[int(name[1])]
                src, dst = R[name], R[name[:-3]]
                size = lev.nz if lev.nz % 128 == 0 else lev.lanes
                for s, half in enumerate((0, 0, 1)):
                    for at in range(0, lev.lanes, size):
                        load(
                            src.at[:, half],
                            dst.at[:, pl.ds(s * lev.lanes + at, size), pl.ds(at, size)],
                        )
            else:
                load(R[name], R[name[:-3]])

    chebyshev_table(R["spectrum"], R["coef"])
    for l, lev in enumerate(levels):
        for n in "xyd":
            R[f"recv{n}{l}"][...] = jnp.zeros_like(R[f"recv{n}{l}"])
            R[f"send{n}{l}"][...] = jnp.zeros_like(R[f"send{n}{l}"])
        R[f"u{l}"][...] = jnp.zeros_like(R[f"u{l}"])
        R[f"pend{l}"][...] = jnp.zeros_like(R[f"pend{l}"])
    for n in "xyd":
        R[f"got{n}"][...] = jnp.zeros_like(R[f"got{n}"])
    for c in range(3):
        R["r0"][c, 0 : top.base] = jnp.zeros((top.base, top.lanes), F32)

    barrier = pltpu.get_barrier_semaphore()
    for dx, dy in DIRS:

        @pl.when(reach(dx, dy))
        def _():
            pl.semaphore_signal(
                barrier, inc=1, device_id=device(dx, dy), device_id_type=pl.DeviceIdType.MESH
            )

    for one in moves[:first_moves]:
        one.wait()
    scale = R["moduli"][...] * (1.0 - R["pinned"][...].astype(F32))
    s0 = R["s0"]
    s0[0 : top.base] = jnp.zeros((top.base, top.lanes), F32)
    for v in range(vecs):
        s0[body_rows, v * nz : (v + 1) * nz] = scale
    put = R["put"]
    put[...] = jnp.zeros_like(put)
    for c in range(3):
        for x in range(top.nx):
            at = top.base + x * top.run
            put[c, x : x + 1, :] = R["r0"][c, at : at + 1, :]
    for x in range(top.nx):
        at = top.base + x * top.run
        put[3, x : x + 1, :] = s0[at : at + 1, :]
    for c in range(4):
        R["putd"][c : c + 1, :] = put[c, 0:1, :]
    R["putd"][4:8, :] = jnp.zeros((4, top.lanes), F32)
    edge = pl.ds(top.base, top.run)

    def first_copies():
        plan = (
            (-1, 0, R["r0"].at[:, edge, :], R["gotx"].at[pl.ds(0, 3)]),
            (-1, 0, s0.at[edge, :], R["gotx"].at[3]),
            (0, -1, put, R["goty"]),
            (-1, -1, R["putd"], R["gotd"]),
        )
        for i, (dx, dy, src, dst) in enumerate(plan):
            yield dx, dy, pltpu.make_async_remote_copy(
                src_ref=src,
                dst_ref=dst,
                send_sem=R["fsend"].at[i],
                recv_sem=R["frecv"].at[i],
                device_id=device(dx, dy),
                device_id_type=pl.DeviceIdType.MESH,
            )

    around = [
        1 + (me > 0).astype(jnp.int32) + (me < n - 1).astype(jnp.int32)
        for me, n in ((me_x, gx_n), (me_y, gy_n))
    ]
    pl.semaphore_wait(barrier, around[0] * around[1] - 1)
    for dx, dy, copy in first_copies():
        pl.when(reach(dx, dy))(copy.start)
    for one in moves[first_moves:]:
        one.wait()

    def copies(l, slot):
        for i, (dx, dy) in enumerate(DIRS):
            kind, at = ("d", i - 4) if dx and dy else ("x", i) if dx else ("y", i - 2)
            yield dx, dy, pltpu.make_async_remote_copy(
                src_ref=R[f"send{kind}{l}"].at[at],
                dst_ref=R[f"recv{kind}{l}"].at[slot, at],
                send_sem=R[f"ssem{l}"].at[i],
                recv_sem=R[f"rsem{l}"].at[slot, i],
                device_id=device(dx, dy),
                device_id_type=pl.DeviceIdType.MESH,
            )

    def send(l, slot, part):
        lev = levels[l]
        ys, run, nx = lev.ys, lev.run, lev.nx
        sx, sy, sd = (R[f"send{n}{l}"] for n in "xyd")
        tile = 3 * run
        for c in range(3):
            sx[0, c * run : (c + 1) * run] = part[c][lev.base : lev.base + run]
            sx[1, c * run : (c + 1) * run] = part[c][2 * ys : 2 * ys + run]
            low, high = part[c][0:ys], part[c][ys : 2 * ys]
            sx[0, tile + c : tile + c + 1] = low[0:1]
            sx[0, tile + 3 + c : tile + 4 + c] = high[0:1]
            sx[1, tile + c : tile + c + 1] = low[nx : nx + 1]
            sx[1, tile + 3 + c : tile + 4 + c] = high[nx : nx + 1]
            sy[0, c * ys : (c + 1) * ys] = low
            sy[1, c * ys : (c + 1) * ys] = high
            sd[0, 3 + c : 4 + c] = low[0:1]
            sd[1, c : c + 1] = high[0:1]
            sd[2, 3 + c : 4 + c] = low[nx : nx + 1]
            sd[3, c : c + 1] = high[nx : nx + 1]
        for dx, dy, copy in copies(l, slot):
            pl.when(reach(dx, dy))(copy.start)

    def arrive(l, slot):
        lev = levels[l]
        ys, run, nx = lev.ys, lev.run, lev.nx
        for dx, dy, copy in copies(l, slot):
            pl.when(reach(-dx, -dy))(copy.wait_recv)
            pl.when(reach(dx, dy))(copy.wait_send)
        rx, ry, rd = (R[f"recv{n}{l}"] for n in "xyd")
        tile = pl.ds(3 * run, 8)
        left = rx[slot, 1, tile, :] + rd[slot, 2] + rd[slot, 3]
        right = rx[slot, 0, tile, :] + rd[slot, 0] + rd[slot, 1]
        at = lax.broadcasted_iota(jnp.int32, (ys, lev.lanes), 0)
        out = []
        for c in range(3):
            pieces = []
            for k, src in ((0, 1), (1, 0)):
                val = ry[slot, src, c * ys : (c + 1) * ys, :]
                val = val + jnp.where(at == 0, left[3 * k + c : 3 * k + c + 1], 0.0)
                val = val + jnp.where(at == nx, right[3 * k + c : 3 * k + c + 1], 0.0)
                pieces.append(val)
            pieces.append(rx[slot, 0, c * run : (c + 1) * run, :])
            pieces.append(rx[slot, 1, c * run : (c + 1) * run, :])
            out.append(jnp.concatenate(pieces, axis=0))
        return out

    def set_u(l, c, a, b, value):
        lev = levels[l]
        hi, lo = halves(value)
        at = c * lev.kb + a
        R[f"u{l}"][at : at + b - a] = hi
        R[f"u{l}"][at + lev.kp : at + lev.kp + b - a] = hi
        R[f"u{l}"][at + 2 * lev.kp : at + 2 * lev.kp + b - a] = lo

    def span(l, blk):
        lev = levels[l]
        return (0, lev.nb) if blk == "b" else (lev.nb, lev.rows)

    def prepare(l, a, b):
        s = R[f"s{l}"][a:b]
        f = jnp.where(s == 0.0, 1.0, 0.0)
        R[f"f{l}"][a:b] = f
        square = s * s
        m_z, k_z = R[f"kl{l}"][0:1, :], R[f"kl{l}"][1:2, :]
        for c in range(3):
            kd = R[f"kr{l}"][a:b, c : c + 1] * m_z + R[f"kr{l}"][a:b, 3 + c : 4 + c] * k_z
            R[f"dinv{l}"][c, a:b] = 1.0 / (square * kd + f)

    def begin(l, a, b, source):
        scale = R["coef"][l, 12]
        s = R[f"s{l}"][a:b]
        for c in range(3):
            first = scale * (R[f"dinv{l}"][c, a:b] * source[c])
            R[f"r{l}"][c, a:b] = source[c]
            R[f"d{l}"][c, a:b] = first
            R[f"x{l}"][c, a:b] = first
            set_u(l, c, a, b, s * first)

    def local_sums(l, blk):
        lev = levels[l]
        a, b = span(l, blk)
        n, kb = b - a, lev.kb
        u, w1, w2 = R[f"u{l}"], R[f"w1{blk}{l}"], R[f"w2{blk}{l}"]
        both = mm(w1[...], u[0 : 2 * kb])
        last = mm(w2[...], u[2 * kb : 3 * kb])
        mass = w2[3 * n : 4 * n]
        plain = [mm(mass, u[0:kb]), mm(mass, u[kb : 2 * kb]), last[3 * n : 4 * n]]
        stretch = (2.0 * MU_SHEAR + LAMBDA_BULK) / MU_SHEAR
        plain[2] = stretch * plain[2]

        def along(which, parts):
            return mm(jnp.concatenate([wide3(v) for v in parts], axis=0), R[f"z{l}"][which])

        zm = along(M_, [both[0:n], both[n : 2 * n], last[2 * n : 3 * n]])
        zk = along(K_, plain)
        zt = along(T_, [last[0:n], last[n : 2 * n]])
        zg = along(G_, [both[2 * n : 3 * n]])
        return [
            zm[0:n] + zk[0:n] + zt[0:n],
            zm[n : 2 * n] + zk[n : 2 * n] + zt[n : 2 * n],
            zm[2 * n : 3 * n] + zk[2 * n : 3 * n] + zg,
        ]

    def advance(l, k, a, b, sums):
        c1, c2 = R["coef"][l, 2 * k], R["coef"][l, 2 * k + 1]
        s, f = R[f"s{l}"][a:b], R[f"f{l}"][a:b]
        for c in range(3):
            d = R[f"d{l}"][c, a:b]
            res = R[f"r{l}"][c, a:b] - (s * sums[c] + f * d)
            new = c1 * d + c2 * (R[f"dinv{l}"][c, a:b] * res)
            R[f"r{l}"][c, a:b] = res
            R[f"d{l}"][c, a:b] = new
            R[f"x{l}"][c, a:b] += new
            set_u(l, c, a, b, s * new)

    def smooth(l, k, slot, beside=None):
        lev = levels[l]
        own, pend = R[f"own{l}"], R[f"pend{l}"]
        part = local_sums(l, "b")
        for c in range(3):
            part[c] = part[c] + pend[c]
            own[c] = part[c]
            pend[c] = jnp.zeros_like(pend[c])
        send(l, slot, part)
        inner = local_sums(l, "i")
        advance(l, k, lev.nb, lev.rows, inner)
        if beside is not None:
            beside()
        got = arrive(l, slot)
        advance(l, k, 0, lev.nb, [own[c] + got[c] for c in range(3)])

    def restrict(l):
        lev = levels[l]
        masked = []
        for blk in "bi":
            a, b = span(l, blk)
            sums = local_sums(l, blk)
            s, f = R[f"s{l}"][a:b], R[f"f{l}"][a:b]
            free = 1.0 - f
            if blk == "b":
                row = lax.broadcasted_iota(jnp.int32, (b - a, lev.lanes), 0)
                mine = jnp.logical_or(row < lev.nx, row >= lev.base)
                free = jnp.where(mine, free, 0.0)
            piece = []
            for c in range(3):
                r, d = R[f"r{l}"][c, a:b], R[f"d{l}"][c, a:b]
                piece.append(free * r - s * sums[c])
                if blk == "b":
                    R[f"pend{l}"][c] = sums[c]
                    R[f"r{l}"][c, a:b] = r - f * d
                else:
                    R[f"r{l}"][c, a:b] = r - (s * sums[c] + f * d)
            masked.append(piece)
        flat = []
        for c in range(3):
            field = jnp.concatenate([masked[0][c], masked[1][c]], axis=0)
            flat.append(wide2(mm(R[f"dp{l}"][...], tall2(field))))
        down = mm(jnp.concatenate(flat, axis=0), R[f"dz{l}"][...])
        n = levels[l + 1].rows
        return [down[c * n : (c + 1) * n] for c in range(3)]

    def descend(l, slot, sums):
        lev = levels[l]
        own = R[f"own{l}"]
        for c in range(3):
            own[c] = sums[c][0 : lev.nb]
        send(l, slot, [sums[c][0 : lev.nb] for c in range(3)])
        free = 1.0 - R[f"f{l}"][lev.nb : lev.rows]
        begin(l, lev.nb, lev.rows, [free * sums[c][lev.nb : lev.rows] for c in range(3)])
        got = arrive(l, slot)
        free = 1.0 - R[f"f{l}"][0 : lev.nb]
        begin(l, 0, lev.nb, [free * (own[c] + got[c]) for c in range(3)])

    def ascend(l):
        lev, n = levels[l], levels[l + 1].rows
        field = jnp.concatenate([wide2(R[f"x{l + 1}"][c]) for c in range(3)], axis=0)
        fine = mm(field, R[f"uz{l}"][...])
        free, s = 1.0 - R[f"f{l}"][...], R[f"s{l}"][...]
        for c in range(3):
            step = free * mm(R[f"up{l}"][...], tall2(fine[c * n : (c + 1) * n]))
            R[f"d{l}"][c] = step
            R[f"x{l}"][c] += step
            set_u(l, c, 0, lev.rows, s * step)

    def build(l):
        lev = levels[l]
        lines = []
        for axis in "xy":
            tall = mm(R[f"e{axis}{l}"][...], R[f"t{axis}{l}"][...])
            lines.append(
                [
                    mm(tall[:, 128 * i : 128 * (i + 1)].astype(BF16), R[f"c{axis}{l}"][...])
                    for i in range(4)
                ]
            )
        X, Y = lines
        cc = LAMBDA_BULK + MU_SHEAR
        big = MU_SHEAR + cc
        kxmy, mxky = X[K_] * Y[M_], X[M_] * Y[K_]
        first = (
            (0, 0, big * kxmy + MU_SHEAR * mxky),
            (0, 1, cc * (X[G_] * Y[T_])),
            (1, 0, cc * (X[T_] * Y[G_])),
            (1, 1, MU_SHEAR * kxmy + big * mxky),
            (2, 0, cc * (X[T_] * Y[M_])),
            (2, 1, cc * (X[M_] * Y[T_])),
        )
        second = (
            cc * (X[G_] * Y[M_]),
            cc * (X[M_] * Y[G_]),
            MU_SHEAR * (kxmy + mxky),
            X[M_] * Y[M_],
        )
        lane = lax.broadcasted_iota(jnp.int32, (lev.rows, lev.seg), 1)
        middle = jnp.logical_and(lane >= lev.kp, lane < 2 * lev.kp)

        def store(kind, group, at, value):
            hi, lo = halves(value)
            for blk in "bi":
                a, b = span(l, blk)
                ref, row = R[f"{kind}{blk}{l}"], group * (b - a)
                row = slice(row, row + b - a)
                if lev.packed:
                    mixed = jnp.where(middle, lo.astype(F32), hi.astype(F32)).astype(BF16)
                    ref[row, at : at + 256] = mixed[a:b]
                else:
                    for s, half in enumerate((hi, lo, hi)):
                        start = at + s * lev.kp
                        ref[row, start : start + lev.kp] = half[a:b]

        for group, side, value in first:
            store("w1", group, side * lev.kb, value)
        for group, value in enumerate(second):
            store("w2", group, 0, value)

    build(0)

    def clear_spare(a, b):
        lead = lax.broadcasted_iota(jnp.int32, (b - a, top.lanes), 0) % top.run == 0
        s0[a:b] = jnp.where(lead, 0.0, s0[a:b])

    clear_spare(top.nb, top.rows)
    prepare(0, top.nb, top.rows)
    begin(0, top.nb, top.rows, [R["r0"][c, top.nb : top.rows] for c in range(3)])
    for dx, dy, copy in first_copies():
        pl.when(reach(dx, dy))(copy.wait_send)
        pl.when(reach(-dx, -dy))(copy.wait_recv)
    clear_spare(top.base, top.nb)
    ys, run, nx = top.ys, top.run, top.nx
    at = lax.broadcasted_iota(jnp.int32, (ys, top.lanes), 0)
    for c in range(4):
        dst = s0 if c == 3 else R["r0"].at[c]
        low = jnp.where(at == nx, R["gotx"][c, 0:1, :], put[c])
        high = jnp.where(at == nx, R["gotd"][c : c + 1, :], R["goty"][c])
        dst[0:ys] = low
        dst[ys : 2 * ys] = high
        side = R["gotx"][c]
        if c == 3:
            row = lax.broadcasted_iota(jnp.int32, (run, top.lanes), 0)
            side = jnp.where(row == 0, 0.0, side)
        dst[2 * ys : 2 * ys + run] = side
    prepare(0, 0, top.nb)
    begin(0, 0, top.nb, [R["r0"][c, 0 : top.nb] for c in range(3)])

    def coarse_setup():
        whole = s0[...]
        parts = []
        rest = whole
        for _ in range(3):
            part = rest.astype(BF16)
            parts.append(part)
            rest = rest - part.astype(F32)
        for l in range(1, len(levels)):
            sel_x, sel_z = R[f"sx{l}"][...], R[f"sz{l}"][...]
            picked = [mm(sel_x, part).astype(BF16) for part in parts]
            R[f"s{l}"][...] = sum(mm(part, sel_z) for part in picked)
            prepare(l, 0, levels[l].rows)
            build(l)

    def pre(k, _):
        smooth(0, k, k % 2, lambda: pl.when(k == 0)(coarse_setup))
        return 0

    def cycle(l):
        last = l == len(levels) - 1
        skip = 0 if l == 0 else 1

        def body(k, _):
            smooth(l, k, (k + skip) % 2)
            return 0

        def tail(k, _):
            smooth(l, k, (k + skip + 1) % 2)
            return 0

        if last:
            lax.fori_loop(0, COARSE_DEG - 1, body, 0)
            return
        lax.fori_loop(0, DEG - 1, pre if l == 0 else body, 0)
        descend(l + 1, 0, restrict(l))
        cycle(l + 1)
        ascend(l)
        lax.fori_loop(DEG, 2 * DEG, tail, 0)

    cycle(0)
    for c in range(3):
        for x in range(nx):
            row = top.base + x * run
            R["x0"][c, row : row + 1, :] = R["x0"][c, x : x + 1, :]
    backs = [
        pltpu.make_async_copy(
            R["x0"].at[:, body_rows, pl.ds(v * nz, nz)], R["out"].at[v], R["lsem"].at[v]
        )
        for v in range(vecs)
    ]
    for one in backs:
        one.start()
    for one in backs:
        one.wait()


def chebyshev_table(spectrum, coef):
    for l in range(3):
        low, top = spectrum[l, 0], spectrum[l, 1]
        center = 0.5 * (top + low)
        radius = 0.5 * (top - low)
        ratio = center / radius
        rho = 1.0 / ratio
        steps = []
        for _ in range(COARSE_DEG - 1):
            rho_next = 1.0 / (2.0 * ratio - rho)
            steps.append((rho_next * rho, 2.0 * rho_next / radius))
            rho = rho_next
        smooth = steps[: DEG - 1]
        flat = [(0.0, 0.0), (0.0, 1.0 / center)]
        picked = steps if l == 2 else smooth + flat + smooth
        for k, two in enumerate(picked):
            coef[l, 2 * k] = jnp.asarray(two[0], F32)
            coef[l, 2 * k + 1] = jnp.asarray(two[1], F32)
        coef[l, 12] = 1.0 / center


def local(modes, moduli, pinned, spectrum):
    vecs, _, nx, ny, nz = modes.shape
    levels = []
    names, args = [], []

    def add(name, value):
        names.append(name)
        args.append(value)

    for degree in DEGREES:
        step = DEGREES[0] // degree
        levels.append(Level(degree, nx // step, ny // step, nz // step, vecs))
    top = levels[0]
    assert ny == top.run and nz % 128 == 0
    add("spectrum", spectrum)
    add("modes", modes.reshape(vecs, 3, nx * ny, nz))
    add("moduli_in", moduli.reshape(nx * ny, nz))
    add("pinned_in", pinned.reshape(nx * ny, nz))
    for l, lev in enumerate(levels):
        for axis, mats in zip("xy", lev.factors()):
            for key, mat in zip("etc", mats):
                add(f"{key}{axis}{l}_in", jnp.asarray(mat))
        add(f"z{l}_in", jnp.asarray(lev.lines()))
        for key, mat in zip(("kr", "kl"), lev.diagonal()):
            add(f"{key}{l}_in", jnp.asarray(mat))
        if l + 1 < len(levels):
            for key, mat in zip(("dp", "dz", "up", "uz"), transfer(lev, levels[l + 1])):
                add(f"{key}{l}_in", jnp.asarray(mat))
        if l:
            for key, mat in zip(("sx", "sz"), lev.sample(top)):
                add(f"{key}{l}_in", jnp.asarray(mat))

    specs = [
        pl.BlockSpec(memory_space=pltpu.SMEM if n == "spectrum" else pl.ANY) for n in names
    ]
    scratch = []
    all_names = names + ["out"]

    def temp(name, what):
        all_names.append(name)
        scratch.append(what)

    temp("coef", pltpu.SMEM((3, 13), F32))
    temp("lsem", pltpu.SemaphoreType.DMA((len(names) + 24,)))
    for name, value in zip(names, args):
        if name.endswith("_in"):
            shape = value.shape
            if name[0] == "z":
                lanes = levels[int(name[1])].lanes
                shape = (4, 3 * lanes, lanes)
            elif name[0] == "t":
                shape = shape[1:]
            temp(name[:-3], pltpu.VMEM(shape, value.dtype))
    for l, lev in enumerate(levels):
        field = (3, lev.rows, lev.lanes)
        for n in ("s", "f"):
            temp(f"{n}{l}", pltpu.VMEM(field[1:], F32))
        for n in ("r", "d", "x", "dinv"):
            temp(f"{n}{l}", pltpu.VMEM(field, F32))
        for n in ("own", "pend"):
            temp(f"{n}{l}", pltpu.VMEM((3, lev.nb, lev.lanes), F32))
        temp(f"u{l}", pltpu.VMEM((3 * lev.kb, lev.lanes), BF16))
        for blk, n in (("b", lev.nb), ("i", lev.rows - lev.nb)):
            temp(f"w1{blk}{l}", pltpu.VMEM((3 * n, 2 * lev.kb), BF16))
            temp(f"w2{blk}{l}", pltpu.VMEM((4 * n, lev.kb), BF16))
        for n, shape in (
            ("x", (2, 3 * lev.run + 8, lev.lanes)),
            ("y", (2, 3 * lev.ys, lev.lanes)),
            ("d", (4, 8, lev.lanes)),
        ):
            temp(f"send{n}{l}", pltpu.VMEM(shape, F32))
            temp(f"recv{n}{l}", pltpu.VMEM((2,) + shape, F32))
        temp(f"ssem{l}", pltpu.SemaphoreType.DMA((len(DIRS),)))
        temp(f"rsem{l}", pltpu.SemaphoreType.DMA((2, len(DIRS))))
    temp("put", pltpu.VMEM((4, top.ys, top.lanes), F32))
    temp("putd", pltpu.VMEM((8, top.lanes), F32))
    temp("gotx", pltpu.VMEM((4, top.run, top.lanes), F32))
    temp("goty", pltpu.VMEM((4, top.ys, top.lanes), F32))
    temp("gotd", pltpu.VMEM((8, top.lanes), F32))
    temp("fsend", pltpu.SemaphoreType.DMA((4,)))
    temp("frecv", pltpu.SemaphoreType.DMA((4,)))
    out = pl.pallas_call(
        functools.partial(kernel, levels, all_names),
        out_shape=jax.ShapeDtypeStruct((vecs, 3, nx * ny, nz), F32),
        in_specs=specs,
        out_specs=pl.BlockSpec(memory_space=pl.ANY),
        scratch_shapes=scratch,
        compiler_params=pltpu.CompilerParams(
            collective_id=0, has_side_effects=True, vmem_limit_bytes=60 * 1024 * 1024
        ),
    )(*args)
    return out.reshape(modes.shape)


def solution(mesh):
    placed = (P(None, None, "gx", "gy", None), P("gx", "gy", None), P("gx", "gy", None), P())
    return jax.shard_map(
        local,
        mesh=mesh,
        in_specs=placed,
        out_specs=P(None, None, "gx", "gy", None),
        check_vma=False,
    )
```

```python
import functools

import jax
import jax.numpy as jnp
import numpy as np
from jax import lax
from jax.experimental import pallas as pl
from jax.experimental.pallas import tpu as pltpu
from jax.sharding import PartitionSpec as P

DEG = 3
COARSE_DEG = 4
DEGREES = (4, 2, 1)
MU_SHEAR = 1.0
LAMBDA_BULK = 1.5
PROLONG_TABLES = {
    4: np.array(
        [[1.0, 0.0, 0.0], [0.375, 0.75, -0.125], [0.0, 1.0, 0.0], [-0.125, 0.75, 0.375]]
    ),
    2: np.array([[1.0, 0.0], [0.5, 0.5]]),
}
DIRS = ((-1, 0), (1, 0), (0, -1), (0, 1), (-1, -1), (-1, 1), (1, -1), (1, 1))
F32 = jnp.float32
BF16 = jnp.bfloat16
M_, K_, G_, T_ = range(4)


def element_matrices(degree):
    nodes = [float(place) / degree for place in range(degree + 1)]
    gauss_x, gauss_w = np.polynomial.legendre.leggauss(8)
    points = 0.5 * (gauss_x + 1.0)
    weights = 0.5 * gauss_w
    values = np.zeros((degree + 1, points.size))
    slopes = np.zeros((degree + 1, points.size))
    for column in range(degree + 1):
        product = np.ones(points.size)
        for other in range(degree + 1):
            if other != column:
                product = product * (points - nodes[other]) / (nodes[column] - nodes[other])
        values[column] = product
        for skipped in range(degree + 1):
            if skipped != column:
                part = np.ones(points.size) / (nodes[column] - nodes[skipped])
                for other in range(degree + 1):
                    if other != column and other != skipped:
                        part = part * (points - nodes[other]) / (nodes[column] - nodes[other])
                slopes[column] += part
    mass = (values * weights) @ values.T
    stiff = (slopes * weights) @ slopes.T
    mixed = (slopes * weights) @ values.T
    return [mass, stiff, mixed, mixed.T]


def assembled(element, count, ghost):
    p = element.shape[0] - 1
    out = np.zeros((count + 1, count + 1))
    for e in range(count // p):
        out[e * p : e * p + p + 1, e * p : e * p + p + 1] += element
    if ghost:
        out[0, 0] += element[p, p]
    return out


def up(n, m):
    return -(-n // m) * m


def bf16_parts(mat, count):
    rest = np.asarray(mat, np.float64)
    parts = []
    for _ in range(count):
        part = rest.astype(np.float32).astype(BF16)
        parts.append(part)
        rest = rest - part.astype(np.float64)
    return parts


def exact_bf16(mat):
    out = np.asarray(mat, np.float32).astype(BF16)
    assert np.array_equal(out.astype(np.float64), mat)
    return out


class Level:
    def __init__(self, degree, nx, ny, nz, vecs):
        self.p, self.nx, self.ny, self.nz, self.vecs = degree, nx, ny, nz, vecs
        self.ys = up(nx + 1, 8)
        self.run = up(ny, 8)
        self.base = 2 * self.ys + self.run
        self.rows = up(self.base + nx * self.run, 16)
        self.nb = self.base + self.run
        assert self.nb % 16 == 0
        self.lanes = up(vecs * nz, 128)
        self.low = 0
        self.where = {(x, y): self.row(x, y) for x in range(nx + 1) for y in range(ny + 1)}
        self.spans = (nx, ny)
        self.columns()

    def columns(self):
        if 3 * self.rows <= 256:
            self.kp, self.kb = self.rows, 256
        else:
            self.kp = up(self.rows, 128)
            self.kb = 3 * self.kp
        self.packed = self.kb == 256
        self.seg = 256 if self.packed else self.kp

    def row(self, x, y):
        if y == 0:
            return x
        if y == self.ny:
            return self.ys + x
        if x == self.nx:
            return 2 * self.ys + y
        return self.base + self.run * x + y

    def factors(self):
        out = []
        for axis, n in enumerate(self.spans):
            expand = np.zeros((self.rows, 32))
            spread = np.zeros((128, self.seg))
            for at, row in self.where.items():
                expand[row, at[axis] + self.low] = 1
                for copy in range(3 if self.packed else 1):
                    for part in range(3):
                        spread[32 * part + at[axis] + self.low, copy * self.kp + row] = 1
            table = np.zeros((2, 32, 512), BF16)
            for ghost in range(2):
                for i, element in enumerate(element_matrices(self.p)):
                    parts = bf16_parts(assembled(element, n, ghost), 3)
                    for part, mat in enumerate(parts):
                        at = 128 * i + 32 * part
                        table[ghost, : n + 1, at : at + n + 1] = mat
            out.append((exact_bf16(expand), table, exact_bf16(spread)))
        return out

    def lines(self):
        p, n = self.p, self.nz
        mats = []
        for e in element_matrices(p):
            full = assembled(e, n, True)[:n, :n].T
            if n % 128:
                lifted = np.zeros((self.lanes, self.lanes))
                size = self.vecs * n
                lifted[:size, :size] = np.kron(np.eye(self.vecs), full)
                full = lifted
            mats.append(np.stack(bf16_parts(full, 2)))
        return np.stack(mats)

    def diagonal(self):
        def center(which, count):
            p = self.p
            e = element_matrices(p)[which]
            line = np.array([e[a, a] + (e[p, p] if a == 0 else 0.0) for a in range(p)])
            return line[np.arange(count) % p]

        rows = np.zeros((self.rows, 128), np.float32)
        m_x, m_y, m_z = [center(0, n) for n in (self.nx + self.p, self.ny + self.p, self.nz)]
        k_x, k_y, k_z = [center(1, n) for n in (self.nx + self.p, self.ny + self.p, self.nz)]
        for c in range(3):
            coef = [MU_SHEAR + (LAMBDA_BULK + MU_SHEAR) * (c == e) for e in range(3)]
            for (x, y), row in self.where.items():
                x, y = x % self.p, y % self.p
                rows[row, c] = coef[0] * k_x[x] * m_y[y] + coef[1] * m_x[x] * k_y[y]
                rows[row, 3 + c] = coef[2] * m_x[x] * m_y[y]
        lanes = np.zeros((8, self.lanes), np.float32)
        lanes[0, : self.vecs * self.nz] = np.tile(m_z, self.vecs)
        lanes[1, : self.vecs * self.nz] = np.tile(k_z, self.vecs)
        return rows, lanes

    def sample(self, top):
        step = top.p // self.p
        sel_x = np.zeros((self.rows, top.rows))
        for (x, y), row in self.where.items():
            if (x * step, y * step) in top.where:
                sel_x[row, top.where[x * step, y * step]] = 1
        sel_z = np.zeros((top.lanes, self.lanes))
        for v in range(self.vecs):
            for z in range(self.nz):
                sel_z[v * top.nz + z * step, v * self.nz + z] = 1
        return exact_bf16(sel_x), exact_bf16(sel_z)


class Wide(Level):
    def __init__(self, degree, nx, ny, nz, vecs, ring):
        self.p, self.nx, self.ny, self.nz, self.vecs = degree, nx, ny, nz, vecs
        self.low = ring * degree
        self.spans = (nx + 2 * self.low, ny + 2 * self.low)
        self.lanes = up(vecs * nz, 128)
        self.half = self.lanes // 2
        assert vecs * nz <= self.half
        self.where = {}
        for x in range(-self.low, nx + self.low + 1):
            for y in range(-self.low, ny + self.low + 1):
                self.where[x, y] = len(self.where)
        self.rows = up(len(self.where), 16)
        self.nb = 0
        self.columns()
        self.plan()

    def plan(self):
        nx, ny, low = self.nx, self.ny, self.low
        closed = [(x, y) for x in range(nx + 1) for y in range(ny + 1)]
        far = [-(-(low + 1) // n) for n in (nx, ny)]
        self.far = far
        self.sections, self.sends = [], []
        self.pack_rows = 0
        at = 0
        kinds = {}
        for dx in range(-far[0], far[0] + 1):
            for dy in range(-far[1], far[1] + 1):
                nodes = tuple(
                    (x, y) for x, y in closed if (x - dx * nx, y - dy * ny) in self.where
                )
                if abs(dx) <= 1 and abs(dy) <= 1:
                    nodes = tuple(closed)
                if not nodes:
                    continue
                if nodes not in kinds:
                    k = len(nodes)
                    size = up(k + -(-k // 2), 8)
                    kinds[nodes] = (self.pack_rows, size)
                    self.sections.append((self.pack_rows, size, nodes))
                    self.pack_rows += size
                start, size = kinds[nodes]
                self.sends.append((dx, dy, start, size, at, nodes))
                at += size
        self.pack_rows = up(self.pack_rows, 16)
        self.got_rows = up(at, 16)

    def gather(self, fine, top):
        table = PROLONG_TABLES[fine.p]
        px, py = interpolation(table, fine.nx), interpolation(table, fine.ny)
        plane = {
            (cx, cy): np.array(
                [
                    [px[x, cx] * py[y, cy], row]
                    for (x, y), row in fine.where.items()
                    if px[x, cx] * py[y, cy] != 0.0
                ]
            )
            for cx in range(self.nx + 1)
            for cy in range(self.ny + 1)
        }
        pack = np.zeros((2, self.pack_rows, 4 * fine.rows))
        scale = np.zeros((self.pack_rows, top.rows))
        step = top.p // self.p
        for start, size, nodes in self.sections:
            k = len(nodes)
            h = -(-k // 2)
            for i, node in enumerate(nodes):
                for weight, row in plane[node]:
                    row = int(row)
                    for side in range(2):
                        pack[side, start + i, row] = weight
                        pack[side, start + i, fine.rows + row] = weight
                    side = i // h
                    pack[side, start + k + i % h, 2 * fine.rows + row] = weight
                    pack[side, start + k + i % h, 3 * fine.rows + row] = weight
                if node[0] < self.nx and node[1] < self.ny:
                    scale[start + i, top.where[node[0] * step, node[1] * step]] = 1
        place = np.zeros((3, self.rows, self.got_rows))
        for dx, dy, start, size, at, nodes in self.sends:
            k = len(nodes)
            h = -(-k // 2)
            for i, (x, y) in enumerate(nodes):
                to = self.where.get((x - dx * self.nx, y - dy * self.ny))
                if to is not None:
                    place[0, to, at + i] = 1
                    place[1 + i // h, to, at + k + i % h] = 1
        down = interpolation(table, fine.nz)[: fine.nz, : self.nz]
        line = np.zeros((2, 2 * fine.lanes, self.lanes))
        size = (self.vecs * fine.nz, self.vecs * self.nz)
        for side in range(2):
            for copy in range(2):
                line[
                    side,
                    copy * fine.lanes : copy * fine.lanes + size[0],
                    side * self.half : side * self.half + size[1],
                ] = np.kron(np.eye(self.vecs), down)
        mats = (
            pack.reshape(2 * self.pack_rows, 4 * fine.rows),
            scale,
            place.reshape(3 * self.rows, self.got_rows),
            line.reshape(4 * fine.lanes, self.lanes),
        )
        return [exact_bf16(m) for m in mats]


def interpolation(table, count):
    q = table.shape[0]
    half = q // 2
    out = np.zeros((count + 1, count // 2 + 1))
    for i in range(count + 1):
        for t in range(half + 1):
            j = half * (i // q) + t
            if table[i % q, t] != 0.0:
                out[i, j] += table[i % q, t]
    return out


def transfer(fine, coarse):
    table = PROLONG_TABLES[fine.p]
    px, py = interpolation(table, fine.nx), interpolation(table, fine.ny)
    pz = interpolation(table, fine.nz)[: fine.nz, : coarse.nz]
    plane = np.zeros((fine.rows, coarse.rows))
    for (x, y), row in fine.where.items():
        for (cx, cy), col in coarse.where.items():
            if 0 <= cx <= coarse.nx and 0 <= cy <= coarse.ny:
                plane[row, col] = px[x, cx] * py[y, cy]
    line = np.zeros((coarse.lanes, fine.lanes))
    size = (fine.vecs * coarse.nz, fine.vecs * fine.nz)
    line[: size[0], : size[1]] = np.kron(np.eye(fine.vecs), pz.T)
    down = (np.tile(plane.T, (1, 2)), np.tile(line.T, (2, 1)))
    upward = (np.tile(plane, (1, 2)), np.tile(line, (2, 1)))
    return [exact_bf16(m) for m in down + upward]


def halves(value):
    hi = value.astype(BF16)
    return hi, (value - hi.astype(F32)).astype(BF16)


def mm(a, b):
    return lax.dot_general(a, b, (((1,), (0,)), ((), ())), preferred_element_type=F32)


def wide3(value):
    hi, lo = halves(value)
    return jnp.concatenate([hi, lo, hi], axis=1)


def wide2(value):
    hi, lo = halves(value)
    return jnp.concatenate([hi, lo], axis=1)


def tall2(value):
    hi, lo = halves(value)
    return jnp.concatenate([hi, lo], axis=0)


def kernel(levels, names, *refs):
    R = dict(zip(names, refs))
    gx_n, gy_n = lax.axis_size("gx"), lax.axis_size("gy")
    me_x, me_y = lax.axis_index("gx"), lax.axis_index("gy")

    def reach(dx, dy):
        ok = None
        for d, me, n in ((dx, me_x, gx_n), (dy, me_y, gy_n)):
            if d:
                here = me + d < n if d > 0 else me + d >= 0
                ok = here if ok is None else jnp.logical_and(ok, here)
        return ok

    def device(dx, dy):
        return (jnp.clip(me_x + dx, 0, gx_n - 1), jnp.clip(me_y + dy, 0, gy_n - 1))

    top = levels[0]
    vecs, nz = top.vecs, top.nz
    body_rows = pl.ds(top.base, top.nx * top.run)

    moves = []

    def load(src, dst):
        moves.append(pltpu.make_async_copy(src, dst, R["lsem"].at[len(moves)]))
        moves[-1].start()

    load(R["moduli_in"], R["moduli"])
    load(R["pinned_in"], R["pinned"])
    load(R["spectrum_in"], R["spectrum"])
    for v in range(vecs):
        load(R["modes"].at[v], R["r0"].at[:, body_rows, pl.ds(v * nz, nz)])
    first_moves = len(moves)
    for l, lev in enumerate(levels):
        if lev.nz % 128 == 0:
            R[f"z{l}"][...] = jnp.zeros_like(R[f"z{l}"])
        load(R[f"tx{l}_in"].at[jnp.where(me_x == 0, 1, 0)], R[f"tx{l}"])
        load(R[f"ty{l}_in"].at[jnp.where(me_y == 0, 1, 0)], R[f"ty{l}"])
    for name in names:
        if name.endswith("_in") and name[:2] not in ("mo", "pi", "sp", "tx", "ty"):
            if name[0] == "z":
                lev = levels[int(name[1])]
                src, dst = R[name], R[name[:-3]]
                size = lev.nz if lev.nz % 128 == 0 else lev.lanes
                for s, half in enumerate((0, 0, 1)):
                    for at in range(0, lev.lanes, size):
                        load(
                            src.at[:, half],
                            dst.at[:, pl.ds(s * lev.lanes + at, size), pl.ds(at, size)],
                        )
            else:
                load(R[name], R[name[:-3]])

    wide = levels[-1]
    edged = range(len(levels) - 1)

    def clear(name):
        R[name][...] = jnp.zeros_like(R[name])

    for l in edged:
        for n in "xyd":
            clear(f"recv{n}{l}")
    for n in ("gotx", "goty", "gotd", "gets", "getb"):
        clear(n)

    barrier = pltpu.get_barrier_semaphore()
    peers = [(dx, dy) for dx, dy, *_ in wide.sends if dx or dy]
    assert set(DIRS) <= set(peers)
    for dx, dy in peers:

        @pl.when(reach(dx, dy))
        def _():
            pl.semaphore_signal(
                barrier, inc=1, device_id=device(dx, dy), device_id_type=pl.DeviceIdType.MESH
            )

    for l in edged:
        for n in "xyd":
            clear(f"send{n}{l}")
        clear(f"pend{l}")
    for l in range(len(levels)):
        clear(f"u{l}")

    for one in moves[:first_moves]:
        one.wait()
    chebyshev_table(R["spectrum"], R["coef"])
    scale = R["moduli"][...] * (1.0 - R["pinned"][...].astype(F32))
    s0 = R["s0"]
    s0[0 : top.base] = jnp.zeros((top.base, top.lanes), F32)
    for v in range(vecs):
        s0[body_rows, v * nz : (v + 1) * nz] = scale
    put = R["put"]
    put[...] = jnp.zeros_like(put)
    for c in range(3):
        for x in range(top.nx):
            at = top.base + x * top.run
            put[c, x : x + 1, :] = R["r0"][c, at : at + 1, :]
    for x in range(top.nx):
        at = top.base + x * top.run
        put[3, x : x + 1, :] = s0[at : at + 1, :]
    for c in range(4):
        R["putd"][c : c + 1, :] = put[c, 0:1, :]
    R["putd"][4:8, :] = jnp.zeros((4, top.lanes), F32)
    edge = pl.ds(top.base, top.run)

    def first_copies():
        plan = (
            (-1, 0, R["r0"].at[:, edge, :], R["gotx"].at[pl.ds(0, 3)]),
            (-1, 0, s0.at[edge, :], R["gotx"].at[3]),
            (0, -1, put, R["goty"]),
            (-1, -1, R["putd"], R["gotd"]),
        )
        for i, (dx, dy, src, dst) in enumerate(plan):
            yield dx, dy, pltpu.make_async_remote_copy(
                src_ref=src,
                dst_ref=dst,
                send_sem=R["fsend"].at[i],
                recv_sem=R["frecv"].at[i],
                device_id=device(dx, dy),
                device_id_type=pl.DeviceIdType.MESH,
            )

    around = []
    for me, n, far in ((me_x, gx_n, wide.far[0]), (me_y, gy_n, wide.far[1])):
        around.append(1 + jnp.minimum(me, far) + jnp.minimum(n - 1 - me, far))
    pl.semaphore_wait(barrier, around[0] * around[1] - 1)
    for dx, dy, copy in first_copies():
        pl.when(reach(dx, dy))(copy.start)
    for one in moves[first_moves:]:
        one.wait()

    def copies(l, slot):
        for i, (dx, dy) in enumerate(DIRS):
            kind, at = ("d", i - 4) if dx and dy else ("x", i) if dx else ("y", i - 2)
            yield dx, dy, pltpu.make_async_remote_copy(
                src_ref=R[f"send{kind}{l}"].at[at],
                dst_ref=R[f"recv{kind}{l}"].at[slot, at],
                send_sem=R[f"ssem{l}"].at[i],
                recv_sem=R[f"rsem{l}"].at[slot, i],
                device_id=device(dx, dy),
                device_id_type=pl.DeviceIdType.MESH,
            )

    def send(l, slot, part):
        lev = levels[l]
        ys, run, nx = lev.ys, lev.run, lev.nx
        sx, sy, sd = (R[f"send{n}{l}"] for n in "xyd")
        tile = 3 * run
        for c in range(3):
            sx[0, c * run : (c + 1) * run] = part[c][lev.base : lev.base + run]
            sx[1, c * run : (c + 1) * run] = part[c][2 * ys : 2 * ys + run]
            low, high = part[c][0:ys], part[c][ys : 2 * ys]
            sx[0, tile + c : tile + c + 1] = low[0:1]
            sx[0, tile + 3 + c : tile + 4 + c] = high[0:1]
            sx[1, tile + c : tile + c + 1] = low[nx : nx + 1]
            sx[1, tile + 3 + c : tile + 4 + c] = high[nx : nx + 1]
            sy[0, c * ys : (c + 1) * ys] = low
            sy[1, c * ys : (c + 1) * ys] = high
            sd[0, 3 + c : 4 + c] = low[0:1]
            sd[1, c : c + 1] = high[0:1]
            sd[2, 3 + c : 4 + c] = low[nx : nx + 1]
            sd[3, c : c + 1] = high[nx : nx + 1]
        for dx, dy, copy in copies(l, slot):
            pl.when(reach(dx, dy))(copy.start)

    def arrive(l, slot):
        lev = levels[l]
        ys, run, nx = lev.ys, lev.run, lev.nx
        for dx, dy, copy in copies(l, slot):
            pl.when(reach(-dx, -dy))(copy.wait_recv)
            pl.when(reach(dx, dy))(copy.wait_send)
        rx, ry, rd = (R[f"recv{n}{l}"] for n in "xyd")
        tile = pl.ds(3 * run, 8)
        left = rx[slot, 1, tile, :] + rd[slot, 2] + rd[slot, 3]
        right = rx[slot, 0, tile, :] + rd[slot, 0] + rd[slot, 1]
        at = lax.broadcasted_iota(jnp.int32, (ys, lev.lanes), 0)
        out = []
        for c in range(3):
            pieces = []
            for k, src in ((0, 1), (1, 0)):
                val = ry[slot, src, c * ys : (c + 1) * ys, :]
                val = val + jnp.where(at == 0, left[3 * k + c : 3 * k + c + 1], 0.0)
                val = val + jnp.where(at == nx, right[3 * k + c : 3 * k + c + 1], 0.0)
                pieces.append(val)
            pieces.append(rx[slot, 0, c * run : (c + 1) * run, :])
            pieces.append(rx[slot, 1, c * run : (c + 1) * run, :])
            out.append(jnp.concatenate(pieces, axis=0))
        return out

    def wide_copies(kind):
        index = 0
        for dx, dy, start, size, at, nodes in wide.sends:
            if dx == 0 and dy == 0:
                continue
            count = up(len(nodes), 8) if kind == "s" else size
            yield dx, dy, pltpu.make_async_remote_copy(
                src_ref=R[f"pack{kind}"].at[pl.ds(start, count)],
                dst_ref=R[f"get{kind}"].at[pl.ds(at, count)],
                send_sem=R[f"wsend{kind}"].at[index],
                recv_sem=R[f"wrecv{kind}"].at[index],
                device_id=device(dx, dy),
                device_id_type=pl.DeviceIdType.MESH,
            )
            index += 1

    def wide_send(kind, value):
        R[f"pack{kind}"][...] = value
        for dx, dy, start, size, at, nodes in wide.sends:
            if dx == 0 and dy == 0:
                R[f"get{kind}"][at : at + size] = value[start : start + size]
        for dx, dy, copy in wide_copies(kind):
            pl.when(reach(dx, dy))(copy.start)

    def wide_wait(kind):
        for dx, dy, copy in wide_copies(kind):
            pl.when(reach(-dx, -dy))(copy.wait_recv)
            pl.when(reach(dx, dy))(copy.wait_send)

    def thirds(value):
        parts = []
        for _ in range(3):
            parts.append(value.astype(BF16))
            value = value - parts[-1].astype(F32)
        return parts

    def wide_scale_send():
        sel = R["gs"][...]
        picked = [mm(sel, part).astype(BF16) for part in thirds(s0[...])]
        wide_send("s", sum(mm(part, R["sz"][...]) for part in picked))

    def wide_scale_take():
        wide_wait("s")
        place = R["place"][0 : wide.rows]
        R[f"s{len(levels) - 1}"][...] = sum(mm(place, part) for part in thirds(R["gets"][...]))
        prepare(len(levels) - 1, 0, wide.rows)

    def set_u(l, c, a, b, value):
        lev = levels[l]
        hi, lo = halves(value)
        at = c * lev.kb + a
        R[f"u{l}"][at : at + b - a] = hi
        R[f"u{l}"][at + lev.kp : at + lev.kp + b - a] = hi
        R[f"u{l}"][at + 2 * lev.kp : at + 2 * lev.kp + b - a] = lo

    def span(l, blk):
        lev = levels[l]
        return (0, lev.nb) if blk == "b" else (lev.nb, lev.rows)

    def prepare(l, a, b):
        s = R[f"s{l}"][a:b]
        f = jnp.where(s == 0.0, 1.0, 0.0)
        R[f"f{l}"][a:b] = f
        square = s * s
        m_z, k_z = R[f"kl{l}"][0:1, :], R[f"kl{l}"][1:2, :]
        for c in range(3):
            kd = R[f"kr{l}"][a:b, c : c + 1] * m_z + R[f"kr{l}"][a:b, 3 + c : 4 + c] * k_z
            R[f"dinv{l}"][c, a:b] = 1.0 / (square * kd + f)

    def begin(l, a, b, source):
        scale = R["coef"][l, 12]
        s = R[f"s{l}"][a:b]
        for c in range(3):
            first = scale * (R[f"dinv{l}"][c, a:b] * source[c])
            R[f"r{l}"][c, a:b] = source[c]
            R[f"d{l}"][c, a:b] = first
            R[f"x{l}"][c, a:b] = first
            set_u(l, c, a, b, s * first)

    def local_sums(l, blk):
        lev = levels[l]
        a, b = span(l, blk)
        n, kb = b - a, lev.kb
        u, w1, w2 = R[f"u{l}"], R[f"w1{blk}{l}"], R[f"w2{blk}{l}"]
        both = mm(w1[...], u[0 : 2 * kb])
        last = mm(w2[...], u[2 * kb : 3 * kb])
        mass = w2[3 * n : 4 * n]
        plain = [mm(mass, u[0:kb]), mm(mass, u[kb : 2 * kb]), last[3 * n : 4 * n]]
        stretch = (2.0 * MU_SHEAR + LAMBDA_BULK) / MU_SHEAR
        plain[2] = stretch * plain[2]

        def along(which, parts):
            return mm(jnp.concatenate([wide3(v) for v in parts], axis=0), R[f"z{l}"][which])

        zm = along(M_, [both[0:n], both[n : 2 * n], last[2 * n : 3 * n]])
        zk = along(K_, plain)
        zt = along(T_, [last[0:n], last[n : 2 * n]])
        zg = along(G_, [both[2 * n : 3 * n]])
        return [
            zm[0:n] + zk[0:n] + zt[0:n],
            zm[n : 2 * n] + zk[n : 2 * n] + zt[n : 2 * n],
            zm[2 * n : 3 * n] + zk[2 * n : 3 * n] + zg,
        ]

    def advance(l, k, a, b, sums):
        c1, c2 = R["coef"][l, 2 * k], R["coef"][l, 2 * k + 1]
        s, f = R[f"s{l}"][a:b], R[f"f{l}"][a:b]
        for c in range(3):
            d = R[f"d{l}"][c, a:b]
            res = R[f"r{l}"][c, a:b] - (s * sums[c] + f * d)
            new = c1 * d + c2 * (R[f"dinv{l}"][c, a:b] * res)
            R[f"r{l}"][c, a:b] = res
            R[f"d{l}"][c, a:b] = new
            R[f"x{l}"][c, a:b] += new
            set_u(l, c, a, b, s * new)

    def smooth(l, k, slot, beside=None):
        lev = levels[l]
        own, pend = R[f"own{l}"], R[f"pend{l}"]
        part = local_sums(l, "b")
        for c in range(3):
            part[c] = part[c] + pend[c]
            own[c] = part[c]
            pend[c] = jnp.zeros_like(pend[c])
        send(l, slot, part)
        inner = local_sums(l, "i")
        advance(l, k, lev.nb, lev.rows, inner)
        if beside is not None:
            beside()
        got = arrive(l, slot)
        advance(l, k, 0, lev.nb, [own[c] + got[c] for c in range(3)])

    def restrict(l):
        lev = levels[l]
        masked = []
        for blk in "bi":
            a, b = span(l, blk)
            sums = local_sums(l, blk)
            s, f = R[f"s{l}"][a:b], R[f"f{l}"][a:b]
            free = 1.0 - f
            if blk == "b":
                row = lax.broadcasted_iota(jnp.int32, (b - a, lev.lanes), 0)
                mine = jnp.logical_or(row < lev.nx, row >= lev.base)
                free = jnp.where(mine, free, 0.0)
            piece = []
            for c in range(3):
                r, d = R[f"r{l}"][c, a:b], R[f"d{l}"][c, a:b]
                piece.append(free * r - s * sums[c])
                if blk == "b":
                    R[f"pend{l}"][c] = sums[c]
                    R[f"r{l}"][c, a:b] = r - f * d
                else:
                    R[f"r{l}"][c, a:b] = r - (s * sums[c] + f * d)
            masked.append(piece)
        fields = [
            tall2(jnp.concatenate([masked[0][c], masked[1][c]], axis=0)) for c in range(3)
        ]
        if l + 1 == len(levels) - 1:
            n = wide.pack_rows
            flat = []
            for side in range(2):
                mat = R["gp"][side * n : (side + 1) * n]
                field = jnp.concatenate([fields[side], fields[2]], axis=0)
                flat.append(wide2(mm(mat, field)))
            return mm(jnp.concatenate(flat, axis=1), R["gz"][...])
        flat = [wide2(mm(R[f"dp{l}"][...], field)) for field in fields]
        down = mm(jnp.concatenate(flat, axis=0), R[f"dz{l}"][...])
        n = levels[l + 1].rows
        return [down[c * n : (c + 1) * n] for c in range(3)]

    def descend(l, slot, sums):
        lev = levels[l]
        own = R[f"own{l}"]
        for c in range(3):
            own[c] = sums[c][0 : lev.nb]
        send(l, slot, [sums[c][0 : lev.nb] for c in range(3)])
        free = 1.0 - R[f"f{l}"][lev.nb : lev.rows]
        begin(l, lev.nb, lev.rows, [free * sums[c][lev.nb : lev.rows] for c in range(3)])
        if l + 1 == len(levels) - 1:
            wide_scale_take()
        got = arrive(l, slot)
        free = 1.0 - R[f"f{l}"][0 : lev.nb]
        begin(l, 0, lev.nb, [free * (own[c] + got[c]) for c in range(3)])

    def solve_wide(packed):
        l, n, half = len(levels) - 1, wide.rows, wide.half
        wide_send("b", packed)
        wide_wait("b")
        hi, lo = halves(R["getb"][...])
        spread = mm(R["place"][...], hi) + mm(R["place"][...], lo)
        lane = lax.broadcasted_iota(jnp.int32, (n, wide.lanes), 1)
        keep = jnp.where(lane < half, 1.0 - R[f"f{l}"][...], 0.0)
        both, one, two = (spread[i * n : (i + 1) * n] for i in range(3))
        right = [both, pltpu.roll(both, half, 1), one + pltpu.roll(two, half, 1)]
        begin(l, 0, n, [keep * v for v in right])

        def body(k, _):
            advance(l, k, 0, n, local_sums(l, "i"))
            return 0

        lax.fori_loop(0, COARSE_DEG - 1, body, 0)

    def ascend(l):
        lev, n = levels[l], levels[l + 1].rows
        field = jnp.concatenate([wide2(R[f"x{l + 1}"][c]) for c in range(3)], axis=0)
        fine = mm(field, R[f"uz{l}"][...])
        free, s = 1.0 - R[f"f{l}"][...], R[f"s{l}"][...]
        for c in range(3):
            step = free * mm(R[f"up{l}"][...], tall2(fine[c * n : (c + 1) * n]))
            R[f"d{l}"][c] = step
            R[f"x{l}"][c] += step
            set_u(l, c, 0, lev.rows, s * step)

    def build(l):
        lev = levels[l]
        lines = []
        for axis in "xy":
            tall = mm(R[f"e{axis}{l}"][...], R[f"t{axis}{l}"][...])
            lines.append(
                [
                    mm(tall[:, 128 * i : 128 * (i + 1)].astype(BF16), R[f"c{axis}{l}"][...])
                    for i in range(4)
                ]
            )
        X, Y = lines
        cc = LAMBDA_BULK + MU_SHEAR
        big = MU_SHEAR + cc
        kxmy, mxky = X[K_] * Y[M_], X[M_] * Y[K_]
        first = (
            (0, 0, big * kxmy + MU_SHEAR * mxky),
            (0, 1, cc * (X[G_] * Y[T_])),
            (1, 0, cc * (X[T_] * Y[G_])),
            (1, 1, MU_SHEAR * kxmy + big * mxky),
            (2, 0, cc * (X[T_] * Y[M_])),
            (2, 1, cc * (X[M_] * Y[T_])),
        )
        second = (
            cc * (X[G_] * Y[M_]),
            cc * (X[M_] * Y[G_]),
            MU_SHEAR * (kxmy + mxky),
            X[M_] * Y[M_],
        )
        lane = lax.broadcasted_iota(jnp.int32, (lev.rows, lev.seg), 1)
        middle = jnp.logical_and(lane >= lev.kp, lane < 2 * lev.kp)

        def store(kind, group, at, value):
            hi, lo = halves(value)
            for blk in "bi" if lev.nb else "i":
                a, b = span(l, blk)
                ref, row = R[f"{kind}{blk}{l}"], group * (b - a)
                row = slice(row, row + b - a)
                if lev.packed:
                    mixed = jnp.where(middle, lo.astype(F32), hi.astype(F32)).astype(BF16)
                    ref[row, at : at + 256] = mixed[a:b]
                else:
                    for s, half in enumerate((hi, lo, hi)):
                        start = at + s * lev.kp
                        ref[row, start : start + lev.kp] = half[a:b]

        for group, side, value in first:
            store("w1", group, side * lev.kb, value)
        for group, value in enumerate(second):
            store("w2", group, 0, value)

    build(0)

    def clear_spare(a, b):
        lead = lax.broadcasted_iota(jnp.int32, (b - a, top.lanes), 0) % top.run == 0
        s0[a:b] = jnp.where(lead, 0.0, s0[a:b])

    clear_spare(top.nb, top.rows)
    prepare(0, top.nb, top.rows)
    begin(0, top.nb, top.rows, [R["r0"][c, top.nb : top.rows] for c in range(3)])
    for dx, dy, copy in first_copies():
        pl.when(reach(dx, dy))(copy.wait_send)
        pl.when(reach(-dx, -dy))(copy.wait_recv)
    clear_spare(top.base, top.nb)
    ys, run, nx = top.ys, top.run, top.nx
    at = lax.broadcasted_iota(jnp.int32, (ys, top.lanes), 0)
    for c in range(4):
        dst = s0 if c == 3 else R["r0"].at[c]
        low = jnp.where(at == nx, R["gotx"][c, 0:1, :], put[c])
        high = jnp.where(at == nx, R["gotd"][c : c + 1, :], R["goty"][c])
        dst[0:ys] = low
        dst[ys : 2 * ys] = high
        side = R["gotx"][c]
        if c == 3:
            row = lax.broadcasted_iota(jnp.int32, (run, top.lanes), 0)
            side = jnp.where(row == 0, 0.0, side)
        dst[2 * ys : 2 * ys + run] = side
    prepare(0, 0, top.nb)
    begin(0, 0, top.nb, [R["r0"][c, 0 : top.nb] for c in range(3)])

    def coarse_setup():
        parts = thirds(s0[...])
        build(len(levels) - 1)
        for l in range(1, len(levels) - 1):
            sel_x, sel_z = R[f"sx{l}"][...], R[f"sz{l}"][...]
            picked = [mm(sel_x, part).astype(BF16) for part in parts]
            R[f"s{l}"][...] = sum(mm(part, sel_z) for part in picked)
            prepare(l, 0, levels[l].rows)
            build(l)

    def pre(k, _):
        smooth(0, k, k % 2, lambda: pl.when(k == 0)(coarse_setup))
        return 0

    def cycle(l):
        skip = 0 if l == 0 else 1

        def body(k, _):
            smooth(l, k, (k + skip) % 2)
            return 0

        def tail(k, _):
            smooth(l, k, (k + skip + 1) % 2)
            return 0

        lax.fori_loop(0, DEG - 1, pre if l == 0 else body, 0)
        if l == 0:
            wide_scale_send()
        if l + 1 == len(levels) - 1:
            solve_wide(restrict(l))
        else:
            descend(l + 1, 0, restrict(l))
            cycle(l + 1)
        ascend(l)
        lax.fori_loop(DEG, 2 * DEG, tail, 0)

    cycle(0)
    for c in range(3):
        for x in range(nx):
            row = top.base + x * run
            R["x0"][c, row : row + 1, :] = R["x0"][c, x : x + 1, :]
    backs = [
        pltpu.make_async_copy(
            R["x0"].at[:, body_rows, pl.ds(v * nz, nz)], R["out"].at[v], R["lsem"].at[v]
        )
        for v in range(vecs)
    ]
    for one in backs:
        one.start()
    for one in backs:
        one.wait()


def chebyshev_table(spectrum, coef):
    for l in range(3):
        low, top = spectrum[l, 0], spectrum[l, 1]
        center = 0.5 * (top + low)
        radius = 0.5 * (top - low)
        ratio = center / radius
        rho = 1.0 / ratio
        steps = []
        for _ in range(COARSE_DEG - 1):
            rho_next = 1.0 / (2.0 * ratio - rho)
            steps.append((rho_next * rho, 2.0 * rho_next / radius))
            rho = rho_next
        smooth = steps[: DEG - 1]
        flat = [(0.0, 0.0), (0.0, 1.0 / center)]
        picked = steps if l == 2 else smooth + flat + smooth
        for k, two in enumerate(picked):
            coef[l, 2 * k] = jnp.asarray(two[0], F32)
            coef[l, 2 * k + 1] = jnp.asarray(two[1], F32)
        coef[l, 12] = 1.0 / center


def local(modes, moduli, pinned, spectrum):
    vecs, _, nx, ny, nz = modes.shape
    levels = []
    names, args = [], []

    def add(name, value):
        names.append(name)
        args.append(value)

    for degree in DEGREES:
        step = DEGREES[0] // degree
        size = (degree, nx // step, ny // step, nz // step, vecs)
        levels.append(Level(*size) if step < DEGREES[0] else Wide(*size, COARSE_DEG - 1))
    top = levels[0]
    assert ny == top.run and nz % 128 == 0
    add("spectrum_in", spectrum)
    add("modes", modes.reshape(vecs, 3, nx * ny, nz))
    add("moduli_in", moduli.reshape(nx * ny, nz))
    add("pinned_in", pinned.reshape(nx * ny, nz))
    for l, lev in enumerate(levels):
        for axis, mats in zip("xy", lev.factors()):
            for key, mat in zip("etc", mats):
                add(f"{key}{axis}{l}_in", jnp.asarray(mat))
        add(f"z{l}_in", jnp.asarray(lev.lines()))
        for key, mat in zip(("kr", "kl"), lev.diagonal()):
            add(f"{key}{l}_in", jnp.asarray(mat))
        if l + 1 < len(levels):
            coarsest = l + 2 == len(levels)
            for key, mat in zip(("dp", "dz", "up", "uz"), transfer(lev, levels[l + 1])):
                if key[0] == "u" or not coarsest:
                    add(f"{key}{l}_in", jnp.asarray(mat))
        if 0 < l < len(levels) - 1:
            for key, mat in zip(("sx", "sz"), lev.sample(top)):
                add(f"{key}{l}_in", jnp.asarray(mat))
    wide = levels[-1]
    for key, mat in zip(("gp", "gs", "place", "gz"), wide.gather(levels[-2], top)):
        add(f"{key}_in", jnp.asarray(mat))
    add("sz_in", jnp.asarray(wide.sample(top)[1]))

    specs = [pl.BlockSpec(memory_space=pl.ANY) for n in names]
    scratch = []
    all_names = names + ["out"]

    def temp(name, what):
        all_names.append(name)
        scratch.append(what)

    temp("coef", pltpu.SMEM((3, 13), F32))
    temp("lsem", pltpu.SemaphoreType.DMA((len(names) + 24,)))
    for name, value in zip(names, args):
        if name == "spectrum_in":
            temp("spectrum", pltpu.SMEM(value.shape, F32))
        elif name.endswith("_in"):
            shape = value.shape
            if name[0] == "z":
                lanes = levels[int(name[1])].lanes
                shape = (4, 3 * lanes, lanes)
            elif name[0] == "t":
                shape = shape[1:]
            temp(name[:-3], pltpu.VMEM(shape, value.dtype))
    for l, lev in enumerate(levels):
        field = (3, lev.rows, lev.lanes)
        for n in ("s", "f"):
            temp(f"{n}{l}", pltpu.VMEM(field[1:], F32))
        for n in ("r", "d", "x", "dinv"):
            temp(f"{n}{l}", pltpu.VMEM(field, F32))
        temp(f"u{l}", pltpu.VMEM((3 * lev.kb, lev.lanes), BF16))
        for blk, n in (("b", lev.nb), ("i", lev.rows - lev.nb)):
            if n:
                temp(f"w1{blk}{l}", pltpu.VMEM((3 * n, 2 * lev.kb), BF16))
                temp(f"w2{blk}{l}", pltpu.VMEM((4 * n, lev.kb), BF16))
        if lev is wide:
            continue
        for n in ("own", "pend"):
            temp(f"{n}{l}", pltpu.VMEM((3, lev.nb, lev.lanes), F32))
        for n, shape in (
            ("x", (2, 3 * lev.run + 8, lev.lanes)),
            ("y", (2, 3 * lev.ys, lev.lanes)),
            ("d", (4, 8, lev.lanes)),
        ):
            temp(f"send{n}{l}", pltpu.VMEM(shape, F32))
            temp(f"recv{n}{l}", pltpu.VMEM((2,) + shape, F32))
        temp(f"ssem{l}", pltpu.SemaphoreType.DMA((len(DIRS),)))
        temp(f"rsem{l}", pltpu.SemaphoreType.DMA((2, len(DIRS))))
    for kind in "sb":
        temp(f"pack{kind}", pltpu.VMEM((wide.pack_rows, wide.lanes), F32))
        temp(f"get{kind}", pltpu.VMEM((wide.got_rows, wide.lanes), F32))
        temp(f"wsend{kind}", pltpu.SemaphoreType.DMA((len(wide.sends) - 1,)))
        temp(f"wrecv{kind}", pltpu.SemaphoreType.DMA((len(wide.sends) - 1,)))
    temp("put", pltpu.VMEM((4, top.ys, top.lanes), F32))
    temp("putd", pltpu.VMEM((8, top.lanes), F32))
    temp("gotx", pltpu.VMEM((4, top.run, top.lanes), F32))
    temp("goty", pltpu.VMEM((4, top.ys, top.lanes), F32))
    temp("gotd", pltpu.VMEM((8, top.lanes), F32))
    temp("fsend", pltpu.SemaphoreType.DMA((4,)))
    temp("frecv", pltpu.SemaphoreType.DMA((4,)))
    out = pl.pallas_call(
        functools.partial(kernel, levels, all_names),
        out_shape=jax.ShapeDtypeStruct((vecs, 3, nx * ny, nz), F32),
        in_specs=specs,
        out_specs=pl.BlockSpec(memory_space=pl.ANY),
        scratch_shapes=scratch,
        compiler_params=pltpu.CompilerParams(
            collective_id=0, has_side_effects=True, vmem_limit_bytes=60 * 1024 * 1024
        ),
    )(*args)
    return out.reshape(modes.shape)


def solution(mesh):
    placed = (P(None, None, "gx", "gy", None), P("gx", "gy", None), P("gx", "gy", None), P())
    return jax.shard_map(
        local,
        mesh=mesh,
        in_specs=placed,
        out_specs=P(None, None, "gx", "gy", None),
        check_vma=False,
    )
```

```python
import functools

import jax
import jax.numpy as jnp
import numpy as np
from jax import lax
from jax.experimental import pallas as pl
from jax.experimental.pallas import tpu as pltpu
from jax.sharding import PartitionSpec as P

DEG = 3
COARSE_DEG = 4
DEGREES = (4, 2, 1)
MU_SHEAR = 1.0
LAMBDA_BULK = 1.5
PROLONG_TABLES = {
    4: np.array(
        [[1.0, 0.0, 0.0], [0.375, 0.75, -0.125], [0.0, 1.0, 0.0], [-0.125, 0.75, 0.375]]
    ),
    2: np.array([[1.0, 0.0], [0.5, 0.5]]),
}
DIRS = ((-1, 0), (1, 0), (0, -1), (0, 1), (-1, -1), (-1, 1), (1, -1), (1, 1))
F32 = jnp.float32
BF16 = jnp.bfloat16
M_, K_, G_, T_ = range(4)


def element_matrices(degree):
    nodes = [float(place) / degree for place in range(degree + 1)]
    gauss_x, gauss_w = np.polynomial.legendre.leggauss(8)
    points = 0.5 * (gauss_x + 1.0)
    weights = 0.5 * gauss_w
    values = np.zeros((degree + 1, points.size))
    slopes = np.zeros((degree + 1, points.size))
    for column in range(degree + 1):
        product = np.ones(points.size)
        for other in range(degree + 1):
            if other != column:
                product = product * (points - nodes[other]) / (nodes[column] - nodes[other])
        values[column] = product
        for skipped in range(degree + 1):
            if skipped != column:
                part = np.ones(points.size) / (nodes[column] - nodes[skipped])
                for other in range(degree + 1):
                    if other != column and other != skipped:
                        part = part * (points - nodes[other]) / (nodes[column] - nodes[other])
                slopes[column] += part
    mass = (values * weights) @ values.T
    stiff = (slopes * weights) @ slopes.T
    mixed = (slopes * weights) @ values.T
    return [mass, stiff, mixed, mixed.T]


def assembled(element, count, ghost):
    p = element.shape[0] - 1
    out = np.zeros((count + 1, count + 1))
    for e in range(count // p):
        out[e * p : e * p + p + 1, e * p : e * p + p + 1] += element
    if ghost:
        out[0, 0] += element[p, p]
    return out


def up(n, m):
    return -(-n // m) * m


def bf16_parts(mat, count):
    rest = np.asarray(mat, np.float64)
    parts = []
    for _ in range(count):
        part = rest.astype(np.float32).astype(BF16)
        parts.append(part)
        rest = rest - part.astype(np.float64)
    return parts


def exact_bf16(mat):
    out = np.asarray(mat, np.float32).astype(BF16)
    assert np.array_equal(out.astype(np.float64), mat)
    return out


class Level:
    def __init__(self, degree, nx, ny, nz, vecs):
        self.p, self.nx, self.ny, self.nz, self.vecs = degree, nx, ny, nz, vecs
        self.ys = up(nx + 1, 8)
        self.run = up(ny, 8)
        self.base = 2 * self.ys + self.run
        self.rows = up(self.base + nx * self.run, 16)
        self.nb = self.base + self.run
        assert self.nb % 16 == 0
        self.lanes = up(vecs * nz, 128)
        self.low = 0
        self.where = {(x, y): self.row(x, y) for x in range(nx + 1) for y in range(ny + 1)}
        self.spans = (nx, ny)
        self.columns()

    def columns(self):
        if 3 * self.rows <= 256:
            self.kp, self.kb = self.rows, 256
        else:
            self.kp = up(self.rows, 128)
            self.kb = 3 * self.kp
        self.packed = self.kb == 256
        self.split = not self.packed and 0 < 3 * self.nb <= 256 == self.kp
        self.seg = 256 if self.packed else self.kp

    def row(self, x, y):
        if y == 0:
            return x
        if y == self.ny:
            return self.ys + x
        if x == self.nx:
            return 2 * self.ys + y
        return self.base + self.run * x + y

    def factors(self):
        out = []
        for axis, n in enumerate(self.spans):
            expand = np.zeros((self.rows, 32))
            spread = np.zeros((128, self.seg))
            for at, row in self.where.items():
                expand[row, at[axis] + self.low] = 1
                for copy in range(3 if self.packed else 1):
                    for part in range(3):
                        spread[32 * part + at[axis] + self.low, copy * self.kp + row] = 1
            table = np.zeros((2, 32, 512), BF16)
            for ghost in range(2):
                for i, element in enumerate(element_matrices(self.p)):
                    parts = bf16_parts(assembled(element, n, ghost), 3)
                    for part, mat in enumerate(parts):
                        at = 128 * i + 32 * part
                        table[ghost, : n + 1, at : at + n + 1] = mat
            out.append((exact_bf16(expand), table, exact_bf16(spread)))
        return out

    def lines(self):
        p, n = self.p, self.nz
        mats = []
        for e in element_matrices(p):
            full = assembled(e, n, True)[:n, :n].T
            if n % 128:
                lifted = np.zeros((self.lanes, self.lanes))
                size = self.vecs * n
                lifted[:size, :size] = np.kron(np.eye(self.vecs), full)
                full = lifted
            mats.append(np.stack(bf16_parts(full, 2)))
        return np.stack(mats)

    def diagonal(self):
        def center(which, count):
            p = self.p
            e = element_matrices(p)[which]
            line = np.array([e[a, a] + (e[p, p] if a == 0 else 0.0) for a in range(p)])
            return line[np.arange(count) % p]

        rows = np.zeros((self.rows, 128), np.float32)
        m_x, m_y, m_z = [center(0, n) for n in (self.nx + self.p, self.ny + self.p, self.nz)]
        k_x, k_y, k_z = [center(1, n) for n in (self.nx + self.p, self.ny + self.p, self.nz)]
        for c in range(3):
            coef = [MU_SHEAR + (LAMBDA_BULK + MU_SHEAR) * (c == e) for e in range(3)]
            for (x, y), row in self.where.items():
                x, y = x % self.p, y % self.p
                rows[row, c] = coef[0] * k_x[x] * m_y[y] + coef[1] * m_x[x] * k_y[y]
                rows[row, 3 + c] = coef[2] * m_x[x] * m_y[y]
        lanes = np.zeros((8, self.lanes), np.float32)
        lanes[0, : self.vecs * self.nz] = np.tile(m_z, self.vecs)
        lanes[1, : self.vecs * self.nz] = np.tile(k_z, self.vecs)
        return rows, lanes

    def sample(self, top):
        step = top.p // self.p
        sel_x = np.zeros((self.rows, top.rows))
        for (x, y), row in self.where.items():
            if (x * step, y * step) in top.where:
                sel_x[row, top.where[x * step, y * step]] = 1
        sel_z = np.zeros((top.lanes, self.lanes))
        for v in range(self.vecs):
            for z in range(self.nz):
                sel_z[v * top.nz + z * step, v * self.nz + z] = 1
        return exact_bf16(sel_x), exact_bf16(sel_z)


class Wide(Level):
    def __init__(self, degree, nx, ny, nz, vecs, ring):
        self.p, self.nx, self.ny, self.nz, self.vecs = degree, nx, ny, nz, vecs
        self.low = ring * degree
        self.spans = (nx + 2 * self.low, ny + 2 * self.low)
        self.lanes = up(vecs * nz, 128)
        self.half = self.lanes // 2
        assert vecs * nz <= self.half
        self.where = {}
        for x in range(-self.low, nx + self.low + 1):
            for y in range(-self.low, ny + self.low + 1):
                self.where[x, y] = len(self.where)
        self.rows = up(len(self.where), 16)
        self.nb = 0
        self.columns()
        self.plan()

    def plan(self):
        nx, ny, low = self.nx, self.ny, self.low
        closed = [(x, y) for x in range(nx + 1) for y in range(ny + 1)]
        far = [-(-(low + 1) // n) for n in (nx, ny)]
        self.far = far
        self.sections, self.sends = [], []
        self.pack_rows = 0
        at = 0
        kinds = {}
        for dx in range(-far[0], far[0] + 1):
            for dy in range(-far[1], far[1] + 1):
                nodes = tuple(
                    (x, y) for x, y in closed if (x - dx * nx, y - dy * ny) in self.where
                )
                if abs(dx) <= 1 and abs(dy) <= 1:
                    nodes = tuple(closed)
                if not nodes:
                    continue
                if nodes not in kinds:
                    k = len(nodes)
                    size = up(k + -(-k // 2), 8)
                    kinds[nodes] = (self.pack_rows, size)
                    self.sections.append((self.pack_rows, size, nodes))
                    self.pack_rows += size
                start, size = kinds[nodes]
                self.sends.append((dx, dy, start, size, at, nodes))
                at += size
        self.pack_rows = up(self.pack_rows, 16)
        self.got_rows = up(at, 16)

    def gather(self, fine, top):
        table = PROLONG_TABLES[fine.p]
        px, py = interpolation(table, fine.nx), interpolation(table, fine.ny)
        plane = {
            (cx, cy): np.array(
                [
                    [px[x, cx] * py[y, cy], row]
                    for (x, y), row in fine.where.items()
                    if px[x, cx] * py[y, cy] != 0.0
                ]
            )
            for cx in range(self.nx + 1)
            for cy in range(self.ny + 1)
        }
        pack = np.zeros((2, self.pack_rows, 4 * fine.rows))
        scale = np.zeros((self.pack_rows, top.rows))
        step = top.p // self.p
        for start, size, nodes in self.sections:
            k = len(nodes)
            h = -(-k // 2)
            for i, node in enumerate(nodes):
                for weight, row in plane[node]:
                    row = int(row)
                    for side in range(2):
                        pack[side, start + i, row] = weight
                        pack[side, start + i, fine.rows + row] = weight
                    side = i // h
                    pack[side, start + k + i % h, 2 * fine.rows + row] = weight
                    pack[side, start + k + i % h, 3 * fine.rows + row] = weight
                if node[0] < self.nx and node[1] < self.ny:
                    scale[start + i, top.where[node[0] * step, node[1] * step]] = 1
        place = np.zeros((3, self.rows, self.got_rows))
        for dx, dy, start, size, at, nodes in self.sends:
            k = len(nodes)
            h = -(-k // 2)
            for i, (x, y) in enumerate(nodes):
                to = self.where.get((x - dx * self.nx, y - dy * self.ny))
                if to is not None:
                    place[0, to, at + i] = 1
                    place[1 + i // h, to, at + k + i % h] = 1
        down = interpolation(table, fine.nz)[: fine.nz, : self.nz]
        line = np.zeros((2, 2 * fine.lanes, self.lanes))
        size = (self.vecs * fine.nz, self.vecs * self.nz)
        for side in range(2):
            for copy in range(2):
                line[
                    side,
                    copy * fine.lanes : copy * fine.lanes + size[0],
                    side * self.half : side * self.half + size[1],
                ] = np.kron(np.eye(self.vecs), down)
        mats = (
            pack.reshape(2 * self.pack_rows, 4 * fine.rows),
            scale,
            place.reshape(3 * self.rows, self.got_rows),
            line.reshape(4 * fine.lanes, self.lanes),
        )
        return [exact_bf16(m) for m in mats]


def interpolation(table, count):
    q = table.shape[0]
    half = q // 2
    out = np.zeros((count + 1, count // 2 + 1))
    for i in range(count + 1):
        for t in range(half + 1):
            j = half * (i // q) + t
            if table[i % q, t] != 0.0:
                out[i, j] += table[i % q, t]
    return out


def transfer(fine, coarse):
    table = PROLONG_TABLES[fine.p]
    px, py = interpolation(table, fine.nx), interpolation(table, fine.ny)
    pz = interpolation(table, fine.nz)[: fine.nz, : coarse.nz]
    plane = np.zeros((fine.rows, coarse.rows))
    for (x, y), row in fine.where.items():
        for (cx, cy), col in coarse.where.items():
            if 0 <= cx <= coarse.nx and 0 <= cy <= coarse.ny:
                plane[row, col] = px[x, cx] * py[y, cy]
    line = np.zeros((coarse.lanes, fine.lanes))
    size = (fine.vecs * coarse.nz, fine.vecs * fine.nz)
    line[: size[0], : size[1]] = np.kron(np.eye(fine.vecs), pz.T)
    down = (np.tile(plane.T, (1, 2)), np.tile(line.T, (2, 1)))
    upward = (np.tile(plane, (1, 2)), np.tile(line, (2, 1)))
    return [exact_bf16(m) for m in down + upward]


def halves(value):
    hi = value.astype(BF16)
    return hi, (value - hi.astype(F32)).astype(BF16)


def mm(a, b):
    return lax.dot_general(a, b, (((1,), (0,)), ((), ())), preferred_element_type=F32)


def wide3(value):
    hi, lo = halves(value)
    return jnp.concatenate([hi, lo, hi], axis=1)


def wide2(value):
    hi, lo = halves(value)
    return jnp.concatenate([hi, lo], axis=1)


def tall2(value):
    hi, lo = halves(value)
    return jnp.concatenate([hi, lo], axis=0)


def kernel(levels, names, *refs):
    R = dict(zip(names, refs))
    gx_n, gy_n = lax.axis_size("gx"), lax.axis_size("gy")
    me_x, me_y = lax.axis_index("gx"), lax.axis_index("gy")

    def reach(dx, dy):
        ok = None
        for d, me, n in ((dx, me_x, gx_n), (dy, me_y, gy_n)):
            if d:
                here = me + d < n if d > 0 else me + d >= 0
                ok = here if ok is None else jnp.logical_and(ok, here)
        return ok

    def device(dx, dy):
        return (jnp.clip(me_x + dx, 0, gx_n - 1), jnp.clip(me_y + dy, 0, gy_n - 1))

    top = levels[0]
    vecs, nz = top.vecs, top.nz
    body_rows = pl.ds(top.base, top.nx * top.run)

    moves = []

    def load(src, dst):
        moves.append(pltpu.make_async_copy(src, dst, R["lsem"].at[len(moves)]))
        moves[-1].start()

    load(R["moduli_in"], R["moduli"])
    load(R["pinned_in"], R["pinned"])
    load(R["spectrum_in"], R["spectrum"])
    for v in range(vecs):
        load(R["modes"].at[v], R["r0"].at[:, body_rows, pl.ds(v * nz, nz)])
    first_moves = len(moves)
    for l, lev in enumerate(levels):
        if lev.nz % 128 == 0:
            R[f"z{l}"][...] = jnp.zeros_like(R[f"z{l}"])
        load(R[f"tx{l}_in"].at[jnp.where(me_x == 0, 1, 0)], R[f"tx{l}"])
        load(R[f"ty{l}_in"].at[jnp.where(me_y == 0, 1, 0)], R[f"ty{l}"])
    for name in names:
        if name.endswith("_in") and name[:2] not in ("mo", "pi", "sp", "tx", "ty"):
            if name[0] == "z":
                lev = levels[int(name[1])]
                src, dst = R[name], R[name[:-3]]
                size = lev.nz if lev.nz % 128 == 0 else lev.lanes
                for s, half in enumerate((0, 0, 1)):
                    for at in range(0, lev.lanes, size):
                        load(
                            src.at[:, half],
                            dst.at[:, pl.ds(s * lev.lanes + at, size), pl.ds(at, size)],
                        )
            else:
                load(R[name], R[name[:-3]])

    wide = levels[-1]
    edged = range(len(levels) - 1)

    def clear(name):
        R[name][...] = jnp.zeros_like(R[name])

    for l in edged:
        for n in "xyd":
            clear(f"recv{n}{l}")
    for n in ("gotx", "goty", "gotd", "gets", "getb"):
        clear(n)

    barrier = pltpu.get_barrier_semaphore()
    peers = [(dx, dy) for dx, dy, *_ in wide.sends if dx or dy]
    assert set(DIRS) <= set(peers)
    for dx, dy in peers:

        @pl.when(reach(dx, dy))
        def _():
            pl.semaphore_signal(
                barrier, inc=1, device_id=device(dx, dy), device_id_type=pl.DeviceIdType.MESH
            )

    for l in edged:
        for n in "xyd":
            clear(f"send{n}{l}")
        clear(f"pend{l}")
    for l in range(len(levels)):
        clear(f"u{l}")
        if levels[l].split:
            clear(f"ub{l}")

    for one in moves[:first_moves]:
        one.wait()
    chebyshev_table(R["spectrum"], R["coef"])
    scale = R["moduli"][...] * (1.0 - R["pinned"][...].astype(F32))
    s0 = R["s0"]
    s0[0 : top.base] = jnp.zeros((top.base, top.lanes), F32)
    for v in range(vecs):
        s0[body_rows, v * nz : (v + 1) * nz] = scale
    put = R["put"]
    put[...] = jnp.zeros_like(put)
    for c in range(3):
        for x in range(top.nx):
            at = top.base + x * top.run
            put[c, x : x + 1, :] = R["r0"][c, at : at + 1, :]
    for x in range(top.nx):
        at = top.base + x * top.run
        put[3, x : x + 1, :] = s0[at : at + 1, :]
    for c in range(4):
        R["putd"][c : c + 1, :] = put[c, 0:1, :]
    R["putd"][4:8, :] = jnp.zeros((4, top.lanes), F32)
    edge = pl.ds(top.base, top.run)

    def first_copies():
        plan = (
            (-1, 0, R["r0"].at[:, edge, :], R["gotx"].at[pl.ds(0, 3)]),
            (-1, 0, s0.at[edge, :], R["gotx"].at[3]),
            (0, -1, put, R["goty"]),
            (-1, -1, R["putd"], R["gotd"]),
        )
        for i, (dx, dy, src, dst) in enumerate(plan):
            yield dx, dy, pltpu.make_async_remote_copy(
                src_ref=src,
                dst_ref=dst,
                send_sem=R["fsend"].at[i],
                recv_sem=R["frecv"].at[i],
                device_id=device(dx, dy),
                device_id_type=pl.DeviceIdType.MESH,
            )

    around = []
    for me, n, far in ((me_x, gx_n, wide.far[0]), (me_y, gy_n, wide.far[1])):
        around.append(1 + jnp.minimum(me, far) + jnp.minimum(n - 1 - me, far))
    pl.semaphore_wait(barrier, around[0] * around[1] - 1)
    for dx, dy, copy in first_copies():
        pl.when(reach(dx, dy))(copy.start)
    for one in moves[first_moves:]:
        one.wait()

    def copies(l, slot):
        for i, (dx, dy) in enumerate(DIRS):
            kind, at = ("d", i - 4) if dx and dy else ("x", i) if dx else ("y", i - 2)
            src, dst = R[f"send{kind}{l}"].at[at], R[f"recv{kind}{l}"].at[slot, at]
            if kind == "d":
                src, dst = src.at[pl.ds(0, 3)], dst.at[pl.ds(0, 3)]
            yield dx, dy, pltpu.make_async_remote_copy(
                src_ref=src,
                dst_ref=dst,
                send_sem=R[f"ssem{l}"].at[i],
                recv_sem=R[f"rsem{l}"].at[slot, i],
                device_id=device(dx, dy),
                device_id_type=pl.DeviceIdType.MESH,
            )

    def send(l, slot, part):
        lev = levels[l]
        ys, run, nx = lev.ys, lev.run, lev.nx
        sx, sy, sd = (R[f"send{n}{l}"] for n in "xyd")
        tile = 3 * run
        order = list(copies(l, slot))
        lows, highs = [v[0:ys] for v in part], [v[ys : 2 * ys] for v in part]
        for c in range(3):
            low, high = lows[c], highs[c]
            sx[0, c * run : (c + 1) * run] = part[c][lev.base : lev.base + run]
            sx[1, c * run : (c + 1) * run] = part[c][2 * ys : 2 * ys + run]
            sx[0, tile + c : tile + c + 1] = low[0:1]
            sx[0, tile + 3 + c : tile + 4 + c] = high[0:1]
            sx[1, tile + c : tile + c + 1] = low[nx : nx + 1]
            sx[1, tile + 3 + c : tile + 4 + c] = high[nx : nx + 1]
        for dx, dy, copy in order[0:2]:
            pl.when(reach(dx, dy))(copy.start)
        for c in range(3):
            low, high = lows[c], highs[c]
            sd[0, c : c + 1] = low[0:1]
            sd[1, c : c + 1] = high[0:1]
            sd[2, c : c + 1] = low[nx : nx + 1]
            sd[3, c : c + 1] = high[nx : nx + 1]
        for dx, dy, copy in order[4:8]:
            pl.when(reach(dx, dy))(copy.start)
        for c in range(3):
            sy[0, c * ys : (c + 1) * ys] = lows[c]
            sy[1, c * ys : (c + 1) * ys] = highs[c]
        for dx, dy, copy in order[2:4]:
            pl.when(reach(dx, dy))(copy.start)

    def arrive(l, slot):
        lev = levels[l]
        ys, run, nx = lev.ys, lev.run, lev.nx
        for dx, dy, copy in copies(l, slot):
            pl.when(reach(-dx, -dy))(copy.wait_recv)
            pl.when(reach(dx, dy))(copy.wait_send)
        rx, ry, rd = (R[f"recv{n}{l}"] for n in "xyd")
        tile = pl.ds(3 * run, 8)
        left, right = rx[slot, 1, tile, :], rx[slot, 0, tile, :]
        at = lax.broadcasted_iota(jnp.int32, (ys, lev.lanes), 0)
        out = []
        for c in range(3):
            pieces = []
            for k, src in ((0, 1), (1, 0)):
                val = ry[slot, src, c * ys : (c + 1) * ys, :]
                row = slice(3 * k + c, 3 * k + c + 1)
                low = left[row] + rd[slot, 3 - k, c : c + 1, :]
                high = right[row] + rd[slot, 1 - k, c : c + 1, :]
                val = val + jnp.where(at == 0, low, 0.0) + jnp.where(at == nx, high, 0.0)
                pieces.append(val)
            pieces.append(rx[slot, 0, c * run : (c + 1) * run, :])
            pieces.append(rx[slot, 1, c * run : (c + 1) * run, :])
            out.append(jnp.concatenate(pieces, axis=0))
        return out

    def wide_copies(kind):
        index = 0
        for dx, dy, start, size, at, nodes in wide.sends:
            if dx == 0 and dy == 0:
                continue
            count = up(len(nodes), 8) if kind == "s" else size
            yield dx, dy, pltpu.make_async_remote_copy(
                src_ref=R[f"pack{kind}"].at[pl.ds(start, count)],
                dst_ref=R[f"get{kind}"].at[pl.ds(at, count)],
                send_sem=R[f"wsend{kind}"].at[index],
                recv_sem=R[f"wrecv{kind}"].at[index],
                device_id=device(dx, dy),
                device_id_type=pl.DeviceIdType.MESH,
            )
            index += 1

    def wide_send(kind, value):
        R[f"pack{kind}"][...] = value
        for dx, dy, start, size, at, nodes in wide.sends:
            if dx == 0 and dy == 0:
                R[f"get{kind}"][at : at + size] = value[start : start + size]
        for dx, dy, copy in wide_copies(kind):
            pl.when(reach(dx, dy))(copy.start)

    def wide_wait(kind):
        for dx, dy, copy in wide_copies(kind):
            pl.when(reach(-dx, -dy))(copy.wait_recv)
            pl.when(reach(dx, dy))(copy.wait_send)

    def thirds(value):
        parts = []
        for _ in range(3):
            parts.append(value.astype(BF16))
            value = value - parts[-1].astype(F32)
        return parts

    def wide_scale_send():
        sel = R["gs"][...]
        picked = [mm(sel, part).astype(BF16) for part in thirds(s0[...])]
        wide_send("s", sum(mm(part, R["sz"][...]) for part in picked))

    def wide_scale_take():
        wide_wait("s")
        place = R["place"][0 : wide.rows]
        R[f"s{len(levels) - 1}"][...] = sum(mm(place, part) for part in thirds(R["gets"][...]))
        prepare(len(levels) - 1, 0, wide.rows)

    def set_u(l, c, a, b, value):
        lev = levels[l]
        hi, lo = halves(value)
        at = c * lev.kb + a
        R[f"u{l}"][at : at + b - a] = hi
        R[f"u{l}"][at + lev.kp : at + lev.kp + b - a] = hi
        R[f"u{l}"][at + 2 * lev.kp : at + 2 * lev.kp + b - a] = lo
        if lev.split and a < lev.nb:
            n = min(b, lev.nb) - a
            for i, half in enumerate((hi, hi, lo)):
                at = 256 * c + i * lev.nb + a
                R[f"ub{l}"][at : at + n] = half[0:n]

    def span(l, blk):
        lev = levels[l]
        return (0, lev.nb) if blk == "b" else (lev.nb, lev.rows)

    def prepare(l, a, b):
        s = R[f"s{l}"][a:b]
        f = jnp.where(s == 0.0, 1.0, 0.0)
        R[f"f{l}"][a:b] = f
        square = s * s
        m_z, k_z = R[f"kl{l}"][0:1, :], R[f"kl{l}"][1:2, :]
        for c in range(3):
            kd = R[f"kr{l}"][a:b, c : c + 1] * m_z + R[f"kr{l}"][a:b, 3 + c : 4 + c] * k_z
            R[f"dinv{l}"][c, a:b] = 1.0 / (square * kd + f)

    def begin(l, a, b, source):
        scale = R["coef"][l, 12]
        s = R[f"s{l}"][a:b]
        for c in range(3):
            first = scale * (R[f"dinv{l}"][c, a:b] * source[c])
            R[f"r{l}"][c, a:b] = source[c]
            R[f"d{l}"][c, a:b] = first
            R[f"x{l}"][c, a:b] = first
            set_u(l, c, a, b, s * first)

    def ahead(l):
        lev = levels[l]
        if lev.split:
            for c in range(3):
                u = R[f"u{l}"][c * lev.kb : (c + 1) * lev.kb]
                R[f"pre{l}"][c] = mm(R[f"wi{l}"][c], u)

    def plane_sums(l, blk, n):
        lev = levels[l]
        kb = lev.kb
        if blk == "b" and lev.split:
            q = [
                R[f"pre{l}"][c] + mm(R[f"wb{l}"][c], R[f"ub{l}"][256 * c : 256 * (c + 1)])
                for c in range(3)
            ]
            q = [[v[i * n : (i + 1) * n] for i in range(4)] for v in q]
            both = [q[0][i] + q[1][i] for i in range(3)]
            last, plain = q[2], [q[0][3], q[1][3], q[2][3]]
        else:
            u, w1, w2 = R[f"u{l}"], R[f"w1{blk}{l}"], R[f"w2{blk}{l}"]
            both = mm(w1[...], u[0 : 2 * kb])
            last = mm(w2[...], u[2 * kb : 3 * kb])
            both = [both[i * n : (i + 1) * n] for i in range(3)]
            last = [last[i * n : (i + 1) * n] for i in range(4)]
            mass = w2[3 * n : 4 * n]
            plain = [mm(mass, u[0:kb]), mm(mass, u[kb : 2 * kb]), last[3]]
        stretch = (2.0 * MU_SHEAR + LAMBDA_BULK) / MU_SHEAR
        plain[2] = stretch * plain[2]
        return [both[0], both[1], last[2]], plain, [last[0], last[1]], [both[2]]

    def local_sums(l, blk):
        lev = levels[l]
        a, b = span(l, blk)
        n = b - a

        def along(which, parts):
            z = R[f"z{l}"]
            if blk == "b" and lev.split:
                pairs = [halves(v) for v in parts]
                high = [v for v, _ in pairs]
                tall = jnp.concatenate(high + [v for _, v in pairs], axis=0)
                first = mm(tall, z[which, 0 : lev.lanes])
                m = len(parts) * n
                low = mm(jnp.concatenate(high, axis=0), z[which, 2 * lev.lanes : 3 * lev.lanes])
                return first[0:m] + first[m : 2 * m] + low
            return mm(jnp.concatenate([wide3(v) for v in parts], axis=0), z[which])

        mass, stiff, trans, mixed = plane_sums(l, blk, n)
        zm = along(M_, mass)
        zk = along(K_, stiff)
        zt = along(T_, trans)
        zg = along(G_, mixed)
        return [
            zm[0:n] + zk[0:n] + zt[0:n],
            zm[n : 2 * n] + zk[n : 2 * n] + zt[n : 2 * n],
            zm[2 * n : 3 * n] + zk[2 * n : 3 * n] + zg,
        ]

    def advance(l, k, a, b, sums):
        c1, c2 = R["coef"][l, 2 * k], R["coef"][l, 2 * k + 1]
        s, f = R[f"s{l}"][a:b], R[f"f{l}"][a:b]
        for c in range(3):
            d = R[f"d{l}"][c, a:b]
            res = R[f"r{l}"][c, a:b] - (s * sums[c] + f * d)
            new = c1 * d + c2 * (R[f"dinv{l}"][c, a:b] * res)
            R[f"r{l}"][c, a:b] = res
            R[f"d{l}"][c, a:b] = new
            R[f"x{l}"][c, a:b] += new
            set_u(l, c, a, b, s * new)

    def smooth(l, k, slot, beside=None):
        lev = levels[l]
        own, pend = R[f"own{l}"], R[f"pend{l}"]
        part = local_sums(l, "b")
        for c in range(3):
            part[c] = part[c] + pend[c]
            own[c] = part[c]
            pend[c] = jnp.zeros_like(pend[c])
        send(l, slot, part)
        inner = local_sums(l, "i")
        advance(l, k, lev.nb, lev.rows, inner)
        ahead(l)
        if beside is not None:
            beside()
        got = arrive(l, slot)
        advance(l, k, 0, lev.nb, [own[c] + got[c] for c in range(3)])

    def restrict(l):
        lev = levels[l]
        masked = []
        for blk in "bi":
            a, b = span(l, blk)
            sums = local_sums(l, blk)
            s, f = R[f"s{l}"][a:b], R[f"f{l}"][a:b]
            free = 1.0 - f
            if blk == "b":
                row = lax.broadcasted_iota(jnp.int32, (b - a, lev.lanes), 0)
                mine = jnp.logical_or(row < lev.nx, row >= lev.base)
                free = jnp.where(mine, free, 0.0)
            piece = []
            for c in range(3):
                r, d = R[f"r{l}"][c, a:b], R[f"d{l}"][c, a:b]
                piece.append(free * r - s * sums[c])
                if blk == "b":
                    R[f"pend{l}"][c] = sums[c]
                    R[f"r{l}"][c, a:b] = r - f * d
                else:
                    R[f"r{l}"][c, a:b] = r - (s * sums[c] + f * d)
            masked.append(piece)
        fields = [
            tall2(jnp.concatenate([masked[0][c], masked[1][c]], axis=0)) for c in range(3)
        ]
        if l + 1 == len(levels) - 1:
            n = wide.pack_rows
            flat = []
            for side in range(2):
                mat = R["gp"][side * n : (side + 1) * n]
                field = jnp.concatenate([fields[side], fields[2]], axis=0)
                flat.append(wide2(mm(mat, field)))
            return mm(jnp.concatenate(flat, axis=1), R["gz"][...])
        flat = [wide2(mm(R[f"dp{l}"][...], field)) for field in fields]
        down = mm(jnp.concatenate(flat, axis=0), R[f"dz{l}"][...])
        n = levels[l + 1].rows
        return [down[c * n : (c + 1) * n] for c in range(3)]

    def descend(l, slot, sums):
        lev = levels[l]
        own = R[f"own{l}"]
        for c in range(3):
            own[c] = sums[c][0 : lev.nb]
        send(l, slot, [sums[c][0 : lev.nb] for c in range(3)])
        free = 1.0 - R[f"f{l}"][lev.nb : lev.rows]
        begin(l, lev.nb, lev.rows, [free * sums[c][lev.nb : lev.rows] for c in range(3)])
        if l + 1 == len(levels) - 1:
            wide_scale_take()
        got = arrive(l, slot)
        free = 1.0 - R[f"f{l}"][0 : lev.nb]
        begin(l, 0, lev.nb, [free * (own[c] + got[c]) for c in range(3)])

    def solve_wide(packed):
        l, n, half = len(levels) - 1, wide.rows, wide.half
        wide_send("b", packed)
        wide_wait("b")
        hi, lo = halves(R["getb"][...])
        spread = mm(R["place"][...], hi) + mm(R["place"][...], lo)
        lane = lax.broadcasted_iota(jnp.int32, (n, wide.lanes), 1)
        keep = jnp.where(lane < half, 1.0 - R[f"f{l}"][...], 0.0)
        both, one, two = (spread[i * n : (i + 1) * n] for i in range(3))
        right = [both, pltpu.roll(both, half, 1), one + pltpu.roll(two, half, 1)]
        begin(l, 0, n, [keep * v for v in right])

        def body(k, _):
            advance(l, k, 0, n, local_sums(l, "i"))
            return 0

        lax.fori_loop(0, COARSE_DEG - 1, body, 0)

    def ascend(l):
        lev, n = levels[l], levels[l + 1].rows
        field = jnp.concatenate([wide2(R[f"x{l + 1}"][c]) for c in range(3)], axis=0)
        fine = mm(field, R[f"uz{l}"][...])
        free, s = 1.0 - R[f"f{l}"][...], R[f"s{l}"][...]
        for c in range(3):
            step = free * mm(R[f"up{l}"][...], tall2(fine[c * n : (c + 1) * n]))
            R[f"d{l}"][c] = step
            R[f"x{l}"][c] += step
            set_u(l, c, 0, lev.rows, s * step)
        ahead(l)

    def build(l):
        lev = levels[l]
        lines = []
        for axis in "xy":
            tall = mm(R[f"e{axis}{l}"][...], R[f"t{axis}{l}"][...])
            lines.append(
                [
                    mm(tall[:, 128 * i : 128 * (i + 1)].astype(BF16), R[f"c{axis}{l}"][...])
                    for i in range(4)
                ]
            )
        X, Y = lines
        cc = LAMBDA_BULK + MU_SHEAR
        big = MU_SHEAR + cc
        kxmy, mxky = X[K_] * Y[M_], X[M_] * Y[K_]
        first = (
            (0, 0, big * kxmy + MU_SHEAR * mxky),
            (0, 1, cc * (X[G_] * Y[T_])),
            (1, 0, cc * (X[T_] * Y[G_])),
            (1, 1, MU_SHEAR * kxmy + big * mxky),
            (2, 0, cc * (X[T_] * Y[M_])),
            (2, 1, cc * (X[M_] * Y[T_])),
        )
        second = (
            cc * (X[G_] * Y[M_]),
            cc * (X[M_] * Y[G_]),
            MU_SHEAR * (kxmy + mxky),
            X[M_] * Y[M_],
        )
        lane = lax.broadcasted_iota(jnp.int32, (lev.rows, lev.seg), 1)
        middle = jnp.logical_and(lane >= lev.kp, lane < 2 * lev.kp)

        def store(kind, group, at, value):
            hi, lo = halves(value)
            for blk in "bi" if lev.nb and not lev.split else "i":
                a, b = span(l, blk)
                ref, row = R[f"{kind}{blk}{l}"], group * (b - a)
                row = slice(row, row + b - a)
                if lev.packed:
                    mixed = jnp.where(middle, lo.astype(F32), hi.astype(F32)).astype(BF16)
                    ref[row, at : at + 256] = mixed[a:b]
                else:
                    for s, half in enumerate((hi, lo, hi)):
                        start = at + s * lev.kp
                        ref[row, start : start + lev.kp] = half[a:b]

        for group, side, value in first:
            store("w1", group, side * lev.kb, value)
        for group, value in enumerate(second):
            store("w2", group, 0, value)
        if lev.split:
            n, kp = lev.nb, lev.kp
            lane = lax.broadcasted_iota(jnp.int32, (n, kp), 1)
            parts = [(side, group, value) for group, side, value in first]
            parts += [(2, group, value) for group, value in enumerate(second)]
            parts += [(0, 3, second[3]), (1, 3, second[3])]
            for side, group, value in parts:
                hi, lo = (v.astype(F32) for v in halves(value[0:n]))
                rows = slice(group * n, (group + 1) * n)
                inner = [jnp.where(lane >= n, v, 0.0).astype(BF16) for v in (hi, lo)]
                for i, half in enumerate((inner[0], inner[1], inner[0])):
                    R[f"wi{l}"][side, rows, i * kp : (i + 1) * kp] = half
                hi, lo = (jnp.where(lane < n, v, 0.0) for v in (hi, lo))
                mixed = hi + pltpu.roll(lo, n, 1) + pltpu.roll(hi, 2 * n, 1)
                R[f"wb{l}"][side, rows] = mixed.astype(BF16)

    build(0)

    def clear_spare(a, b):
        lead = lax.broadcasted_iota(jnp.int32, (b - a, top.lanes), 0) % top.run == 0
        s0[a:b] = jnp.where(lead, 0.0, s0[a:b])

    clear_spare(top.nb, top.rows)
    prepare(0, top.nb, top.rows)
    begin(0, top.nb, top.rows, [R["r0"][c, top.nb : top.rows] for c in range(3)])
    ahead(0)
    for dx, dy, copy in first_copies():
        pl.when(reach(dx, dy))(copy.wait_send)
        pl.when(reach(-dx, -dy))(copy.wait_recv)
    clear_spare(top.base, top.nb)
    ys, run, nx = top.ys, top.run, top.nx
    at = lax.broadcasted_iota(jnp.int32, (ys, top.lanes), 0)
    for c in range(4):
        dst = s0 if c == 3 else R["r0"].at[c]
        low = jnp.where(at == nx, R["gotx"][c, 0:1, :], put[c])
        high = jnp.where(at == nx, R["gotd"][c : c + 1, :], R["goty"][c])
        dst[0:ys] = low
        dst[ys : 2 * ys] = high
        side = R["gotx"][c]
        if c == 3:
            row = lax.broadcasted_iota(jnp.int32, (run, top.lanes), 0)
            side = jnp.where(row == 0, 0.0, side)
        dst[2 * ys : 2 * ys + run] = side
    prepare(0, 0, top.nb)
    begin(0, 0, top.nb, [R["r0"][c, 0 : top.nb] for c in range(3)])

    def coarse_setup():
        parts = thirds(s0[...])
        build(len(levels) - 1)
        for l in range(1, len(levels) - 1):
            sel_x, sel_z = R[f"sx{l}"][...], R[f"sz{l}"][...]
            picked = [mm(sel_x, part).astype(BF16) for part in parts]
            R[f"s{l}"][...] = sum(mm(part, sel_z) for part in picked)
            prepare(l, 0, levels[l].rows)
            build(l)

    def pre(k, _):
        smooth(0, k, k % 2, lambda: pl.when(k == 0)(coarse_setup))
        return 0

    def cycle(l):
        skip = 0 if l == 0 else 1

        def body(k, _):
            smooth(l, k, (k + skip) % 2)
            return 0

        def tail(k, _):
            smooth(l, k, (k + skip + 1) % 2)
            return 0

        lax.fori_loop(0, DEG - 1, pre if l == 0 else body, 0)
        if l == 0:
            wide_scale_send()
        if l + 1 == len(levels) - 1:
            solve_wide(restrict(l))
        else:
            descend(l + 1, 0, restrict(l))
            cycle(l + 1)
        ascend(l)
        lax.fori_loop(DEG, 2 * DEG, tail, 0)

    cycle(0)
    for c in range(3):
        for x in range(nx):
            row = top.base + x * run
            R["x0"][c, row : row + 1, :] = R["x0"][c, x : x + 1, :]
    for v in range(vecs):
        R["out"][v] = R["x0"][:, top.base : top.base + nx * run, v * nz : (v + 1) * nz]


def chebyshev_table(spectrum, coef):
    for l in range(3):
        low, top = spectrum[0, l], spectrum[1, l]
        center = 0.5 * (top + low)
        radius = 0.5 * (top - low)
        ratio = center / radius
        rho = 1.0 / ratio
        steps = []
        for _ in range(COARSE_DEG - 1):
            rho_next = 1.0 / (2.0 * ratio - rho)
            steps.append((rho_next * rho, 2.0 * rho_next / radius))
            rho = rho_next
        smooth = steps[: DEG - 1]
        flat = [(0.0, 0.0), (0.0, 1.0 / center)]
        picked = steps if l == 2 else smooth + flat + smooth
        for k, two in enumerate(picked):
            coef[l, 2 * k] = jnp.asarray(two[0], F32)
            coef[l, 2 * k + 1] = jnp.asarray(two[1], F32)
        coef[l, 12] = 1.0 / center


def local(modes, moduli, pinned, spectrum):
    vecs, _, nx, ny, nz = modes.shape
    levels = []
    names, args = [], []

    def add(name, value):
        names.append(name)
        args.append(value)

    for degree in DEGREES:
        step = DEGREES[0] // degree
        size = (degree, nx // step, ny // step, nz // step, vecs)
        levels.append(Level(*size) if step < DEGREES[0] else Wide(*size, COARSE_DEG - 1))
    top = levels[0]
    assert ny == top.run and nz % 128 == 0
    add("spectrum_in", spectrum.T)
    add("modes", modes.reshape(vecs, 3, nx * ny, nz))
    add("moduli_in", moduli.reshape(nx * ny, nz))
    add("pinned_in", pinned.reshape(nx * ny, nz))
    for l, lev in enumerate(levels):
        for axis, mats in zip("xy", lev.factors()):
            for key, mat in zip("etc", mats):
                add(f"{key}{axis}{l}_in", jnp.asarray(mat))
        add(f"z{l}_in", jnp.asarray(lev.lines()))
        for key, mat in zip(("kr", "kl"), lev.diagonal()):
            add(f"{key}{l}_in", jnp.asarray(mat))
        if l + 1 < len(levels):
            coarsest = l + 2 == len(levels)
            for key, mat in zip(("dp", "dz", "up", "uz"), transfer(lev, levels[l + 1])):
                if key[0] == "u" or not coarsest:
                    add(f"{key}{l}_in", jnp.asarray(mat))
        if 0 < l < len(levels) - 1:
            for key, mat in zip(("sx", "sz"), lev.sample(top)):
                add(f"{key}{l}_in", jnp.asarray(mat))
    wide = levels[-1]
    for key, mat in zip(("gp", "gs", "place", "gz"), wide.gather(levels[-2], top)):
        add(f"{key}_in", jnp.asarray(mat))
    add("sz_in", jnp.asarray(wide.sample(top)[1]))

    specs = [pl.BlockSpec(memory_space=pl.ANY) for n in names]
    scratch = []
    all_names = names + ["out"]

    def temp(name, what):
        all_names.append(name)
        scratch.append(what)

    temp("coef", pltpu.SMEM((3, 13), F32))
    temp("lsem", pltpu.SemaphoreType.DMA((len(names) + 24,)))
    for name, value in zip(names, args):
        if name == "spectrum_in":
            temp("spectrum", pltpu.SMEM(value.shape, F32))
        elif name.endswith("_in"):
            shape = value.shape
            if name[0] == "z":
                lanes = levels[int(name[1])].lanes
                shape = (4, 3 * lanes, lanes)
            elif name[0] == "t":
                shape = shape[1:]
            temp(name[:-3], pltpu.VMEM(shape, value.dtype))
    for l, lev in enumerate(levels):
        field = (3, lev.rows, lev.lanes)
        for n in ("s", "f"):
            temp(f"{n}{l}", pltpu.VMEM(field[1:], F32))
        for n in ("r", "d", "x", "dinv"):
            temp(f"{n}{l}", pltpu.VMEM(field, F32))
        temp(f"u{l}", pltpu.VMEM((3 * lev.kb, lev.lanes), BF16))
        for blk, n in (("b", lev.nb), ("i", lev.rows - lev.nb)):
            if n and not (blk == "b" and lev.split):
                temp(f"w1{blk}{l}", pltpu.VMEM((3 * n, 2 * lev.kb), BF16))
                temp(f"w2{blk}{l}", pltpu.VMEM((4 * n, lev.kb), BF16))
        if lev.split:
            temp(f"ub{l}", pltpu.VMEM((3 * 256, lev.lanes), BF16))
            temp(f"pre{l}", pltpu.VMEM((3, 4 * lev.nb, lev.lanes), F32))
            temp(f"wi{l}", pltpu.VMEM((3, 4 * lev.nb, lev.kb), BF16))
            temp(f"wb{l}", pltpu.VMEM((3, 4 * lev.nb, 256), BF16))
        if lev is wide:
            continue
        for n in ("own", "pend"):
            temp(f"{n}{l}", pltpu.VMEM((3, lev.nb, lev.lanes), F32))
        for n, shape in (
            ("x", (2, 3 * lev.run + 8, lev.lanes)),
            ("y", (2, 3 * lev.ys, lev.lanes)),
            ("d", (4, 8, lev.lanes)),
        ):
            temp(f"send{n}{l}", pltpu.VMEM(shape, F32))
            temp(f"recv{n}{l}", pltpu.VMEM((2,) + shape, F32))
        temp(f"ssem{l}", pltpu.SemaphoreType.DMA((len(DIRS),)))
        temp(f"rsem{l}", pltpu.SemaphoreType.DMA((2, len(DIRS))))
    for kind in "sb":
        temp(f"pack{kind}", pltpu.VMEM((wide.pack_rows, wide.lanes), F32))
        temp(f"get{kind}", pltpu.VMEM((wide.got_rows, wide.lanes), F32))
        temp(f"wsend{kind}", pltpu.SemaphoreType.DMA((len(wide.sends) - 1,)))
        temp(f"wrecv{kind}", pltpu.SemaphoreType.DMA((len(wide.sends) - 1,)))
    temp("put", pltpu.VMEM((4, top.ys, top.lanes), F32))
    temp("putd", pltpu.VMEM((8, top.lanes), F32))
    temp("gotx", pltpu.VMEM((4, top.run, top.lanes), F32))
    temp("goty", pltpu.VMEM((4, top.ys, top.lanes), F32))
    temp("gotd", pltpu.VMEM((8, top.lanes), F32))
    temp("fsend", pltpu.SemaphoreType.DMA((4,)))
    temp("frecv", pltpu.SemaphoreType.DMA((4,)))
    out = pl.pallas_call(
        functools.partial(kernel, levels, all_names),
        out_shape=pltpu.VMEM((vecs, 3, nx * ny, nz), F32),
        in_specs=specs,
        out_specs=pl.BlockSpec(memory_space=pltpu.VMEM),
        scratch_shapes=scratch,
        compiler_params=pltpu.CompilerParams(
            collective_id=0, has_side_effects=True, vmem_limit_bytes=62 * 1024 * 1024
        ),
    )(*args)
    return out.reshape(modes.shape)


def solution(mesh):
    placed = (P(None, None, "gx", "gy", None), P("gx", "gy", None), P("gx", "gy", None), P())
    return jax.shard_map(
        local,
        mesh=mesh,
        in_specs=placed,
        out_specs=P(None, None, "gx", "gy", None),
        check_vma=False,
    )
```

```python
import functools

import jax
import jax.numpy as jnp
import numpy as np
from jax import lax
from jax.experimental import pallas as pl
from jax.experimental.pallas import tpu as pltpu
from jax.sharding import PartitionSpec as P

DEG = 3
COARSE_DEG = 4
DEGREES = (4, 2, 1)
MU_SHEAR = 1.0
LAMBDA_BULK = 1.5
PROLONG_TABLES = {
    4: np.array(
        [[1.0, 0.0, 0.0], [0.375, 0.75, -0.125], [0.0, 1.0, 0.0], [-0.125, 0.75, 0.375]]
    ),
    2: np.array([[1.0, 0.0], [0.5, 0.5]]),
}
DIRS = ((-1, 0), (1, 0), (0, -1), (0, 1), (-1, -1), (-1, 1), (1, -1), (1, 1))
F32 = jnp.float32
BF16 = jnp.bfloat16
M_, K_, G_, T_ = range(4)


def element_matrices(degree):
    nodes = [float(place) / degree for place in range(degree + 1)]
    gauss_x, gauss_w = np.polynomial.legendre.leggauss(8)
    points = 0.5 * (gauss_x + 1.0)
    weights = 0.5 * gauss_w
    values = np.zeros((degree + 1, points.size))
    slopes = np.zeros((degree + 1, points.size))
    for column in range(degree + 1):
        product = np.ones(points.size)
        for other in range(degree + 1):
            if other != column:
                product = product * (points - nodes[other]) / (nodes[column] - nodes[other])
        values[column] = product
        for skipped in range(degree + 1):
            if skipped != column:
                part = np.ones(points.size) / (nodes[column] - nodes[skipped])
                for other in range(degree + 1):
                    if other != column and other != skipped:
                        part = part * (points - nodes[other]) / (nodes[column] - nodes[other])
                slopes[column] += part
    mass = (values * weights) @ values.T
    stiff = (slopes * weights) @ slopes.T
    mixed = (slopes * weights) @ values.T
    return [mass, stiff, mixed, mixed.T]


def assembled(element, count, ghost):
    p = element.shape[0] - 1
    out = np.zeros((count + 1, count + 1))
    for e in range(count // p):
        out[e * p : e * p + p + 1, e * p : e * p + p + 1] += element
    if ghost:
        out[0, 0] += element[p, p]
    return out


def up(n, m):
    return -(-n // m) * m


def bf16_parts(mat, count):
    rest = np.asarray(mat, np.float64)
    parts = []
    for _ in range(count):
        part = rest.astype(np.float32).astype(BF16)
        parts.append(part)
        rest = rest - part.astype(np.float64)
    return parts


def exact_bf16(mat):
    out = np.asarray(mat, np.float32).astype(BF16)
    assert np.array_equal(out.astype(np.float64), mat)
    return out


class Level:
    def __init__(self, degree, nx, ny, nz, vecs):
        self.p, self.nx, self.ny, self.nz, self.vecs = degree, nx, ny, nz, vecs
        self.ys = up(nx + 1, 8)
        self.run = up(ny, 8)
        self.base = 2 * self.ys + self.run
        self.rows = up(self.base + nx * self.run, 16)
        self.nb = self.base + self.run
        assert self.nb % 16 == 0
        self.lanes = up(vecs * nz, 128)
        self.low = 0
        self.where = {(x, y): self.row(x, y) for x in range(nx + 1) for y in range(ny + 1)}
        self.spans = (nx, ny)
        self.columns()

    def columns(self):
        if 3 * self.rows <= 256:
            self.kp, self.kb = self.rows, 256
        else:
            self.kp = up(self.rows, 128)
            self.kb = 3 * self.kp
        self.packed = self.kb == 256
        self.split = not self.packed and 0 < 3 * self.nb <= 256 == self.kp
        self.seg = 256 if self.packed else self.kp

    def row(self, x, y):
        if y == 0:
            return x
        if y == self.ny:
            return self.ys + x
        if x == self.nx:
            return 2 * self.ys + y
        return self.base + self.run * x + y

    def factors(self):
        out = []
        for axis, n in enumerate(self.spans):
            expand = np.zeros((self.rows, 32))
            spread = np.zeros((128, self.seg))
            for at, row in self.where.items():
                expand[row, at[axis] + self.low] = 1
                for copy in range(3 if self.packed else 1):
                    for part in range(3):
                        spread[32 * part + at[axis] + self.low, copy * self.kp + row] = 1
            table = np.zeros((2, 32, 512), BF16)
            for ghost in range(2):
                for i, element in enumerate(element_matrices(self.p)):
                    parts = bf16_parts(assembled(element, n, ghost), 3)
                    for part, mat in enumerate(parts):
                        at = 128 * i + 32 * part
                        table[ghost, : n + 1, at : at + n + 1] = mat
            out.append((exact_bf16(expand), table, exact_bf16(spread)))
        return out

    def lines(self):
        p, n = self.p, self.nz
        mats = []
        for e in element_matrices(p):
            full = assembled(e, n, True)[:n, :n].T
            if n % 128:
                lifted = np.zeros((self.lanes, self.lanes))
                size = self.vecs * n
                lifted[:size, :size] = np.kron(np.eye(self.vecs), full)
                full = lifted
            mats.append(np.stack(bf16_parts(full, 2)))
        return np.stack(mats)

    def diagonal(self):
        def center(which, count):
            p = self.p
            e = element_matrices(p)[which]
            line = np.array([e[a, a] + (e[p, p] if a == 0 else 0.0) for a in range(p)])
            return line[np.arange(count) % p]

        rows = np.zeros((self.rows, 128), np.float32)
        m_x, m_y, m_z = [center(0, n) for n in (self.nx + self.p, self.ny + self.p, self.nz)]
        k_x, k_y, k_z = [center(1, n) for n in (self.nx + self.p, self.ny + self.p, self.nz)]
        for c in range(3):
            coef = [MU_SHEAR + (LAMBDA_BULK + MU_SHEAR) * (c == e) for e in range(3)]
            for (x, y), row in self.where.items():
                x, y = x % self.p, y % self.p
                rows[row, c] = coef[0] * k_x[x] * m_y[y] + coef[1] * m_x[x] * k_y[y]
                rows[row, 3 + c] = coef[2] * m_x[x] * m_y[y]
        lanes = np.zeros((8, self.lanes), np.float32)
        lanes[0, : self.vecs * self.nz] = np.tile(m_z, self.vecs)
        lanes[1, : self.vecs * self.nz] = np.tile(k_z, self.vecs)
        return rows, lanes

    def sample(self, top):
        step = top.p // self.p
        sel_x = np.zeros((self.rows, top.rows))
        for (x, y), row in self.where.items():
            if (x * step, y * step) in top.where:
                sel_x[row, top.where[x * step, y * step]] = 1
        sel_z = np.zeros((top.lanes, self.lanes))
        for v in range(self.vecs):
            for z in range(self.nz):
                sel_z[v * top.nz + z * step, v * self.nz + z] = 1
        return exact_bf16(sel_x), exact_bf16(sel_z)


class Wide(Level):
    def __init__(self, degree, nx, ny, nz, vecs, ring):
        self.p, self.nx, self.ny, self.nz, self.vecs = degree, nx, ny, nz, vecs
        self.low = ring * degree
        self.spans = (nx + 2 * self.low, ny + 2 * self.low)
        self.lanes = up(vecs * nz, 128)
        self.half = self.lanes // 2
        assert vecs * nz <= self.half
        spots = [
            (max(-x, x - nx, -y, y - ny, 0), x, y)
            for x in range(-self.low, nx + self.low + 1)
            for y in range(-self.low, ny + self.low + 1)
        ]
        self.where = {(x, y): row for row, (_, x, y) in enumerate(sorted(spots))}
        self.rows = up(len(self.where), 16)
        self.needed = [
            up(sum(away <= (ring - 1 - k) * degree for away, _, _ in spots), 16)
            for k in range(ring)
        ]
        self.nb = 0
        self.columns()
        self.plan()

    def plan(self):
        nx, ny, low = self.nx, self.ny, self.low
        closed = [(x, y) for x in range(nx + 1) for y in range(ny + 1)]
        far = [-(-(low + 1) // n) for n in (nx, ny)]
        self.far = far
        self.sections, self.sends = [], []
        self.pack_rows = 0
        at = 0
        kinds = {}
        for dx in range(-far[0], far[0] + 1):
            for dy in range(-far[1], far[1] + 1):
                nodes = tuple(
                    (x, y) for x, y in closed if (x - dx * nx, y - dy * ny) in self.where
                )
                if abs(dx) <= 1 and abs(dy) <= 1:
                    nodes = tuple(closed)
                if not nodes:
                    continue
                if nodes not in kinds:
                    k = len(nodes)
                    size = up(k + -(-k // 2), 8)
                    kinds[nodes] = (self.pack_rows, size)
                    self.sections.append((self.pack_rows, size, nodes))
                    self.pack_rows += size
                start, size = kinds[nodes]
                self.sends.append((dx, dy, start, size, at, nodes))
                at += size
        self.pack_rows = up(self.pack_rows, 16)
        self.got_rows = up(at, 16)

    def gather(self, fine, top):
        table = PROLONG_TABLES[fine.p]
        px, py = interpolation(table, fine.nx), interpolation(table, fine.ny)
        plane = {
            (cx, cy): np.array(
                [
                    [px[x, cx] * py[y, cy], row]
                    for (x, y), row in fine.where.items()
                    if px[x, cx] * py[y, cy] != 0.0
                ]
            )
            for cx in range(self.nx + 1)
            for cy in range(self.ny + 1)
        }
        pack = np.zeros((2, self.pack_rows, 4 * fine.rows))
        scale = np.zeros((self.pack_rows, top.rows))
        step = top.p // self.p
        for start, size, nodes in self.sections:
            k = len(nodes)
            h = -(-k // 2)
            for i, node in enumerate(nodes):
                for weight, row in plane[node]:
                    row = int(row)
                    for side in range(2):
                        pack[side, start + i, row] = weight
                        pack[side, start + i, fine.rows + row] = weight
                    side = i // h
                    pack[side, start + k + i % h, 2 * fine.rows + row] = weight
                    pack[side, start + k + i % h, 3 * fine.rows + row] = weight
                if node[0] < self.nx and node[1] < self.ny:
                    scale[start + i, top.where[node[0] * step, node[1] * step]] = 1
        place = np.zeros((3, self.rows, self.got_rows))
        for dx, dy, start, size, at, nodes in self.sends:
            k = len(nodes)
            h = -(-k // 2)
            for i, (x, y) in enumerate(nodes):
                to = self.where.get((x - dx * self.nx, y - dy * self.ny))
                if to is not None:
                    place[0, to, at + i] = 1
                    place[1 + i // h, to, at + k + i % h] = 1
        down = interpolation(table, fine.nz)[: fine.nz, : self.nz]
        line = np.zeros((2, 2 * fine.lanes, self.lanes))
        size = (self.vecs * fine.nz, self.vecs * self.nz)
        for side in range(2):
            for copy in range(2):
                line[
                    side,
                    copy * fine.lanes : copy * fine.lanes + size[0],
                    side * self.half : side * self.half + size[1],
                ] = np.kron(np.eye(self.vecs), down)
        mats = (
            pack.reshape(2 * self.pack_rows, 4 * fine.rows),
            scale,
            place.reshape(3 * self.rows, self.got_rows),
            line.reshape(4 * fine.lanes, self.lanes),
        )
        return [exact_bf16(m) for m in mats]


def interpolation(table, count):
    q = table.shape[0]
    half = q // 2
    out = np.zeros((count + 1, count // 2 + 1))
    for i in range(count + 1):
        for t in range(half + 1):
            j = half * (i // q) + t
            if table[i % q, t] != 0.0:
                out[i, j] += table[i % q, t]
    return out


def transfer(fine, coarse):
    table = PROLONG_TABLES[fine.p]
    px, py = interpolation(table, fine.nx), interpolation(table, fine.ny)
    pz = interpolation(table, fine.nz)[: fine.nz, : coarse.nz]
    plane = np.zeros((fine.rows, coarse.rows))
    for (x, y), row in fine.where.items():
        for (cx, cy), col in coarse.where.items():
            if 0 <= cx <= coarse.nx and 0 <= cy <= coarse.ny:
                plane[row, col] = px[x, cx] * py[y, cy]
    line = np.zeros((coarse.lanes, fine.lanes))
    size = (fine.vecs * coarse.nz, fine.vecs * fine.nz)
    line[: size[0], : size[1]] = np.kron(np.eye(fine.vecs), pz.T)
    down = (np.tile(plane.T, (1, 2)), np.tile(line.T, (2, 1)))
    upward = (np.tile(plane, (1, 2)), np.tile(line, (2, 1)))
    return [exact_bf16(m) for m in down + upward]


def halves(value):
    hi = value.astype(BF16)
    return hi, (value - hi.astype(F32)).astype(BF16)


def mm(a, b):
    return lax.dot_general(a, b, (((1,), (0,)), ((), ())), preferred_element_type=F32)


def wide3(value):
    hi, lo = halves(value)
    return jnp.concatenate([hi, lo, hi], axis=1)


def wide2(value):
    hi, lo = halves(value)
    return jnp.concatenate([hi, lo], axis=1)


def tall2(value):
    hi, lo = halves(value)
    return jnp.concatenate([hi, lo], axis=0)


def kernel(levels, names, *refs):
    R = dict(zip(names, refs))
    gx_n, gy_n = lax.axis_size("gx"), lax.axis_size("gy")
    me_x, me_y = lax.axis_index("gx"), lax.axis_index("gy")

    def reach(dx, dy):
        ok = None
        for d, me, n in ((dx, me_x, gx_n), (dy, me_y, gy_n)):
            if d:
                here = me + d < n if d > 0 else me + d >= 0
                ok = here if ok is None else jnp.logical_and(ok, here)
        return ok

    def device(dx, dy):
        return (jnp.clip(me_x + dx, 0, gx_n - 1), jnp.clip(me_y + dy, 0, gy_n - 1))

    top = levels[0]
    vecs, nz = top.vecs, top.nz
    body_rows = pl.ds(top.base, top.nx * top.run)

    moves = []

    def load(src, dst):
        moves.append(pltpu.make_async_copy(src, dst, R["lsem"].at[len(moves)]))
        moves[-1].start()

    load(R["moduli_in"], R["moduli"])
    load(R["pinned_in"], R["pinned"])
    load(R["spectrum_in"], R["spectrum"])
    for v in range(vecs):
        load(R["modes"].at[v], R["r0"].at[:, body_rows, pl.ds(v * nz, nz)])
    first_moves = len(moves)
    for l, lev in enumerate(levels):
        if lev.nz % 128 == 0:
            R[f"z{l}"][...] = jnp.zeros_like(R[f"z{l}"])
        load(R[f"tx{l}_in"].at[jnp.where(me_x == 0, 1, 0)], R[f"tx{l}"])
        load(R[f"ty{l}_in"].at[jnp.where(me_y == 0, 1, 0)], R[f"ty{l}"])
    for name in names:
        if name.endswith("_in") and name[:2] not in ("mo", "pi", "sp", "tx", "ty"):
            if name[0] == "z":
                lev = levels[int(name[1])]
                src, dst = R[name], R[name[:-3]]
                size = lev.nz if lev.nz % 128 == 0 else lev.lanes
                for s, half in enumerate((0, 0, 1)):
                    for at in range(0, lev.lanes, size):
                        load(
                            src.at[:, half],
                            dst.at[:, pl.ds(s * lev.lanes + at, size), pl.ds(at, size)],
                        )
            else:
                load(R[name], R[name[:-3]])

    wide = levels[-1]
    edged = range(len(levels) - 1)

    def clear(name):
        R[name][...] = jnp.zeros_like(R[name])

    for l in edged:
        for n in "xyd":
            clear(f"recv{n}{l}")
    for n in ("gotx", "goty", "gotd", "gets", "getb"):
        clear(n)

    barrier = pltpu.get_barrier_semaphore()
    peers = [(dx, dy) for dx, dy, *_ in wide.sends if dx or dy]
    assert set(DIRS) <= set(peers)
    for dx, dy in peers:

        @pl.when(reach(dx, dy))
        def _():
            pl.semaphore_signal(
                barrier, inc=1, device_id=device(dx, dy), device_id_type=pl.DeviceIdType.MESH
            )

    for l in edged:
        for n in "xyd":
            clear(f"send{n}{l}")
        clear(f"pend{l}")
    for l in range(len(levels)):
        clear(f"u{l}")
        if levels[l].split:
            clear(f"ub{l}")

    for one in moves[:first_moves]:
        one.wait()
    chebyshev_table(R["spectrum"], R["coef"])
    scale = R["moduli"][...] * (1.0 - R["pinned"][...].astype(F32))
    s0 = R["s0"]
    s0[0 : top.base] = jnp.zeros((top.base, top.lanes), F32)
    for v in range(vecs):
        s0[body_rows, v * nz : (v + 1) * nz] = scale
    put = R["put"]
    put[...] = jnp.zeros_like(put)
    for c in range(3):
        for x in range(top.nx):
            at = top.base + x * top.run
            put[c, x : x + 1, :] = R["r0"][c, at : at + 1, :]
    for x in range(top.nx):
        at = top.base + x * top.run
        put[3, x : x + 1, :] = s0[at : at + 1, :]
    for c in range(4):
        R["putd"][c : c + 1, :] = put[c, 0:1, :]
    R["putd"][4:8, :] = jnp.zeros((4, top.lanes), F32)
    edge = pl.ds(top.base, top.run)

    def first_copies():
        plan = (
            (-1, 0, R["r0"].at[:, edge, :], R["gotx"].at[pl.ds(0, 3)]),
            (-1, 0, s0.at[edge, :], R["gotx"].at[3]),
            (0, -1, put, R["goty"]),
            (-1, -1, R["putd"], R["gotd"]),
        )
        for i, (dx, dy, src, dst) in enumerate(plan):
            yield dx, dy, pltpu.make_async_remote_copy(
                src_ref=src,
                dst_ref=dst,
                send_sem=R["fsend"].at[i],
                recv_sem=R["frecv"].at[i],
                device_id=device(dx, dy),
                device_id_type=pl.DeviceIdType.MESH,
            )

    around = []
    for me, n, far in ((me_x, gx_n, wide.far[0]), (me_y, gy_n, wide.far[1])):
        around.append(1 + jnp.minimum(me, far) + jnp.minimum(n - 1 - me, far))
    pl.semaphore_wait(barrier, around[0] * around[1] - 1)
    for dx, dy, copy in first_copies():
        pl.when(reach(dx, dy))(copy.start)
    for one in moves[first_moves:]:
        one.wait()

    def copies(l, slot):
        for i, (dx, dy) in enumerate(DIRS):
            kind, at = ("d", i - 4) if dx and dy else ("x", i) if dx else ("y", i - 2)
            src, dst = R[f"send{kind}{l}"].at[at], R[f"recv{kind}{l}"].at[slot, at]
            if kind == "d":
                src, dst = src.at[pl.ds(0, 3)], dst.at[pl.ds(0, 3)]
            yield dx, dy, pltpu.make_async_remote_copy(
                src_ref=src,
                dst_ref=dst,
                send_sem=R[f"ssem{l}"].at[i],
                recv_sem=R[f"rsem{l}"].at[slot, i],
                device_id=device(dx, dy),
                device_id_type=pl.DeviceIdType.MESH,
            )

    def send(l, slot, part, only=range(8)):
        lev = levels[l]
        ys, run, nx = lev.ys, lev.run, lev.nx
        sx, sy, sd = (R[f"send{n}{l}"] for n in "xyd")
        tile = 3 * run
        order = list(copies(l, slot))
        lows, highs = [v[0:ys] for v in part], [v[ys : 2 * ys] for v in part]
        def launch(which):
            for i in which:
                if i in only:
                    dx, dy, copy = order[i]
                    pl.when(reach(dx, dy))(copy.start)

        for i, start, at in ((0, lev.base, 0), (1, 2 * ys, nx)):
            if i in only:
                for c in range(3):
                    sx[i, c * run : (c + 1) * run] = part[c][start : start + run]
                    sx[i, tile + c : tile + c + 1] = lows[c][at : at + 1]
                    sx[i, tile + 3 + c : tile + 4 + c] = highs[c][at : at + 1]
        launch((0, 1))
        for i, (src, at) in enumerate(((lows, 0), (highs, 0), (lows, nx), (highs, nx))):
            if 4 + i in only:
                for c in range(3):
                    sd[i, c : c + 1] = src[c][at : at + 1]
        launch((4, 5, 6, 7))
        for i, src in enumerate((lows, highs)):
            if 2 + i in only:
                for c in range(3):
                    sy[i, c * ys : (c + 1) * ys] = src[c]
        launch((2, 3))

    def arrive(l, slot, only=range(8)):
        lev = levels[l]
        ys, run, nx = lev.ys, lev.run, lev.nx
        for i, (dx, dy, copy) in enumerate(copies(l, slot)):
            if i in only:
                pl.when(reach(-dx, -dy))(copy.wait_recv)
                pl.when(reach(dx, dy))(copy.wait_send)
        rx, ry, rd = (R[f"recv{n}{l}"] for n in "xyd")
        tile = pl.ds(3 * run, 8)
        left, right = rx[slot, 1, tile, :], rx[slot, 0, tile, :]
        at = lax.broadcasted_iota(jnp.int32, (ys, lev.lanes), 0)
        out = []
        for c in range(3):
            pieces = []
            for k, src in ((0, 1), (1, 0)):
                val = ry[slot, src, c * ys : (c + 1) * ys, :]
                row = slice(3 * k + c, 3 * k + c + 1)
                low = left[row] + rd[slot, 3 - k, c : c + 1, :]
                high = right[row] + rd[slot, 1 - k, c : c + 1, :]
                val = val + jnp.where(at == 0, low, 0.0) + jnp.where(at == nx, high, 0.0)
                pieces.append(val)
            pieces.append(rx[slot, 0, c * run : (c + 1) * run, :])
            pieces.append(rx[slot, 1, c * run : (c + 1) * run, :])
            out.append(jnp.concatenate(pieces, axis=0))
        return out

    def wide_copies(kind):
        index = 0
        for dx, dy, start, size, at, nodes in wide.sends:
            if dx == 0 and dy == 0:
                continue
            count = up(len(nodes), 8) if kind == "s" else size
            yield dx, dy, pltpu.make_async_remote_copy(
                src_ref=R[f"pack{kind}"].at[pl.ds(start, count)],
                dst_ref=R[f"get{kind}"].at[pl.ds(at, count)],
                send_sem=R[f"wsend{kind}"].at[index],
                recv_sem=R[f"wrecv{kind}"].at[index],
                device_id=device(dx, dy),
                device_id_type=pl.DeviceIdType.MESH,
            )
            index += 1

    def wide_send(kind, value):
        R[f"pack{kind}"][...] = value
        for dx, dy, start, size, at, nodes in wide.sends:
            if dx == 0 and dy == 0:
                R[f"get{kind}"][at : at + size] = value[start : start + size]
        for dx, dy, copy in wide_copies(kind):
            pl.when(reach(dx, dy))(copy.start)

    def wide_wait(kind):
        for dx, dy, copy in wide_copies(kind):
            pl.when(reach(-dx, -dy))(copy.wait_recv)
            pl.when(reach(dx, dy))(copy.wait_send)

    def thirds(value):
        parts = []
        for _ in range(3):
            parts.append(value.astype(BF16))
            value = value - parts[-1].astype(F32)
        return parts

    def wide_scale_send():
        sel = R["gs"][...]
        picked = [mm(sel, part).astype(BF16) for part in thirds(s0[...])]
        wide_send("s", sum(mm(part, R["sz"][...]) for part in picked))

    def wide_scale_take():
        wide_wait("s")
        place = R["place"][0 : wide.rows]
        R[f"s{len(levels) - 1}"][...] = sum(mm(place, part) for part in thirds(R["gets"][...]))
        prepare(len(levels) - 1, 0, wide.rows)

    def set_u(l, c, a, b, value):
        lev = levels[l]
        hi, lo = halves(value)
        at = c * lev.kb + a
        R[f"u{l}"][at : at + b - a] = hi
        R[f"u{l}"][at + lev.kp : at + lev.kp + b - a] = hi
        R[f"u{l}"][at + 2 * lev.kp : at + 2 * lev.kp + b - a] = lo
        if lev.split and a < lev.nb:
            n = min(b, lev.nb) - a
            for i, half in enumerate((hi, hi, lo)):
                at = 256 * c + i * lev.nb + a
                R[f"ub{l}"][at : at + n] = half[0:n]

    def span(l, blk):
        lev = levels[l]
        return (0, lev.nb) if blk == "b" else (lev.nb, lev.rows)

    def prepare(l, a, b):
        s = R[f"s{l}"][a:b]
        f = jnp.where(s == 0.0, 1.0, 0.0)
        R[f"f{l}"][a:b] = f
        square = s * s
        m_z, k_z = R[f"kl{l}"][0:1, :], R[f"kl{l}"][1:2, :]
        for c in range(3):
            kd = R[f"kr{l}"][a:b, c : c + 1] * m_z + R[f"kr{l}"][a:b, 3 + c : 4 + c] * k_z
            R[f"dinv{l}"][c, a:b] = 1.0 / (square * kd + f)

    def begin(l, a, b, source):
        scale = R["coef"][l, 12]
        s = R[f"s{l}"][a:b]
        for c in range(3):
            first = scale * (R[f"dinv{l}"][c, a:b] * source[c])
            R[f"r{l}"][c, a:b] = source[c]
            R[f"d{l}"][c, a:b] = first
            R[f"x{l}"][c, a:b] = first
            set_u(l, c, a, b, s * first)

    def ahead(l):
        lev = levels[l]
        if lev.split:
            for c in range(3):
                u = R[f"u{l}"][c * lev.kb : (c + 1) * lev.kb]
                R[f"pre{l}"][c] = mm(R[f"wi{l}"][c], u)

    def plane_sums(l, blk, n, step):
        lev = levels[l]
        kb = lev.kb
        if blk == "b" and lev.split:
            q = [
                R[f"pre{l}"][c] + mm(R[f"wb{l}"][c], R[f"ub{l}"][256 * c : 256 * (c + 1)])
                for c in range(3)
            ]
            q = [[v[i * n : (i + 1) * n] for i in range(4)] for v in q]
            both = [q[0][i] + q[1][i] for i in range(3)]
            last, plain = q[2], [q[0][3], q[1][3], q[2][3]]
        else:
            u, w1, w2 = R[f"u{l}"], R[f"w1{blk}{l}"], R[f"w2{blk}{l}"]
            tall = [
                w[...] if n == step
                else jnp.concatenate([w[i * step : i * step + n] for i in range(g)], axis=0)
                for w, g in ((w1, 3), (w2, 4))
            ]
            both = mm(tall[0], u[0 : 2 * kb])
            last = mm(tall[1], u[2 * kb : 3 * kb])
            both = [both[i * n : (i + 1) * n] for i in range(3)]
            last = [last[i * n : (i + 1) * n] for i in range(4)]
            mass = w2[3 * step : 3 * step + n]
            plain = [mm(mass, u[0:kb]), mm(mass, u[kb : 2 * kb]), last[3]]
        stretch = (2.0 * MU_SHEAR + LAMBDA_BULK) / MU_SHEAR
        plain[2] = stretch * plain[2]
        return [both[0], both[1], last[2]], plain, [last[0], last[1]], [both[2]]

    def local_sums(l, blk, rows=None):
        lev = levels[l]
        a, b = span(l, blk)
        n = rows or b - a

        def along(which, parts):
            z = R[f"z{l}"]
            if blk == "b" and lev.split:
                pairs = [halves(v) for v in parts]
                high = [v for v, _ in pairs]
                tall = jnp.concatenate(high + [v for _, v in pairs], axis=0)
                first = mm(tall, z[which, 0 : lev.lanes])
                m = len(parts) * n
                low = mm(jnp.concatenate(high, axis=0), z[which, 2 * lev.lanes : 3 * lev.lanes])
                return first[0:m] + first[m : 2 * m] + low
            return mm(jnp.concatenate([wide3(v) for v in parts], axis=0), z[which])

        mass, stiff, trans, mixed = plane_sums(l, blk, n, b - a)
        zm = along(M_, mass)
        zk = along(K_, stiff)
        zt = along(T_, trans)
        zg = along(G_, mixed)
        return [
            zm[0:n] + zk[0:n] + zt[0:n],
            zm[n : 2 * n] + zk[n : 2 * n] + zt[n : 2 * n],
            zm[2 * n : 3 * n] + zk[2 * n : 3 * n] + zg,
        ]

    def advance(l, k, a, b, sums):
        c1, c2 = R["coef"][l, 2 * k], R["coef"][l, 2 * k + 1]
        s, f = R[f"s{l}"][a:b], R[f"f{l}"][a:b]
        for c in range(3):
            d = R[f"d{l}"][c, a:b]
            res = R[f"r{l}"][c, a:b] - (s * sums[c] + f * d)
            new = c1 * d + c2 * (R[f"dinv{l}"][c, a:b] * res)
            R[f"r{l}"][c, a:b] = res
            R[f"d{l}"][c, a:b] = new
            R[f"x{l}"][c, a:b] += new
            set_u(l, c, a, b, s * new)

    def smooth(l, k, slot, beside=None):
        lev = levels[l]
        own, pend = R[f"own{l}"], R[f"pend{l}"]
        part = local_sums(l, "b")
        for c in range(3):
            part[c] = part[c] + pend[c]
            own[c] = part[c]
            pend[c] = jnp.zeros_like(pend[c])
        send(l, slot, part)
        inner = local_sums(l, "i")
        advance(l, k, lev.nb, lev.rows, inner)
        ahead(l)
        if beside is not None:
            beside()
        got = arrive(l, slot)
        advance(l, k, 0, lev.nb, [own[c] + got[c] for c in range(3)])

    def finish(k, slot):
        only = [i for i, (dx, dy) in enumerate(DIRS) if dx >= 0 and dy >= 0]
        c1, c2 = R["coef"][0, 2 * k], R["coef"][0, 2 * k + 1]

        def result(c, a, b, sums):
            s, f, d = R["s0"][a:b], R["f0"][a:b], R["d0"][c, a:b]
            res = R["r0"][c, a:b] - (s * sums + f * d)
            return R["x0"][c, a:b] + (c1 * d + c2 * (R["dinv0"][c, a:b] * res))

        def put_out(c, start, value):
            for v in range(vecs):
                size = value.shape[0]
                R["out"][v, c, start : start + size] = value[:, v * nz : (v + 1) * nz]

        own = R["own0"]
        part = local_sums(0, "b")
        for c in range(3):
            part[c] = part[c] + R["pend0"][c]
            own[c] = part[c]
        send(0, slot, part, only)
        inner = local_sums(0, "i")
        for c in range(3):
            put_out(c, top.run, result(c, top.nb, top.rows, inner[c]))
        got = arrive(0, slot, only)
        for c in range(3):
            value = result(c, 0, top.nb, own[c] + got[c])
            put_out(c, 0, value[top.base : top.nb])
            for x in range(top.nx):
                put_out(c, x * top.run, value[x : x + 1])

    def restrict(l):
        lev = levels[l]
        masked = []
        for blk in "bi":
            a, b = span(l, blk)
            sums = local_sums(l, blk)
            s, f = R[f"s{l}"][a:b], R[f"f{l}"][a:b]
            free = 1.0 - f
            if blk == "b":
                row = lax.broadcasted_iota(jnp.int32, (b - a, lev.lanes), 0)
                mine = jnp.logical_or(row < lev.nx, row >= lev.base)
                free = jnp.where(mine, free, 0.0)
            piece = []
            for c in range(3):
                r, d = R[f"r{l}"][c, a:b], R[f"d{l}"][c, a:b]
                piece.append(free * r - s * sums[c])
                if blk == "b":
                    R[f"pend{l}"][c] = sums[c]
                    R[f"r{l}"][c, a:b] = r - f * d
                else:
                    R[f"r{l}"][c, a:b] = r - (s * sums[c] + f * d)
            masked.append(piece)
        fields = [
            tall2(jnp.concatenate([masked[0][c], masked[1][c]], axis=0)) for c in range(3)
        ]
        if l + 1 == len(levels) - 1:
            n = wide.pack_rows
            flat = []
            for side in range(2):
                mat = R["gp"][side * n : (side + 1) * n]
                field = jnp.concatenate([fields[side], fields[2]], axis=0)
                flat.append(wide2(mm(mat, field)))
            return mm(jnp.concatenate(flat, axis=1), R["gz"][...])
        flat = [wide2(mm(R[f"dp{l}"][...], field)) for field in fields]
        down = mm(jnp.concatenate(flat, axis=0), R[f"dz{l}"][...])
        n = levels[l + 1].rows
        return [down[c * n : (c + 1) * n] for c in range(3)]

    def descend(l, slot, sums):
        lev = levels[l]
        own = R[f"own{l}"]
        for c in range(3):
            own[c] = sums[c][0 : lev.nb]
        send(l, slot, [sums[c][0 : lev.nb] for c in range(3)])
        free = 1.0 - R[f"f{l}"][lev.nb : lev.rows]
        begin(l, lev.nb, lev.rows, [free * sums[c][lev.nb : lev.rows] for c in range(3)])
        if l + 1 == len(levels) - 1:
            wide_scale_take()
        got = arrive(l, slot)
        free = 1.0 - R[f"f{l}"][0 : lev.nb]
        begin(l, 0, lev.nb, [free * (own[c] + got[c]) for c in range(3)])

    def solve_wide(packed):
        l, n, half = len(levels) - 1, wide.rows, wide.half
        wide_send("b", packed)
        wide_wait("b")
        hi, lo = halves(R["getb"][...])
        spread = mm(R["place"][...], hi) + mm(R["place"][...], lo)
        lane = lax.broadcasted_iota(jnp.int32, (n, wide.lanes), 1)
        keep = jnp.where(lane < half, 1.0 - R[f"f{l}"][...], 0.0)
        both, one, two = (spread[i * n : (i + 1) * n] for i in range(3))
        right = [both, pltpu.roll(both, half, 1), one + pltpu.roll(two, half, 1)]
        begin(l, 0, n, [keep * v for v in right])

        for k, rows in enumerate(wide.needed):
            advance(l, k, 0, rows, local_sums(l, "i", rows))

    def ascend(l):
        lev, n = levels[l], levels[l + 1].rows
        field = jnp.concatenate([wide2(R[f"x{l + 1}"][c]) for c in range(3)], axis=0)
        fine = mm(field, R[f"uz{l}"][...])
        free, s = 1.0 - R[f"f{l}"][...], R[f"s{l}"][...]
        for c in range(3):
            step = free * mm(R[f"up{l}"][...], tall2(fine[c * n : (c + 1) * n]))
            R[f"d{l}"][c] = step
            R[f"x{l}"][c] += step
            set_u(l, c, 0, lev.rows, s * step)
        ahead(l)

    def build(l):
        lev = levels[l]
        lines = []
        for axis in "xy":
            tall = mm(R[f"e{axis}{l}"][...], R[f"t{axis}{l}"][...])
            lines.append(
                [
                    mm(tall[:, 128 * i : 128 * (i + 1)].astype(BF16), R[f"c{axis}{l}"][...])
                    for i in range(4)
                ]
            )
        X, Y = lines
        cc = LAMBDA_BULK + MU_SHEAR
        big = MU_SHEAR + cc
        kxmy, mxky = X[K_] * Y[M_], X[M_] * Y[K_]
        first = (
            (0, 0, big * kxmy + MU_SHEAR * mxky),
            (0, 1, cc * (X[G_] * Y[T_])),
            (1, 0, cc * (X[T_] * Y[G_])),
            (1, 1, MU_SHEAR * kxmy + big * mxky),
            (2, 0, cc * (X[T_] * Y[M_])),
            (2, 1, cc * (X[M_] * Y[T_])),
        )
        second = (
            cc * (X[G_] * Y[M_]),
            cc * (X[M_] * Y[G_]),
            MU_SHEAR * (kxmy + mxky),
            X[M_] * Y[M_],
        )
        lane = lax.broadcasted_iota(jnp.int32, (lev.rows, lev.seg), 1)
        middle = jnp.logical_and(lane >= lev.kp, lane < 2 * lev.kp)

        def store(kind, group, at, value):
            hi, lo = halves(value)
            for blk in "bi" if lev.nb and not lev.split else "i":
                a, b = span(l, blk)
                ref, row = R[f"{kind}{blk}{l}"], group * (b - a)
                row = slice(row, row + b - a)
                if lev.packed:
                    mixed = jnp.where(middle, lo.astype(F32), hi.astype(F32)).astype(BF16)
                    ref[row, at : at + 256] = mixed[a:b]
                else:
                    for s, half in enumerate((hi, lo, hi)):
                        start = at + s * lev.kp
                        ref[row, start : start + lev.kp] = half[a:b]

        for group, side, value in first:
            store("w1", group, side * lev.kb, value)
        for group, value in enumerate(second):
            store("w2", group, 0, value)
        if lev.split:
            n, kp = lev.nb, lev.kp
            lane = lax.broadcasted_iota(jnp.int32, (n, kp), 1)
            parts = [(side, group, value) for group, side, value in first]
            parts += [(2, group, value) for group, value in enumerate(second)]
            parts += [(0, 3, second[3]), (1, 3, second[3])]
            for side, group, value in parts:
                hi, lo = (v.astype(F32) for v in halves(value[0:n]))
                rows = slice(group * n, (group + 1) * n)
                inner = [jnp.where(lane >= n, v, 0.0).astype(BF16) for v in (hi, lo)]
                for i, half in enumerate((inner[0], inner[1], inner[0])):
                    R[f"wi{l}"][side, rows, i * kp : (i + 1) * kp] = half
                hi, lo = (jnp.where(lane < n, v, 0.0) for v in (hi, lo))
                mixed = hi + pltpu.roll(lo, n, 1) + pltpu.roll(hi, 2 * n, 1)
                R[f"wb{l}"][side, rows] = mixed.astype(BF16)

    build(0)

    def clear_spare(a, b):
        lead = lax.broadcasted_iota(jnp.int32, (b - a, top.lanes), 0) % top.run == 0
        s0[a:b] = jnp.where(lead, 0.0, s0[a:b])

    clear_spare(top.nb, top.rows)
    prepare(0, top.nb, top.rows)
    begin(0, top.nb, top.rows, [R["r0"][c, top.nb : top.rows] for c in range(3)])
    ahead(0)
    for dx, dy, copy in first_copies():
        pl.when(reach(dx, dy))(copy.wait_send)
        pl.when(reach(-dx, -dy))(copy.wait_recv)
    clear_spare(top.base, top.nb)
    ys, run, nx = top.ys, top.run, top.nx
    at = lax.broadcasted_iota(jnp.int32, (ys, top.lanes), 0)
    for c in range(4):
        dst = s0 if c == 3 else R["r0"].at[c]
        low = jnp.where(at == nx, R["gotx"][c, 0:1, :], put[c])
        high = jnp.where(at == nx, R["gotd"][c : c + 1, :], R["goty"][c])
        dst[0:ys] = low
        dst[ys : 2 * ys] = high
        side = R["gotx"][c]
        if c == 3:
            row = lax.broadcasted_iota(jnp.int32, (run, top.lanes), 0)
            side = jnp.where(row == 0, 0.0, side)
        dst[2 * ys : 2 * ys + run] = side
    prepare(0, 0, top.nb)
    begin(0, 0, top.nb, [R["r0"][c, 0 : top.nb] for c in range(3)])

    def coarse_setup():
        parts = thirds(s0[...])
        build(len(levels) - 1)
        for l in range(1, len(levels) - 1):
            sel_x, sel_z = R[f"sx{l}"][...], R[f"sz{l}"][...]
            picked = [mm(sel_x, part).astype(BF16) for part in parts]
            R[f"s{l}"][...] = sum(mm(part, sel_z) for part in picked)
            prepare(l, 0, levels[l].rows)
            build(l)

    def pre(k, _):
        smooth(0, k, k % 2, lambda: pl.when(k == 0)(coarse_setup))
        return 0

    def cycle(l):
        skip = 0 if l == 0 else 1

        def body(k, _):
            smooth(l, k, (k + skip) % 2)
            return 0

        def tail(k, _):
            smooth(l, k, (k + skip + 1) % 2)
            return 0

        lax.fori_loop(0, DEG - 1, pre if l == 0 else body, 0)
        if l == 0:
            wide_scale_send()
        if l + 1 == len(levels) - 1:
            solve_wide(restrict(l))
        else:
            descend(l + 1, 0, restrict(l))
            cycle(l + 1)
        ascend(l)
        if l:
            lax.fori_loop(DEG, 2 * DEG, tail, 0)
        else:
            lax.fori_loop(DEG, 2 * DEG - 1, tail, 0)
            finish(2 * DEG - 1, (2 * DEG + skip) % 2)

    cycle(0)


def chebyshev_table(spectrum, coef):
    for l in range(3):
        low, top = spectrum[0, l], spectrum[1, l]
        center = 0.5 * (top + low)
        radius = 0.5 * (top - low)
        ratio = center / radius
        rho = 1.0 / ratio
        steps = []
        for _ in range(COARSE_DEG - 1):
            rho_next = 1.0 / (2.0 * ratio - rho)
            steps.append((rho_next * rho, 2.0 * rho_next / radius))
            rho = rho_next
        smooth = steps[: DEG - 1]
        flat = [(0.0, 0.0), (0.0, 1.0 / center)]
        picked = steps if l == 2 else smooth + flat + smooth
        for k, two in enumerate(picked):
            coef[l, 2 * k] = jnp.asarray(two[0], F32)
            coef[l, 2 * k + 1] = jnp.asarray(two[1], F32)
        coef[l, 12] = 1.0 / center


def local(modes, moduli, pinned, spectrum):
    vecs, _, nx, ny, nz = modes.shape
    levels = []
    names, args = [], []

    def add(name, value):
        names.append(name)
        args.append(value)

    for degree in DEGREES:
        step = DEGREES[0] // degree
        size = (degree, nx // step, ny // step, nz // step, vecs)
        levels.append(Level(*size) if step < DEGREES[0] else Wide(*size, COARSE_DEG - 1))
    top = levels[0]
    assert ny == top.run and nz % 128 == 0 and top.rows == top.base + nx * ny
    add("spectrum_in", spectrum.T)
    add("modes", modes.reshape(vecs, 3, nx * ny, nz))
    add("moduli_in", moduli.reshape(nx * ny, nz))
    add("pinned_in", pinned.reshape(nx * ny, nz))
    for l, lev in enumerate(levels):
        for axis, mats in zip("xy", lev.factors()):
            for key, mat in zip("etc", mats):
                add(f"{key}{axis}{l}_in", jnp.asarray(mat))
        add(f"z{l}_in", jnp.asarray(lev.lines()))
        for key, mat in zip(("kr", "kl"), lev.diagonal()):
            add(f"{key}{l}_in", jnp.asarray(mat))
        if l + 1 < len(levels):
            coarsest = l + 2 == len(levels)
            for key, mat in zip(("dp", "dz", "up", "uz"), transfer(lev, levels[l + 1])):
                if key[0] == "u" or not coarsest:
                    add(f"{key}{l}_in", jnp.asarray(mat))
        if 0 < l < len(levels) - 1:
            for key, mat in zip(("sx", "sz"), lev.sample(top)):
                add(f"{key}{l}_in", jnp.asarray(mat))
    wide = levels[-1]
    for key, mat in zip(("gp", "gs", "place", "gz"), wide.gather(levels[-2], top)):
        add(f"{key}_in", jnp.asarray(mat))
    add("sz_in", jnp.asarray(wide.sample(top)[1]))

    specs = [pl.BlockSpec(memory_space=pl.ANY) for n in names]
    scratch = []
    all_names = names + ["out"]

    def temp(name, what):
        all_names.append(name)
        scratch.append(what)

    temp("coef", pltpu.SMEM((3, 13), F32))
    temp("lsem", pltpu.SemaphoreType.DMA((len(names) + 24,)))
    for name, value in zip(names, args):
        if name == "spectrum_in":
            temp("spectrum", pltpu.SMEM(value.shape, F32))
        elif name.endswith("_in"):
            shape = value.shape
            if name[0] == "z":
                lanes = levels[int(name[1])].lanes
                shape = (4, 3 * lanes, lanes)
            elif name[0] == "t":
                shape = shape[1:]
            temp(name[:-3], pltpu.VMEM(shape, value.dtype))
    for l, lev in enumerate(levels):
        field = (3, lev.rows, lev.lanes)
        for n in ("s", "f"):
            temp(f"{n}{l}", pltpu.VMEM(field[1:], F32))
        for n in ("r", "d", "x", "dinv"):
            temp(f"{n}{l}", pltpu.VMEM(field, F32))
        temp(f"u{l}", pltpu.VMEM((3 * lev.kb, lev.lanes), BF16))
        for blk, n in (("b", lev.nb), ("i", lev.rows - lev.nb)):
            if n and not (blk == "b" and lev.split):
                temp(f"w1{blk}{l}", pltpu.VMEM((3 * n, 2 * lev.kb), BF16))
                temp(f"w2{blk}{l}", pltpu.VMEM((4 * n, lev.kb), BF16))
        if lev.split:
            temp(f"ub{l}", pltpu.VMEM((3 * 256, lev.lanes), BF16))
            temp(f"pre{l}", pltpu.VMEM((3, 4 * lev.nb, lev.lanes), F32))
            temp(f"wi{l}", pltpu.VMEM((3, 4 * lev.nb, lev.kb), BF16))
            temp(f"wb{l}", pltpu.VMEM((3, 4 * lev.nb, 256), BF16))
        if lev is wide:
            continue
        for n in ("own", "pend"):
            temp(f"{n}{l}", pltpu.VMEM((3, lev.nb, lev.lanes), F32))
        for n, shape in (
            ("x", (2, 3 * lev.run + 8, lev.lanes)),
            ("y", (2, 3 * lev.ys, lev.lanes)),
            ("d", (4, 8, lev.lanes)),
        ):
            temp(f"send{n}{l}", pltpu.VMEM(shape, F32))
            temp(f"recv{n}{l}", pltpu.VMEM((2,) + shape, F32))
        temp(f"ssem{l}", pltpu.SemaphoreType.DMA((len(DIRS),)))
        temp(f"rsem{l}", pltpu.SemaphoreType.DMA((2, len(DIRS))))
    for kind in "sb":
        temp(f"pack{kind}", pltpu.VMEM((wide.pack_rows, wide.lanes), F32))
        temp(f"get{kind}", pltpu.VMEM((wide.got_rows, wide.lanes), F32))
        temp(f"wsend{kind}", pltpu.SemaphoreType.DMA((len(wide.sends) - 1,)))
        temp(f"wrecv{kind}", pltpu.SemaphoreType.DMA((len(wide.sends) - 1,)))
    temp("put", pltpu.VMEM((4, top.ys, top.lanes), F32))
    temp("putd", pltpu.VMEM((8, top.lanes), F32))
    temp("gotx", pltpu.VMEM((4, top.run, top.lanes), F32))
    temp("goty", pltpu.VMEM((4, top.ys, top.lanes), F32))
    temp("gotd", pltpu.VMEM((8, top.lanes), F32))
    temp("fsend", pltpu.SemaphoreType.DMA((4,)))
    temp("frecv", pltpu.SemaphoreType.DMA((4,)))
    out = pl.pallas_call(
        functools.partial(kernel, levels, all_names),
        out_shape=pltpu.VMEM((vecs, 3, nx * ny, nz), F32),
        in_specs=specs,
        out_specs=pl.BlockSpec(memory_space=pltpu.VMEM),
        scratch_shapes=scratch,
        compiler_params=pltpu.CompilerParams(
            collective_id=0, has_side_effects=True, vmem_limit_bytes=62 * 1024 * 1024
        ),
    )(*args)
    return out.reshape(modes.shape)


def solution(mesh):
    placed = (P(None, None, "gx", "gy", None), P("gx", "gy", None), P("gx", "gy", None), P())
    return jax.shard_map(
        local,
        mesh=mesh,
        in_specs=placed,
        out_specs=P(None, None, "gx", "gy", None),
        check_vma=False,
    )
```

```python
import functools

import jax
import jax.numpy as jnp
import numpy as np
from jax import lax
from jax.experimental import pallas as pl
from jax.experimental.pallas import tpu as pltpu
from jax.sharding import PartitionSpec as P

DEG = 3
COARSE_DEG = 4
DEGREES = (4, 2, 1)
MU_SHEAR = 1.0
LAMBDA_BULK = 1.5
PROLONG_TABLES = {
    4: np.array(
        [[1.0, 0.0, 0.0], [0.375, 0.75, -0.125], [0.0, 1.0, 0.0], [-0.125, 0.75, 0.375]]
    ),
    2: np.array([[1.0, 0.0], [0.5, 0.5]]),
}
DIRS = ((-1, 0), (1, 0), (0, -1), (0, 1), (-1, -1), (-1, 1), (1, -1), (1, 1))
F32 = jnp.float32
BF16 = jnp.bfloat16
M_, K_, G_, T_ = range(4)


def element_matrices(degree):
    nodes = [float(place) / degree for place in range(degree + 1)]
    gauss_x, gauss_w = np.polynomial.legendre.leggauss(8)
    points = 0.5 * (gauss_x + 1.0)
    weights = 0.5 * gauss_w
    values = np.zeros((degree + 1, points.size))
    slopes = np.zeros((degree + 1, points.size))
    for column in range(degree + 1):
        product = np.ones(points.size)
        for other in range(degree + 1):
            if other != column:
                product = product * (points - nodes[other]) / (nodes[column] - nodes[other])
        values[column] = product
        for skipped in range(degree + 1):
            if skipped != column:
                part = np.ones(points.size) / (nodes[column] - nodes[skipped])
                for other in range(degree + 1):
                    if other != column and other != skipped:
                        part = part * (points - nodes[other]) / (nodes[column] - nodes[other])
                slopes[column] += part
    mass = (values * weights) @ values.T
    stiff = (slopes * weights) @ slopes.T
    mixed = (slopes * weights) @ values.T
    return [mass, stiff, mixed, mixed.T]


def assembled(element, count, ghost):
    p = element.shape[0] - 1
    out = np.zeros((count + 1, count + 1))
    for e in range(count // p):
        out[e * p : e * p + p + 1, e * p : e * p + p + 1] += element
    if ghost:
        out[0, 0] += element[p, p]
    return out


def up(n, m):
    return -(-n // m) * m


def bf16_parts(mat, count):
    rest = np.asarray(mat, np.float64)
    parts = []
    for _ in range(count):
        part = rest.astype(np.float32).astype(BF16)
        parts.append(part)
        rest = rest - part.astype(np.float64)
    return parts


def exact_bf16(mat):
    out = np.asarray(mat, np.float32).astype(BF16)
    assert np.array_equal(out.astype(np.float64), mat)
    return out


class Level:
    def __init__(self, degree, nx, ny, nz, vecs):
        self.p, self.nx, self.ny, self.nz, self.vecs = degree, nx, ny, nz, vecs
        self.ys = up(nx + 1, 8)
        self.run = up(ny, 8)
        self.base = 2 * self.ys + self.run
        self.rows = up(self.base + nx * self.run, 16)
        self.nb = self.base + self.run
        assert self.nb % 16 == 0
        self.lanes = up(vecs * nz, 128)
        self.low = 0
        self.where = {(x, y): self.row(x, y) for x in range(nx + 1) for y in range(ny + 1)}
        self.spans = (nx, ny)
        self.columns()

    def columns(self):
        if 3 * self.rows <= 256:
            self.kp, self.kb = self.rows, 256
        else:
            self.kp = up(self.rows, 128)
            self.kb = 3 * self.kp
        self.packed = self.kb == 256
        self.split = not self.packed and 0 < 3 * self.nb <= 256 == self.kp
        self.seg = 256 if self.packed else self.kp

    def row(self, x, y):
        if y == 0:
            return x
        if y == self.ny:
            return self.ys + x
        if x == self.nx:
            return 2 * self.ys + y
        return self.base + self.run * x + y

    def factors(self):
        out = []
        for axis, n in enumerate(self.spans):
            expand = np.zeros((self.rows, 32))
            spread = np.zeros((128, self.seg))
            for at, row in self.where.items():
                expand[row, at[axis] + self.low] = 1
                for copy in range(3 if self.packed else 1):
                    for part in range(3):
                        spread[32 * part + at[axis] + self.low, copy * self.kp + row] = 1
            table = np.zeros((2, 32, 512), BF16)
            for ghost in range(2):
                for i, element in enumerate(element_matrices(self.p)):
                    parts = bf16_parts(assembled(element, n, ghost), 3)
                    for part, mat in enumerate(parts):
                        at = 128 * i + 32 * part
                        table[ghost, : n + 1, at : at + n + 1] = mat
            out.append((exact_bf16(expand), table, exact_bf16(spread)))
        return out

    def lines(self):
        p, n = self.p, self.nz
        mats = []
        for e in element_matrices(p):
            full = assembled(e, n, True)[:n, :n].T
            if n % 128:
                lifted = np.zeros((self.lanes, self.lanes))
                size = self.vecs * n
                lifted[:size, :size] = np.kron(np.eye(self.vecs), full)
                full = lifted
            mats.append(np.stack(bf16_parts(full, 2)))
        return np.stack(mats)

    def diagonal(self):
        def center(which, count):
            p = self.p
            e = element_matrices(p)[which]
            line = np.array([e[a, a] + (e[p, p] if a == 0 else 0.0) for a in range(p)])
            return line[np.arange(count) % p]

        rows = np.zeros((self.rows, 128), np.float32)
        m_x, m_y, m_z = [center(0, n) for n in (self.nx + self.p, self.ny + self.p, self.nz)]
        k_x, k_y, k_z = [center(1, n) for n in (self.nx + self.p, self.ny + self.p, self.nz)]
        for c in range(3):
            coef = [MU_SHEAR + (LAMBDA_BULK + MU_SHEAR) * (c == e) for e in range(3)]
            for (x, y), row in self.where.items():
                x, y = x % self.p, y % self.p
                rows[row, c] = coef[0] * k_x[x] * m_y[y] + coef[1] * m_x[x] * k_y[y]
                rows[row, 3 + c] = coef[2] * m_x[x] * m_y[y]
        lanes = np.zeros((8, self.lanes), np.float32)
        lanes[0, : self.vecs * self.nz] = np.tile(m_z, self.vecs)
        lanes[1, : self.vecs * self.nz] = np.tile(k_z, self.vecs)
        return rows, lanes

    def sample(self, top):
        step = top.p // self.p
        sel_x = np.zeros((self.rows, top.rows))
        for (x, y), row in self.where.items():
            if (x * step, y * step) in top.where:
                sel_x[row, top.where[x * step, y * step]] = 1
        sel_z = np.zeros((top.lanes, self.lanes))
        for v in range(self.vecs):
            for z in range(self.nz):
                sel_z[v * top.nz + z * step, v * self.nz + z] = 1
        return exact_bf16(sel_x), exact_bf16(sel_z)


class Wide(Level):
    def __init__(self, degree, nx, ny, nz, vecs, ring):
        self.p, self.nx, self.ny, self.nz, self.vecs = degree, nx, ny, nz, vecs
        self.low = ring * degree
        self.spans = (nx + 2 * self.low, ny + 2 * self.low)
        self.lanes = up(vecs * nz, 128)
        self.half = self.lanes // 2
        assert vecs * nz <= self.half
        spots = [
            (max(-x, x - nx, -y, y - ny, 0), x, y)
            for x in range(-self.low, nx + self.low + 1)
            for y in range(-self.low, ny + self.low + 1)
        ]
        self.where = {(x, y): row for row, (_, x, y) in enumerate(sorted(spots))}
        self.rows = up(len(self.where), 16)
        self.needed = [
            up(sum(away <= (ring - 1 - k) * degree for away, _, _ in spots), 16)
            for k in range(ring)
        ]
        self.nb = 0
        self.columns()
        self.plan()

    def plan(self):
        nx, ny, low = self.nx, self.ny, self.low
        closed = [(x, y) for x in range(nx + 1) for y in range(ny + 1)]
        far = [-(-(low + 1) // n) for n in (nx, ny)]
        self.far = far
        self.sections, self.sends = [], []
        self.pack_rows = 0
        at = 0
        kinds = {}
        for dx in range(-far[0], far[0] + 1):
            for dy in range(-far[1], far[1] + 1):
                nodes = tuple(
                    (x, y) for x, y in closed if (x - dx * nx, y - dy * ny) in self.where
                )
                if not nodes:
                    continue
                if nodes not in kinds:
                    k = len(nodes)
                    size = up(k + -(-k // 2), 8)
                    kinds[nodes] = (self.pack_rows, size)
                    self.sections.append((self.pack_rows, size, nodes))
                    self.pack_rows += size
                start, size = kinds[nodes]
                self.sends.append((dx, dy, start, size, at, nodes))
                at += size
        self.pack_rows = up(self.pack_rows, 16)
        self.got_rows = up(at, 16)

    def gather(self, fine, top):
        table = PROLONG_TABLES[fine.p]
        px, py = interpolation(table, fine.nx), interpolation(table, fine.ny)
        plane = {
            (cx, cy): np.array(
                [
                    [px[x, cx] * py[y, cy], row]
                    for (x, y), row in fine.where.items()
                    if px[x, cx] * py[y, cy] != 0.0
                ]
            )
            for cx in range(self.nx + 1)
            for cy in range(self.ny + 1)
        }
        pack = np.zeros((2, self.pack_rows, 4 * fine.rows))
        scale = np.zeros((self.pack_rows, top.rows))
        step = top.p // self.p
        for start, size, nodes in self.sections:
            k = len(nodes)
            h = -(-k // 2)
            for i, node in enumerate(nodes):
                for weight, row in plane[node]:
                    row = int(row)
                    for side in range(2):
                        pack[side, start + i, row] = weight
                        pack[side, start + i, fine.rows + row] = weight
                    side = i // h
                    pack[side, start + k + i % h, 2 * fine.rows + row] = weight
                    pack[side, start + k + i % h, 3 * fine.rows + row] = weight
                if node[0] < self.nx and node[1] < self.ny:
                    scale[start + i, top.where[node[0] * step, node[1] * step]] = 1
        place = np.zeros((3, self.rows, self.got_rows))
        for dx, dy, start, size, at, nodes in self.sends:
            k = len(nodes)
            h = -(-k // 2)
            for i, (x, y) in enumerate(nodes):
                to = self.where.get((x - dx * self.nx, y - dy * self.ny))
                if to is not None:
                    place[0, to, at + i] = 1
                    place[1 + i // h, to, at + k + i % h] = 1
        down = interpolation(table, fine.nz)[: fine.nz, : self.nz]
        line = np.zeros((2, 2 * fine.lanes, self.lanes))
        size = (self.vecs * fine.nz, self.vecs * self.nz)
        for side in range(2):
            for copy in range(2):
                line[
                    side,
                    copy * fine.lanes : copy * fine.lanes + size[0],
                    side * self.half : side * self.half + size[1],
                ] = np.kron(np.eye(self.vecs), down)
        mats = (
            pack.reshape(2 * self.pack_rows, 4 * fine.rows),
            scale,
            place.reshape(3 * self.rows, self.got_rows),
            line.reshape(4 * fine.lanes, self.lanes),
        )
        return [exact_bf16(m) for m in mats]


def interpolation(table, count):
    q = table.shape[0]
    half = q // 2
    out = np.zeros((count + 1, count // 2 + 1))
    for i in range(count + 1):
        for t in range(half + 1):
            j = half * (i // q) + t
            if table[i % q, t] != 0.0:
                out[i, j] += table[i % q, t]
    return out


def transfer(fine, coarse):
    table = PROLONG_TABLES[fine.p]
    px, py = interpolation(table, fine.nx), interpolation(table, fine.ny)
    pz = interpolation(table, fine.nz)[: fine.nz, : coarse.nz]
    plane = np.zeros((fine.rows, coarse.rows))
    for (x, y), row in fine.where.items():
        for (cx, cy), col in coarse.where.items():
            if 0 <= cx <= coarse.nx and 0 <= cy <= coarse.ny:
                plane[row, col] = px[x, cx] * py[y, cy]
    line = np.zeros((coarse.lanes, fine.lanes))
    size = (fine.vecs * coarse.nz, fine.vecs * fine.nz)
    line[: size[0], : size[1]] = np.kron(np.eye(fine.vecs), pz.T)
    down = (np.tile(plane.T, (1, 2)), np.tile(line.T, (2, 1)))
    upward = (np.tile(plane, (1, 2)), np.tile(line, (2, 1)))
    return [exact_bf16(m) for m in down + upward]


def halves(value):
    hi = value.astype(BF16)
    return hi, (value - hi.astype(F32)).astype(BF16)


def mm(a, b):
    return lax.dot_general(a, b, (((1,), (0,)), ((), ())), preferred_element_type=F32)


def wide3(value):
    hi, lo = halves(value)
    return jnp.concatenate([hi, lo, hi], axis=1)


def wide2(value):
    hi, lo = halves(value)
    return jnp.concatenate([hi, lo], axis=1)


def tall2(value):
    hi, lo = halves(value)
    return jnp.concatenate([hi, lo], axis=0)


def kernel(levels, names, *refs):
    R = dict(zip(names, refs))
    gx_n, gy_n = lax.axis_size("gx"), lax.axis_size("gy")
    me_x, me_y = lax.axis_index("gx"), lax.axis_index("gy")

    def reach(dx, dy):
        ok = None
        for d, me, n in ((dx, me_x, gx_n), (dy, me_y, gy_n)):
            if d:
                here = me + d < n if d > 0 else me + d >= 0
                ok = here if ok is None else jnp.logical_and(ok, here)
        return ok

    def device(dx, dy):
        return (jnp.clip(me_x + dx, 0, gx_n - 1), jnp.clip(me_y + dy, 0, gy_n - 1))

    top = levels[0]
    vecs, nz = top.vecs, top.nz
    body_rows = pl.ds(top.base, top.nx * top.run)

    moves = []

    def load(src, dst):
        moves.append(pltpu.make_async_copy(src, dst, R["lsem"].at[len(moves)]))
        moves[-1].start()

    load(R["moduli_in"], R["moduli"])
    load(R["pinned_in"], R["pinned"])
    load(R["spectrum_in"], R["spectrum"])
    for v in range(vecs):
        load(R["modes"].at[v], R["r0"].at[:, body_rows, pl.ds(v * nz, nz)])
    first_moves = len(moves)
    wide = levels[-1]
    edged = range(len(levels) - 1)

    def clear(name):
        R[name][...] = jnp.zeros_like(R[name])

    for l in edged:
        for n in "xyd":
            clear(f"recv{n}{l}")
    for n in ("gotx", "goty", "gotd", "gets", "getb"):
        clear(n)

    barrier = pltpu.get_barrier_semaphore()
    peers = [(dx, dy) for dx, dy, *_ in wide.sends if dx or dy]
    assert set(DIRS) <= set(peers)
    for dx, dy in peers:

        @pl.when(reach(dx, dy))
        def _():
            pl.semaphore_signal(
                barrier, inc=1, device_id=device(dx, dy), device_id_type=pl.DeviceIdType.MESH
            )

    for l, lev in enumerate(levels):
        if lev.nz % 128 == 0:
            R[f"z{l}"][...] = jnp.zeros_like(R[f"z{l}"])
        load(R[f"tx{l}_in"].at[jnp.where(me_x == 0, 1, 0)], R[f"tx{l}"])
        load(R[f"ty{l}_in"].at[jnp.where(me_y == 0, 1, 0)], R[f"ty{l}"])
    for name in names:
        if name.endswith("_in") and name[:2] not in ("mo", "pi", "sp", "tx", "ty"):
            if name[0] == "z":
                lev = levels[int(name[1])]
                src, dst = R[name], R[name[:-3]]
                size = lev.nz if lev.nz % 128 == 0 else lev.lanes
                for s, half in enumerate((0, 0, 1)):
                    for at in range(0, lev.lanes, size):
                        load(
                            src.at[:, half],
                            dst.at[:, pl.ds(s * lev.lanes + at, size), pl.ds(at, size)],
                        )
            else:
                load(R[name], R[name[:-3]])

    for l in edged:
        for n in "xyd":
            clear(f"send{n}{l}")
        clear(f"pend{l}")
    for l in range(len(levels)):
        clear(f"u{l}")
        if levels[l].split:
            clear(f"ub{l}")

    for one in moves[:first_moves]:
        one.wait()
    chebyshev_table(R["spectrum"], R["coef"])
    scale = R["moduli"][...] * (1.0 - R["pinned"][...].astype(F32))
    s0 = R["s0"]
    s0[0 : top.base] = jnp.zeros((top.base, top.lanes), F32)
    for v in range(vecs):
        s0[body_rows, v * nz : (v + 1) * nz] = scale
    put = R["put"]
    put[...] = jnp.zeros_like(put)
    for c in range(3):
        for x in range(top.nx):
            at = top.base + x * top.run
            put[c, x : x + 1, :] = R["r0"][c, at : at + 1, :]
    for x in range(top.nx):
        at = top.base + x * top.run
        put[3, x : x + 1, :] = s0[at : at + 1, :]
    for c in range(4):
        R["putd"][c : c + 1, :] = put[c, 0:1, :]
    R["putd"][4:8, :] = jnp.zeros((4, top.lanes), F32)
    edge = pl.ds(top.base, top.run)

    def first_copies():
        plan = (
            (-1, 0, R["r0"].at[:, edge, :], R["gotx"].at[pl.ds(0, 3)]),
            (-1, 0, s0.at[edge, :], R["gotx"].at[3]),
            (0, -1, put, R["goty"]),
            (-1, -1, R["putd"], R["gotd"]),
        )
        for i, (dx, dy, src, dst) in enumerate(plan):
            yield dx, dy, pltpu.make_async_remote_copy(
                src_ref=src,
                dst_ref=dst,
                send_sem=R["fsend"].at[i],
                recv_sem=R["frecv"].at[i],
                device_id=device(dx, dy),
                device_id_type=pl.DeviceIdType.MESH,
            )

    around = []
    for me, n, far in ((me_x, gx_n, wide.far[0]), (me_y, gy_n, wide.far[1])):
        around.append(1 + jnp.minimum(me, far) + jnp.minimum(n - 1 - me, far))
    pl.semaphore_wait(barrier, around[0] * around[1] - 1)
    for dx, dy, copy in first_copies():
        pl.when(reach(dx, dy))(copy.start)
    for one in moves[first_moves:]:
        one.wait()

    def copies(l, slot, only):
        for i in only:
            dx, dy = DIRS[i]
            kind, at = ("d", i - 4) if dx and dy else ("x", i) if dx else ("y", i - 2)
            src, dst = R[f"send{kind}{l}"].at[at], R[f"recv{kind}{l}"].at[slot, at]
            if kind == "d":
                src, dst = src.at[pl.ds(0, 3)], dst.at[pl.ds(0, 3)]
            yield i, dx, dy, pltpu.make_async_remote_copy(
                src_ref=src,
                dst_ref=dst,
                send_sem=R[f"ssem{l}"].at[i],
                recv_sem=R[f"rsem{l}"].at[slot, i],
                device_id=device(dx, dy),
                device_id_type=pl.DeviceIdType.MESH,
            )

    def send(l, slot, part, only=range(8)):
        lev = levels[l]
        ys, run, nx = lev.ys, lev.run, lev.nx
        sx, sy, sd = (R[f"send{n}{l}"] for n in "xyd")
        tile = 3 * run
        order = {i: rest for i, *rest in copies(l, slot, only)}
        lows, highs = [v[0:ys] for v in part], [v[ys : 2 * ys] for v in part]
        def launch(which):
            for i in which:
                if i in only:
                    dx, dy, copy = order[i]
                    pl.when(reach(dx, dy))(copy.start)

        for i, start, at in ((0, lev.base, 0), (1, 2 * ys, nx)):
            if i in only:
                for c in range(3):
                    sx[i, c * run : (c + 1) * run] = part[c][start : start + run]
                    sx[i, tile + c : tile + c + 1] = lows[c][at : at + 1]
                    sx[i, tile + 3 + c : tile + 4 + c] = highs[c][at : at + 1]
        launch((0, 1))
        for i, (src, at) in enumerate(((lows, 0), (highs, 0), (lows, nx), (highs, nx))):
            if 4 + i in only:
                for c in range(3):
                    sd[i, c : c + 1] = src[c][at : at + 1]
        launch((4, 5, 6, 7))
        for i, src in enumerate((lows, highs)):
            if 2 + i in only:
                for c in range(3):
                    sy[i, c * ys : (c + 1) * ys] = src[c]
        launch((2, 3))

    def arrive(l, slot, only=range(8)):
        lev = levels[l]
        ys, run, nx = lev.ys, lev.run, lev.nx
        for _, dx, dy, copy in copies(l, slot, only):
            pl.when(reach(-dx, -dy))(copy.wait_recv)
        rx, ry, rd = (R[f"recv{n}{l}"] for n in "xyd")
        tile = pl.ds(3 * run, 8)
        left, right = rx[slot, 1, tile, :], rx[slot, 0, tile, :]
        at = lax.broadcasted_iota(jnp.int32, (ys, lev.lanes), 0)
        out = []
        for c in range(3):
            pieces = []
            for k, src in ((0, 1), (1, 0)):
                val = ry[slot, src, c * ys : (c + 1) * ys, :]
                row = slice(3 * k + c, 3 * k + c + 1)
                low = left[row] + rd[slot, 3 - k, c : c + 1, :]
                high = right[row] + rd[slot, 1 - k, c : c + 1, :]
                val = val + jnp.where(at == 0, low, 0.0) + jnp.where(at == nx, high, 0.0)
                pieces.append(val)
            pieces.append(rx[slot, 0, c * run : (c + 1) * run, :])
            pieces.append(rx[slot, 1, c * run : (c + 1) * run, :])
            out.append(jnp.concatenate(pieces, axis=0))
        return out

    def settle(l, slot, only=range(8)):
        for _, dx, dy, copy in copies(l, slot, only):
            pl.when(reach(dx, dy))(copy.wait_send)

    def wide_copies(kind):
        index = 0
        for dx, dy, start, size, at, nodes in wide.sends:
            if dx == 0 and dy == 0:
                continue
            count = up(len(nodes), 8) if kind == "s" else size
            yield dx, dy, pltpu.make_async_remote_copy(
                src_ref=R[f"pack{kind}"].at[pl.ds(start, count)],
                dst_ref=R[f"get{kind}"].at[pl.ds(at, count)],
                send_sem=R[f"wsend{kind}"].at[index],
                recv_sem=R[f"wrecv{kind}"].at[index],
                device_id=device(dx, dy),
                device_id_type=pl.DeviceIdType.MESH,
            )
            index += 1

    def wide_send(kind, value):
        R[f"pack{kind}"][...] = value
        for dx, dy, start, size, at, nodes in wide.sends:
            if dx == 0 and dy == 0:
                R[f"get{kind}"][at : at + size] = value[start : start + size]
        for dx, dy, copy in wide_copies(kind):
            pl.when(reach(dx, dy))(copy.start)

    def wide_wait(kind):
        for dx, dy, copy in wide_copies(kind):
            pl.when(reach(-dx, -dy))(copy.wait_recv)
            pl.when(reach(dx, dy))(copy.wait_send)

    def thirds(value):
        parts = []
        for _ in range(3):
            parts.append(value.astype(BF16))
            value = value - parts[-1].astype(F32)
        return parts

    def wide_scale_send():
        sel = R["gs"][...]
        picked = [mm(sel, part).astype(BF16) for part in thirds(s0[...])]
        wide_send("s", sum(mm(part, R["sz"][...]) for part in picked))

    def wide_scale_take():
        wide_wait("s")
        place = R["place"][0 : wide.rows]
        R[f"s{len(levels) - 1}"][...] = sum(mm(place, part) for part in thirds(R["gets"][...]))
        prepare(len(levels) - 1, 0, wide.rows)

    def set_u(l, c, a, b, value):
        lev = levels[l]
        hi, lo = halves(value)
        at = c * lev.kb + a
        R[f"u{l}"][at : at + b - a] = hi
        R[f"u{l}"][at + lev.kp : at + lev.kp + b - a] = hi
        R[f"u{l}"][at + 2 * lev.kp : at + 2 * lev.kp + b - a] = lo
        if lev.split and a < lev.nb:
            n = min(b, lev.nb) - a
            for i, half in enumerate((hi, hi, lo)):
                at = 256 * c + i * lev.nb + a
                R[f"ub{l}"][at : at + n] = half[0:n]

    def span(l, blk):
        lev = levels[l]
        return (0, lev.nb) if blk == "b" else (lev.nb, lev.rows)

    def prepare(l, a, b):
        s = R[f"s{l}"][a:b]
        f = jnp.where(s == 0.0, 1.0, 0.0)
        R[f"f{l}"][a:b] = f
        square = s * s
        m_z, k_z = R[f"kl{l}"][0:1, :], R[f"kl{l}"][1:2, :]
        for c in range(3):
            kd = R[f"kr{l}"][a:b, c : c + 1] * m_z + R[f"kr{l}"][a:b, 3 + c : 4 + c] * k_z
            R[f"dinv{l}"][c, a:b] = 1.0 / (square * kd + f)

    def begin(l, a, b, source):
        scale = R["coef"][l, 12]
        s = R[f"s{l}"][a:b]
        for c in range(3):
            first = scale * (R[f"dinv{l}"][c, a:b] * source[c])
            R[f"r{l}"][c, a:b] = source[c]
            R[f"d{l}"][c, a:b] = first
            R[f"x{l}"][c, a:b] = first
            set_u(l, c, a, b, s * first)

    def ahead(l):
        lev = levels[l]
        if lev.split:
            for c in range(3):
                u = R[f"u{l}"][c * lev.kb : (c + 1) * lev.kb]
                R[f"pre{l}"][c] = mm(R[f"wi{l}"][c], u)

    def ahead_inner():
        n = top.rows - top.nb
        u = R["u0"]
        for at in range(0, 3 * top.kb, top.kp):
            u[at : at + top.nb] = jnp.zeros((top.nb, top.lanes), BF16)
        w1, w2, kb = R["w1i0"], R["w2i0"], top.kb
        R["inner"][0 : 3 * n] = mm(w1[...], u[0 : 2 * kb])
        R["inner"][3 * n : 7 * n] = mm(w2[...], u[2 * kb : 3 * kb])
        for c in range(2):
            at = (7 + c) * n
            R["inner"][at : at + n] = mm(w2[3 * n : 4 * n], u[c * kb : (c + 1) * kb])

    def plane_sums(l, blk, n, step, early):
        lev = levels[l]
        kb = lev.kb
        if blk == "b" and lev.split:
            q = [
                R[f"pre{l}"][c] + mm(R[f"wb{l}"][c], R[f"ub{l}"][256 * c : 256 * (c + 1)])
                for c in range(3)
            ]
            q = [[v[i * n : (i + 1) * n] for i in range(4)] for v in q]
            both = [q[0][i] + q[1][i] for i in range(3)]
            last, plain = q[2], [q[0][3], q[1][3], q[2][3]]
        elif early and lev.split:
            q = [mm(R[f"wj{l}"][c], R[f"ub{l}"][256 * c : 256 * (c + 1)]) for c in range(3)]
            q = [[v[i * n : (i + 1) * n] for i in range(4)] for v in q]
            done = [R["inner"][i * n : (i + 1) * n] for i in range(9)]
            both = [done[i] + q[0][i] + q[1][i] for i in range(3)]
            last = [done[3 + i] + q[2][i] for i in range(4)]
            plain = [done[7] + q[0][3], done[8] + q[1][3], last[3]]
        else:
            u, w1, w2 = R[f"u{l}"], R[f"w1{blk}{l}"], R[f"w2{blk}{l}"]
            tall = [
                w[...] if n == step
                else jnp.concatenate([w[i * step : i * step + n] for i in range(g)], axis=0)
                for w, g in ((w1, 3), (w2, 4))
            ]
            both = mm(tall[0], u[0 : 2 * kb])
            last = mm(tall[1], u[2 * kb : 3 * kb])
            both = [both[i * n : (i + 1) * n] for i in range(3)]
            last = [last[i * n : (i + 1) * n] for i in range(4)]
            mass = w2[3 * step : 3 * step + n]
            plain = [mm(mass, u[0:kb]), mm(mass, u[kb : 2 * kb]), last[3]]
        stretch = (2.0 * MU_SHEAR + LAMBDA_BULK) / MU_SHEAR
        plain[2] = stretch * plain[2]
        return [both[0], both[1], last[2]], plain, [last[0], last[1]], [both[2]]

    def local_sums(l, blk, rows=None, early=False):
        lev = levels[l]
        a, b = span(l, blk)
        n = rows or b - a

        def along(which, parts):
            z = R[f"z{l}"]
            if blk == "b" and lev.split:
                pairs = [halves(v) for v in parts]
                high = [v for v, _ in pairs]
                tall = jnp.concatenate(high + [v for _, v in pairs], axis=0)
                first = mm(tall, z[which, 0 : lev.lanes])
                m = len(parts) * n
                low = mm(jnp.concatenate(high, axis=0), z[which, 2 * lev.lanes : 3 * lev.lanes])
                return first[0:m] + first[m : 2 * m] + low
            return mm(jnp.concatenate([wide3(v) for v in parts], axis=0), z[which])

        mass, stiff, trans, mixed = plane_sums(l, blk, n, b - a, early)
        zm = along(M_, mass)
        zk = along(K_, stiff)
        zt = along(T_, trans)
        zg = along(G_, mixed)
        return [
            zm[0:n] + zk[0:n] + zt[0:n],
            zm[n : 2 * n] + zk[n : 2 * n] + zt[n : 2 * n],
            zm[2 * n : 3 * n] + zk[2 * n : 3 * n] + zg,
        ]

    def advance(l, k, a, b, sums):
        c1, c2 = R["coef"][l, 2 * k], R["coef"][l, 2 * k + 1]
        s, f = R[f"s{l}"][a:b], R[f"f{l}"][a:b]
        for c in range(3):
            d = R[f"d{l}"][c, a:b]
            res = R[f"r{l}"][c, a:b] - (s * sums[c] + f * d)
            new = c1 * d + c2 * (R[f"dinv{l}"][c, a:b] * res)
            R[f"r{l}"][c, a:b] = res
            R[f"d{l}"][c, a:b] = new
            R[f"x{l}"][c, a:b] += new
            set_u(l, c, a, b, s * new)

    def smooth(l, k, slot, beside=None):
        lev = levels[l]
        own, pend = R[f"own{l}"], R[f"pend{l}"]
        part = local_sums(l, "b")
        for c in range(3):
            part[c] = part[c] + pend[c]
            own[c] = part[c]
            pend[c] = jnp.zeros_like(pend[c])
        send(l, slot, part)
        inner = local_sums(l, "i")
        advance(l, k, lev.nb, lev.rows, inner)
        ahead(l)
        if beside is not None:
            beside()
        got = arrive(l, slot)
        advance(l, k, 0, lev.nb, [own[c] + got[c] for c in range(3)])
        settle(l, slot)

    def finish(k, slot):
        only = [i for i, (dx, dy) in enumerate(DIRS) if dx >= 0 and dy >= 0]
        c1, c2 = R["coef"][0, 2 * k], R["coef"][0, 2 * k + 1]

        def result(c, a, b, sums):
            s, f, d = R["s0"][a:b], R["f0"][a:b], R["d0"][c, a:b]
            res = R["r0"][c, a:b] - (s * sums + f * d)
            return R["x0"][c, a:b] + (c1 * d + c2 * (R["dinv0"][c, a:b] * res))

        def put_out(c, start, value):
            for v in range(vecs):
                size = value.shape[0]
                R["out"][v, c, start : start + size] = value[:, v * nz : (v + 1) * nz]

        own = R["own0"]
        part = local_sums(0, "b")
        for c in range(3):
            part[c] = part[c] + R["pend0"][c]
            own[c] = part[c]
        send(0, slot, part, only)
        inner = local_sums(0, "i")
        for c in range(3):
            put_out(c, top.run, result(c, top.nb, top.rows, inner[c]))
        got = arrive(0, slot, only)
        for c in range(3):
            value = result(c, 0, top.nb, own[c] + got[c])
            put_out(c, 0, value[top.base : top.nb])
            for x in range(top.nx):
                put_out(c, x * top.run, value[x : x + 1])
        settle(0, slot, only)

    def restrict(l):
        lev = levels[l]
        masked = []
        for blk in "bi":
            a, b = span(l, blk)
            sums = local_sums(l, blk, early=True)
            s, f = R[f"s{l}"][a:b], R[f"f{l}"][a:b]
            free = 1.0 - f
            if blk == "b":
                row = lax.broadcasted_iota(jnp.int32, (b - a, lev.lanes), 0)
                mine = jnp.logical_or(row < lev.nx, row >= lev.base)
                free = jnp.where(mine, free, 0.0)
            piece = []
            for c in range(3):
                r, d = R[f"r{l}"][c, a:b], R[f"d{l}"][c, a:b]
                piece.append(free * r - s * sums[c])
                if blk == "b":
                    R[f"pend{l}"][c] = sums[c]
                    R[f"r{l}"][c, a:b] = r - f * d
                else:
                    R[f"r{l}"][c, a:b] = r - (s * sums[c] + f * d)
            masked.append(piece)
        fields = [
            tall2(jnp.concatenate([masked[0][c], masked[1][c]], axis=0)) for c in range(3)
        ]
        if l + 1 == len(levels) - 1:
            n = wide.pack_rows
            flat = []
            for side in range(2):
                mat = R["gp"][side * n : (side + 1) * n]
                field = jnp.concatenate([fields[side], fields[2]], axis=0)
                flat.append(wide2(mm(mat, field)))
            return mm(jnp.concatenate(flat, axis=1), R["gz"][...])
        flat = [wide2(mm(R[f"dp{l}"][...], field)) for field in fields]
        down = mm(jnp.concatenate(flat, axis=0), R[f"dz{l}"][...])
        n = levels[l + 1].rows
        return [down[c * n : (c + 1) * n] for c in range(3)]

    def descend(l, slot, sums):
        lev = levels[l]
        own = R[f"own{l}"]
        for c in range(3):
            own[c] = sums[c][0 : lev.nb]
        send(l, slot, [sums[c][0 : lev.nb] for c in range(3)])
        free = 1.0 - R[f"f{l}"][lev.nb : lev.rows]
        begin(l, lev.nb, lev.rows, [free * sums[c][lev.nb : lev.rows] for c in range(3)])
        if l + 1 == len(levels) - 1:
            wide_scale_take()
        got = arrive(l, slot)
        free = 1.0 - R[f"f{l}"][0 : lev.nb]
        begin(l, 0, lev.nb, [free * (own[c] + got[c]) for c in range(3)])
        settle(l, slot)

    def solve_wide(packed):
        l, n, half = len(levels) - 1, wide.rows, wide.half
        wide_send("b", packed)
        wide_wait("b")
        hi, lo = halves(R["getb"][...])
        spread = mm(R["place"][...], hi) + mm(R["place"][...], lo)
        lane = lax.broadcasted_iota(jnp.int32, (n, wide.lanes), 1)
        keep = jnp.where(lane < half, 1.0 - R[f"f{l}"][...], 0.0)
        both, one, two = (spread[i * n : (i + 1) * n] for i in range(3))
        right = [both, pltpu.roll(both, half, 1), one + pltpu.roll(two, half, 1)]
        begin(l, 0, n, [keep * v for v in right])

        for k, rows in enumerate(wide.needed):
            advance(l, k, 0, rows, local_sums(l, "i", rows))

    def ascend(l):
        lev, n = levels[l], levels[l + 1].rows
        field = jnp.concatenate([wide2(R[f"x{l + 1}"][c]) for c in range(3)], axis=0)
        fine = mm(field, R[f"uz{l}"][...])
        free, s = 1.0 - R[f"f{l}"][...], R[f"s{l}"][...]
        for c in range(3):
            step = free * mm(R[f"up{l}"][...], tall2(fine[c * n : (c + 1) * n]))
            R[f"d{l}"][c] = step
            R[f"x{l}"][c] += step
            set_u(l, c, 0, lev.rows, s * step)
        ahead(l)

    def build(l):
        lev = levels[l]
        lines = []
        for axis in "xy":
            tall = mm(R[f"e{axis}{l}"][...], R[f"t{axis}{l}"][...])
            lines.append(
                [
                    mm(tall[:, 128 * i : 128 * (i + 1)].astype(BF16), R[f"c{axis}{l}"][...])
                    for i in range(4)
                ]
            )
        X, Y = lines
        cc = LAMBDA_BULK + MU_SHEAR
        big = MU_SHEAR + cc
        kxmy, mxky = X[K_] * Y[M_], X[M_] * Y[K_]
        first = (
            (0, 0, big * kxmy + MU_SHEAR * mxky),
            (0, 1, cc * (X[G_] * Y[T_])),
            (1, 0, cc * (X[T_] * Y[G_])),
            (1, 1, MU_SHEAR * kxmy + big * mxky),
            (2, 0, cc * (X[T_] * Y[M_])),
            (2, 1, cc * (X[M_] * Y[T_])),
        )
        second = (
            cc * (X[G_] * Y[M_]),
            cc * (X[M_] * Y[G_]),
            MU_SHEAR * (kxmy + mxky),
            X[M_] * Y[M_],
        )
        lane = lax.broadcasted_iota(jnp.int32, (lev.rows, lev.seg), 1)
        middle = jnp.logical_and(lane >= lev.kp, lane < 2 * lev.kp)

        def store(kind, group, at, value):
            hi, lo = halves(value)
            for blk in "bi" if lev.nb and not lev.split else "i":
                a, b = span(l, blk)
                ref, row = R[f"{kind}{blk}{l}"], group * (b - a)
                row = slice(row, row + b - a)
                if lev.packed:
                    mixed = jnp.where(middle, lo.astype(F32), hi.astype(F32)).astype(BF16)
                    ref[row, at : at + 256] = mixed[a:b]
                else:
                    for s, half in enumerate((hi, lo, hi)):
                        start = at + s * lev.kp
                        ref[row, start : start + lev.kp] = half[a:b]

        for group, side, value in first:
            store("w1", group, side * lev.kb, value)
        for group, value in enumerate(second):
            store("w2", group, 0, value)
        if lev.split:
            n, kp = lev.nb, lev.kp
            lane = lax.broadcasted_iota(jnp.int32, (lev.rows, kp), 1)
            parts = [(side, group, value) for group, side, value in first]
            parts += [(2, group, value) for group, value in enumerate(second)]
            parts += [(0, 3, second[3]), (1, 3, second[3])]
            for side, group, value in parts:
                hi, lo = (v.astype(F32) for v in halves(value))
                rows = slice(group * n, (group + 1) * n)
                inner = [jnp.where(lane[0:n] >= n, v[0:n], 0.0).astype(BF16) for v in (hi, lo)]
                for i, half in enumerate((inner[0], inner[1], inner[0])):
                    R[f"wi{l}"][side, rows, i * kp : (i + 1) * kp] = half
                hi, lo = (jnp.where(lane < n, v, 0.0) for v in (hi, lo))
                mixed = hi + pltpu.roll(lo, n, 1) + pltpu.roll(hi, 2 * n, 1)
                mixed = mixed.astype(BF16)
                R[f"wb{l}"][side, rows] = mixed[0:n]
                rest = lev.rows - n
                R[f"wj{l}"][side, group * rest : (group + 1) * rest] = mixed[n : lev.rows]

    build(0)

    def clear_spare(a, b):
        lead = lax.broadcasted_iota(jnp.int32, (b - a, top.lanes), 0) % top.run == 0
        s0[a:b] = jnp.where(lead, 0.0, s0[a:b])

    clear_spare(top.nb, top.rows)
    prepare(0, top.nb, top.rows)
    begin(0, top.nb, top.rows, [R["r0"][c, top.nb : top.rows] for c in range(3)])
    ahead(0)
    for dx, dy, copy in first_copies():
        pl.when(reach(dx, dy))(copy.wait_send)
        pl.when(reach(-dx, -dy))(copy.wait_recv)
    clear_spare(top.base, top.nb)
    ys, run, nx = top.ys, top.run, top.nx
    at = lax.broadcasted_iota(jnp.int32, (ys, top.lanes), 0)
    for c in range(4):
        dst = s0 if c == 3 else R["r0"].at[c]
        low = jnp.where(at == nx, R["gotx"][c, 0:1, :], put[c])
        high = jnp.where(at == nx, R["gotd"][c : c + 1, :], R["goty"][c])
        dst[0:ys] = low
        dst[ys : 2 * ys] = high
        side = R["gotx"][c]
        if c == 3:
            row = lax.broadcasted_iota(jnp.int32, (run, top.lanes), 0)
            side = jnp.where(row == 0, 0.0, side)
        dst[2 * ys : 2 * ys + run] = side
    prepare(0, 0, top.nb)
    begin(0, 0, top.nb, [R["r0"][c, 0 : top.nb] for c in range(3)])

    def coarse_setup():
        parts = thirds(s0[...])
        build(len(levels) - 1)
        for l in range(1, len(levels) - 1):
            sel_x, sel_z = R[f"sx{l}"][...], R[f"sz{l}"][...]
            picked = [mm(sel_x, part).astype(BF16) for part in parts]
            R[f"s{l}"][...] = sum(mm(part, sel_z) for part in picked)
            prepare(l, 0, levels[l].rows)
            build(l)

    def pre(k, _):
        def beside():
            pl.when(k == 0)(coarse_setup)
            pl.when(k == DEG - 2)(ahead_inner)

        smooth(0, k, k % 2, beside)
        return 0

    def cycle(l):
        skip = 0 if l == 0 else 1

        def body(k, _):
            smooth(l, k, (k + skip) % 2)
            return 0

        def tail(k, _):
            smooth(l, k, (k + skip + 1) % 2)
            return 0

        lax.fori_loop(0, DEG - 1, pre if l == 0 else body, 0)
        if l == 0:
            wide_scale_send()
        if l + 1 == len(levels) - 1:
            solve_wide(restrict(l))
        else:
            descend(l + 1, 0, restrict(l))
            cycle(l + 1)
        ascend(l)
        if l:
            lax.fori_loop(DEG, 2 * DEG, tail, 0)
        else:
            lax.fori_loop(DEG, 2 * DEG - 1, tail, 0)
            finish(2 * DEG - 1, (2 * DEG + skip) % 2)

    cycle(0)


def chebyshev_table(spectrum, coef):
    for l in range(3):
        low, top = spectrum[0, l], spectrum[1, l]
        center = 0.5 * (top + low)
        radius = 0.5 * (top - low)
        ratio = center / radius
        rho = 1.0 / ratio
        steps = []
        for _ in range(COARSE_DEG - 1):
            rho_next = 1.0 / (2.0 * ratio - rho)
            steps.append((rho_next * rho, 2.0 * rho_next / radius))
            rho = rho_next
        smooth = steps[: DEG - 1]
        flat = [(0.0, 0.0), (0.0, 1.0 / center)]
        picked = steps if l == 2 else smooth + flat + smooth
        for k, two in enumerate(picked):
            coef[l, 2 * k] = jnp.asarray(two[0], F32)
            coef[l, 2 * k + 1] = jnp.asarray(two[1], F32)
        coef[l, 12] = 1.0 / center


def local(modes, moduli, pinned, spectrum):
    vecs, _, nx, ny, nz = modes.shape
    levels = []
    names, args = [], []

    def add(name, value):
        names.append(name)
        args.append(value)

    for degree in DEGREES:
        step = DEGREES[0] // degree
        size = (degree, nx // step, ny // step, nz // step, vecs)
        levels.append(Level(*size) if step < DEGREES[0] else Wide(*size, COARSE_DEG - 1))
    top = levels[0]
    assert ny == top.run and nz % 128 == 0 and top.rows == top.base + nx * ny
    add("spectrum_in", spectrum.T)
    add("modes", modes.reshape(vecs, 3, nx * ny, nz))
    add("moduli_in", moduli.reshape(nx * ny, nz))
    add("pinned_in", pinned.reshape(nx * ny, nz))
    for l, lev in enumerate(levels):
        for axis, mats in zip("xy", lev.factors()):
            for key, mat in zip("etc", mats):
                add(f"{key}{axis}{l}_in", jnp.asarray(mat))
        add(f"z{l}_in", jnp.asarray(lev.lines()))
        for key, mat in zip(("kr", "kl"), lev.diagonal()):
            add(f"{key}{l}_in", jnp.asarray(mat))
        if l + 1 < len(levels):
            coarsest = l + 2 == len(levels)
            for key, mat in zip(("dp", "dz", "up", "uz"), transfer(lev, levels[l + 1])):
                if key[0] == "u" or not coarsest:
                    add(f"{key}{l}_in", jnp.asarray(mat))
        if 0 < l < len(levels) - 1:
            for key, mat in zip(("sx", "sz"), lev.sample(top)):
                add(f"{key}{l}_in", jnp.asarray(mat))
    wide = levels[-1]
    for key, mat in zip(("gp", "gs", "place", "gz"), wide.gather(levels[-2], top)):
        add(f"{key}_in", jnp.asarray(mat))
    add("sz_in", jnp.asarray(wide.sample(top)[1]))

    specs = [pl.BlockSpec(memory_space=pl.ANY) for n in names]
    scratch = []
    all_names = names + ["out"]

    def temp(name, what):
        all_names.append(name)
        scratch.append(what)

    temp("coef", pltpu.SMEM((3, 13), F32))
    temp("lsem", pltpu.SemaphoreType.DMA((len(names) + 24,)))
    for name, value in zip(names, args):
        if name == "spectrum_in":
            temp("spectrum", pltpu.SMEM(value.shape, F32))
        elif name.endswith("_in"):
            shape = value.shape
            if name[0] == "z":
                lanes = levels[int(name[1])].lanes
                shape = (4, 3 * lanes, lanes)
            elif name[0] == "t":
                shape = shape[1:]
            temp(name[:-3], pltpu.VMEM(shape, value.dtype))
    for l, lev in enumerate(levels):
        field = (3, lev.rows, lev.lanes)
        for n in ("s", "f"):
            temp(f"{n}{l}", pltpu.VMEM(field[1:], F32))
        for n in ("r", "d", "x", "dinv"):
            temp(f"{n}{l}", pltpu.VMEM(field, F32))
        temp(f"u{l}", pltpu.VMEM((3 * lev.kb, lev.lanes), BF16))
        for blk, n in (("b", lev.nb), ("i", lev.rows - lev.nb)):
            if n and not (blk == "b" and lev.split):
                temp(f"w1{blk}{l}", pltpu.VMEM((3 * n, 2 * lev.kb), BF16))
                temp(f"w2{blk}{l}", pltpu.VMEM((4 * n, lev.kb), BF16))
        if lev.split:
            temp(f"ub{l}", pltpu.VMEM((3 * 256, lev.lanes), BF16))
            temp(f"pre{l}", pltpu.VMEM((3, 4 * lev.nb, lev.lanes), F32))
            temp(f"wi{l}", pltpu.VMEM((3, 4 * lev.nb, lev.kb), BF16))
            temp(f"wb{l}", pltpu.VMEM((3, 4 * lev.nb, 256), BF16))
            rest = lev.rows - lev.nb
            temp(f"wj{l}", pltpu.VMEM((3, 4 * rest, 256), BF16))
            temp("inner", pltpu.VMEM((9 * rest, lev.lanes), F32))
        if lev is wide:
            continue
        for n in ("own", "pend"):
            temp(f"{n}{l}", pltpu.VMEM((3, lev.nb, lev.lanes), F32))
        for n, shape in (
            ("x", (2, 3 * lev.run + 8, lev.lanes)),
            ("y", (2, 3 * lev.ys, lev.lanes)),
            ("d", (4, 8, lev.lanes)),
        ):
            temp(f"send{n}{l}", pltpu.VMEM(shape, F32))
            temp(f"recv{n}{l}", pltpu.VMEM((2,) + shape, F32))
        temp(f"ssem{l}", pltpu.SemaphoreType.DMA((len(DIRS),)))
        temp(f"rsem{l}", pltpu.SemaphoreType.DMA((2, len(DIRS))))
    for kind in "sb":
        temp(f"pack{kind}", pltpu.VMEM((wide.pack_rows, wide.lanes), F32))
        temp(f"get{kind}", pltpu.VMEM((wide.got_rows, wide.lanes), F32))
        temp(f"wsend{kind}", pltpu.SemaphoreType.DMA((len(wide.sends) - 1,)))
        temp(f"wrecv{kind}", pltpu.SemaphoreType.DMA((len(wide.sends) - 1,)))
    temp("put", pltpu.VMEM((4, top.ys, top.lanes), F32))
    temp("putd", pltpu.VMEM((8, top.lanes), F32))
    temp("gotx", pltpu.VMEM((4, top.run, top.lanes), F32))
    temp("goty", pltpu.VMEM((4, top.ys, top.lanes), F32))
    temp("gotd", pltpu.VMEM((8, top.lanes), F32))
    temp("fsend", pltpu.SemaphoreType.DMA((4,)))
    temp("frecv", pltpu.SemaphoreType.DMA((4,)))
    out = pl.pallas_call(
        functools.partial(kernel, levels, all_names),
        out_shape=pltpu.VMEM((vecs, 3, nx * ny, nz), F32),
        in_specs=specs,
        out_specs=pl.BlockSpec(memory_space=pltpu.VMEM),
        scratch_shapes=scratch,
        compiler_params=pltpu.CompilerParams(
            collective_id=0, has_side_effects=True, vmem_limit_bytes=62 * 1024 * 1024
        ),
    )(*args)
    return out.reshape(modes.shape)


def solution(mesh):
    placed = (P(None, None, "gx", "gy", None), P("gx", "gy", None), P("gx", "gy", None), P())
    return jax.shard_map(
        local,
        mesh=mesh,
        in_specs=placed,
        out_specs=P(None, None, "gx", "gy", None),
        check_vma=False,
    )
```

```python
import functools

import jax
import jax.numpy as jnp
import numpy as np
from jax import lax
from jax.experimental import pallas as pl
from jax.experimental.pallas import tpu as pltpu
from jax.sharding import PartitionSpec as P

DEG = 3
COARSE_DEG = 4
DEGREES = (4, 2, 1)
MU_SHEAR = 1.0
LAMBDA_BULK = 1.5
PROLONG_TABLES = {
    4: np.array(
        [[1.0, 0.0, 0.0], [0.375, 0.75, -0.125], [0.0, 1.0, 0.0], [-0.125, 0.75, 0.375]]
    ),
    2: np.array([[1.0, 0.0], [0.5, 0.5]]),
}
DIRS = ((-1, 0), (1, 0), (0, -1), (0, 1), (-1, -1), (-1, 1), (1, -1), (1, 1))
F32 = jnp.float32
BF16 = jnp.bfloat16
M_, K_, G_, T_ = range(4)


def element_matrices(degree):
    nodes = [float(place) / degree for place in range(degree + 1)]
    gauss_x, gauss_w = np.polynomial.legendre.leggauss(8)
    points = 0.5 * (gauss_x + 1.0)
    weights = 0.5 * gauss_w
    values = np.zeros((degree + 1, points.size))
    slopes = np.zeros((degree + 1, points.size))
    for column in range(degree + 1):
        product = np.ones(points.size)
        for other in range(degree + 1):
            if other != column:
                product = product * (points - nodes[other]) / (nodes[column] - nodes[other])
        values[column] = product
        for skipped in range(degree + 1):
            if skipped != column:
                part = np.ones(points.size) / (nodes[column] - nodes[skipped])
                for other in range(degree + 1):
                    if other != column and other != skipped:
                        part = part * (points - nodes[other]) / (nodes[column] - nodes[other])
                slopes[column] += part
    mass = (values * weights) @ values.T
    stiff = (slopes * weights) @ slopes.T
    mixed = (slopes * weights) @ values.T
    return [mass, stiff, mixed, mixed.T]


def assembled(element, count, ghost):
    p = element.shape[0] - 1
    out = np.zeros((count + 1, count + 1))
    for e in range(count // p):
        out[e * p : e * p + p + 1, e * p : e * p + p + 1] += element
    if ghost:
        out[0, 0] += element[p, p]
    return out


def up(n, m):
    return -(-n // m) * m


def bf16_parts(mat, count):
    rest = np.asarray(mat, np.float64)
    parts = []
    for _ in range(count):
        part = rest.astype(np.float32).astype(BF16)
        parts.append(part)
        rest = rest - part.astype(np.float64)
    return parts


def exact_bf16(mat):
    out = np.asarray(mat, np.float32).astype(BF16)
    assert np.array_equal(out.astype(np.float64), mat)
    return out


class Level:
    def __init__(self, degree, nx, ny, nz, vecs):
        self.p, self.nx, self.ny, self.nz, self.vecs = degree, nx, ny, nz, vecs
        self.ys = up(nx + 1, 8)
        self.run = up(ny, 8)
        self.base = 2 * self.ys + self.run
        self.rows = up(self.base + nx * self.run, 16)
        self.nb = self.base + self.run
        assert self.nb % 16 == 0
        self.lanes = up(vecs * nz, 128)
        self.low = 0
        self.where = {(x, y): self.row(x, y) for x in range(nx + 1) for y in range(ny + 1)}
        self.spans = (nx, ny)
        self.columns()

    def columns(self):
        if 3 * self.rows <= 256:
            self.kp, self.kb = self.rows, 256
        else:
            self.kp = up(self.rows, 128)
            self.kb = 3 * self.kp
        self.packed = self.kb == 256
        self.split = not self.packed and 0 < 3 * self.nb <= 256 == self.kp
        self.seg = 256 if self.packed else self.kp

    def row(self, x, y):
        if y == 0:
            return x
        if y == self.ny:
            return self.ys + x
        if x == self.nx:
            return 2 * self.ys + y
        return self.base + self.run * x + y

    def factors(self):
        out = []
        for axis, n in enumerate(self.spans):
            expand = np.zeros((self.rows, 32))
            spread = np.zeros((128, self.seg))
            for at, row in self.where.items():
                expand[row, at[axis] + self.low] = 1
                for copy in range(3 if self.packed else 1):
                    for part in range(3):
                        spread[32 * part + at[axis] + self.low, copy * self.kp + row] = 1
            table = np.zeros((2, 32, 512), BF16)
            for ghost in range(2):
                for i, element in enumerate(element_matrices(self.p)):
                    parts = bf16_parts(assembled(element, n, ghost), 3)
                    for part, mat in enumerate(parts):
                        at = 128 * i + 32 * part
                        table[ghost, : n + 1, at : at + n + 1] = mat
            out.append((exact_bf16(expand), table, exact_bf16(spread)))
        return out

    def lines(self):
        p, n = self.p, self.nz
        mats = []
        for e in element_matrices(p):
            full = assembled(e, n, True)[:n, :n].T
            if n % 128:
                lifted = np.zeros((self.lanes, self.lanes))
                size = self.vecs * n
                lifted[:size, :size] = np.kron(np.eye(self.vecs), full)
                full = lifted
            mats.append(np.stack(bf16_parts(full, 2)))
        return np.stack(mats)

    def diagonal(self):
        def center(which, count):
            p = self.p
            e = element_matrices(p)[which]
            line = np.array([e[a, a] + (e[p, p] if a == 0 else 0.0) for a in range(p)])
            return line[np.arange(count) % p]

        rows = np.zeros((self.rows, 128), np.float32)
        m_x, m_y, m_z = [center(0, n) for n in (self.nx + self.p, self.ny + self.p, self.nz)]
        k_x, k_y, k_z = [center(1, n) for n in (self.nx + self.p, self.ny + self.p, self.nz)]
        for c in range(3):
            coef = [MU_SHEAR + (LAMBDA_BULK + MU_SHEAR) * (c == e) for e in range(3)]
            for (x, y), row in self.where.items():
                x, y = x % self.p, y % self.p
                rows[row, c] = coef[0] * k_x[x] * m_y[y] + coef[1] * m_x[x] * k_y[y]
                rows[row, 3 + c] = coef[2] * m_x[x] * m_y[y]
        lanes = np.zeros((8, self.lanes), np.float32)
        lanes[0, : self.vecs * self.nz] = np.tile(m_z, self.vecs)
        lanes[1, : self.vecs * self.nz] = np.tile(k_z, self.vecs)
        return rows, lanes

    def sample(self, top):
        step = top.p // self.p
        sel_x = np.zeros((self.rows, top.rows))
        for (x, y), row in self.where.items():
            if (x * step, y * step) in top.where:
                sel_x[row, top.where[x * step, y * step]] = 1
        sel_z = np.zeros((top.lanes, self.lanes))
        for v in range(self.vecs):
            for z in range(self.nz):
                sel_z[v * top.nz + z * step, v * self.nz + z] = 1
        return exact_bf16(sel_x), exact_bf16(sel_z)


class Wide(Level):
    def __init__(self, degree, nx, ny, nz, vecs, ring):
        self.p, self.nx, self.ny, self.nz, self.vecs = degree, nx, ny, nz, vecs
        self.low = ring * degree
        self.spans = (nx + 2 * self.low, ny + 2 * self.low)
        self.lanes = up(vecs * nz, 128)
        self.half = self.lanes // 2
        assert vecs * nz <= self.half
        spots = [
            (max(-x, x - nx, -y, y - ny, 0), x, y)
            for x in range(-self.low, nx + self.low + 1)
            for y in range(-self.low, ny + self.low + 1)
        ]
        self.where = {(x, y): row for row, (_, x, y) in enumerate(sorted(spots))}
        self.rows = up(len(self.where), 16)
        self.needed = [
            up(sum(away <= (ring - 1 - k) * degree for away, _, _ in spots), 16)
            for k in range(ring)
        ]
        self.nb = 0
        self.columns()
        self.plan()

    def plan(self):
        nx, ny, low = self.nx, self.ny, self.low
        closed = [(x, y) for x in range(nx + 1) for y in range(ny + 1)]
        far = [-(-(low + 1) // n) for n in (nx, ny)]
        self.far = far
        self.sections, self.sends = [], []
        self.pack_rows = 0
        at = 0
        kinds = {}
        offsets = [
            (dx, dy) for dx in range(-far[0], far[0] + 1) for dy in range(-far[1], far[1] + 1)
        ]
        for dx, dy in sorted(offsets, key=lambda o: (abs(o[0]) != 1, abs(o[1]), o)):
            nodes = tuple(
                (x, y) for x, y in closed if (x - dx * nx, y - dy * ny) in self.where
            )
            if not nodes:
                continue
            if nodes not in kinds:
                k = len(nodes)
                size = up(k + -(-k // 2), 8)
                kinds[nodes] = (self.pack_rows, size)
                self.sections.append((self.pack_rows, size, nodes))
                self.pack_rows += size
            start, size = kinds[nodes]
            self.sends.append((dx, dy, start, size, at, nodes))
            at += size
        self.pack_rows = up(self.pack_rows, 16)
        self.got_rows = up(at, 16)

    def gather(self, fine, top):
        table = PROLONG_TABLES[fine.p]
        px, py = interpolation(table, fine.nx), interpolation(table, fine.ny)
        plane = {
            (cx, cy): np.array(
                [
                    [px[x, cx] * py[y, cy], row]
                    for (x, y), row in fine.where.items()
                    if px[x, cx] * py[y, cy] != 0.0
                ]
            )
            for cx in range(self.nx + 1)
            for cy in range(self.ny + 1)
        }
        pack = np.zeros((2, self.pack_rows, 4 * fine.rows))
        scale = np.zeros((self.pack_rows, top.rows))
        step = top.p // self.p
        for start, size, nodes in self.sections:
            k = len(nodes)
            h = -(-k // 2)
            for i, node in enumerate(nodes):
                for weight, row in plane[node]:
                    row = int(row)
                    for side in range(2):
                        pack[side, start + i, row] = weight
                        pack[side, start + i, fine.rows + row] = weight
                    side = i // h
                    pack[side, start + k + i % h, 2 * fine.rows + row] = weight
                    pack[side, start + k + i % h, 3 * fine.rows + row] = weight
                if node[0] < self.nx and node[1] < self.ny:
                    scale[start + i, top.where[node[0] * step, node[1] * step]] = 1
        place = np.zeros((3, self.rows, self.got_rows))
        for dx, dy, start, size, at, nodes in self.sends:
            k = len(nodes)
            h = -(-k // 2)
            for i, (x, y) in enumerate(nodes):
                to = self.where.get((x - dx * self.nx, y - dy * self.ny))
                if to is not None:
                    place[0, to, at + i] = 1
                    place[1 + i // h, to, at + k + i % h] = 1
        down = interpolation(table, fine.nz)[: fine.nz, : self.nz]
        line = np.zeros((2, 2 * fine.lanes, self.lanes))
        size = (self.vecs * fine.nz, self.vecs * self.nz)
        for side in range(2):
            for copy in range(2):
                line[
                    side,
                    copy * fine.lanes : copy * fine.lanes + size[0],
                    side * self.half : side * self.half + size[1],
                ] = np.kron(np.eye(self.vecs), down)
        mats = (
            pack.reshape(2 * self.pack_rows, 4 * fine.rows),
            scale,
            place.reshape(3 * self.rows, self.got_rows),
            line.reshape(4 * fine.lanes, self.lanes),
        )
        return [exact_bf16(m) for m in mats]


def interpolation(table, count):
    q = table.shape[0]
    half = q // 2
    out = np.zeros((count + 1, count // 2 + 1))
    for i in range(count + 1):
        for t in range(half + 1):
            j = half * (i // q) + t
            if table[i % q, t] != 0.0:
                out[i, j] += table[i % q, t]
    return out


def transfer(fine, coarse):
    table = PROLONG_TABLES[fine.p]
    px, py = interpolation(table, fine.nx), interpolation(table, fine.ny)
    pz = interpolation(table, fine.nz)[: fine.nz, : coarse.nz]
    plane = np.zeros((fine.rows, coarse.rows))
    for (x, y), row in fine.where.items():
        for (cx, cy), col in coarse.where.items():
            if 0 <= cx <= coarse.nx and 0 <= cy <= coarse.ny:
                plane[row, col] = px[x, cx] * py[y, cy]
    line = np.zeros((coarse.lanes, fine.lanes))
    size = (fine.vecs * coarse.nz, fine.vecs * fine.nz)
    line[: size[0], : size[1]] = np.kron(np.eye(fine.vecs), pz.T)
    down = (np.tile(plane.T, (1, 2)), np.tile(line.T, (2, 1)))
    upward = (np.tile(plane, (1, 2)), np.tile(line, (2, 1)))
    return [exact_bf16(m) for m in down + upward]


def halves(value):
    hi = value.astype(BF16)
    return hi, (value - hi.astype(F32)).astype(BF16)


def mm(a, b):
    return lax.dot_general(a, b, (((1,), (0,)), ((), ())), preferred_element_type=F32)


def wide3(value):
    hi, lo = halves(value)
    return jnp.concatenate([hi, lo, hi], axis=1)


def wide2(value):
    hi, lo = halves(value)
    return jnp.concatenate([hi, lo], axis=1)


def tall2(value):
    hi, lo = halves(value)
    return jnp.concatenate([hi, lo], axis=0)


def kernel(levels, names, *refs):
    R = dict(zip(names, refs))
    gx_n, gy_n = lax.axis_size("gx"), lax.axis_size("gy")
    me_x, me_y = lax.axis_index("gx"), lax.axis_index("gy")

    def reach(dx, dy):
        ok = None
        for d, me, n in ((dx, me_x, gx_n), (dy, me_y, gy_n)):
            if d:
                here = me + d < n if d > 0 else me + d >= 0
                ok = here if ok is None else jnp.logical_and(ok, here)
        return ok

    def device(dx, dy):
        return (jnp.clip(me_x + dx, 0, gx_n - 1), jnp.clip(me_y + dy, 0, gy_n - 1))

    top = levels[0]
    vecs, nz = top.vecs, top.nz
    body_rows = pl.ds(top.base, top.nx * top.run)

    moves = []

    def load(src, dst):
        moves.append(pltpu.make_async_copy(src, dst, R["lsem"].at[len(moves)]))
        moves[-1].start()

    load(R["moduli_in"], R["moduli"])
    load(R["pinned_in"], R["pinned"])
    load(R["spectrum_in"], R["spectrum"])
    for v in range(vecs):
        load(R["modes"].at[v], R["r0"].at[:, body_rows, pl.ds(v * nz, nz)])
    first_moves = len(moves)
    wide = levels[-1]
    edged = range(len(levels) - 1)

    def clear(name):
        R[name][...] = jnp.zeros_like(R[name])

    for l in edged:
        for n in "xyd":
            clear(f"recv{n}{l}")
    for n in ("gotx", "goty", "gotd", "gets", "getb"):
        clear(n)

    barrier = pltpu.get_barrier_semaphore()
    peers = [(dx, dy) for dx, dy, *_ in wide.sends if dx or dy]
    assert set(DIRS) <= set(peers)
    for dx, dy in peers:

        @pl.when(reach(dx, dy))
        def _():
            pl.semaphore_signal(
                barrier, inc=1, device_id=device(dx, dy), device_id_type=pl.DeviceIdType.MESH
            )

    for l, lev in enumerate(levels):
        if lev.nz % 128 == 0:
            R[f"z{l}"][...] = jnp.zeros_like(R[f"z{l}"])
        load(R[f"tx{l}_in"].at[jnp.where(me_x == 0, 1, 0)], R[f"tx{l}"])
        load(R[f"ty{l}_in"].at[jnp.where(me_y == 0, 1, 0)], R[f"ty{l}"])
    for name in names:
        if name.endswith("_in") and name[:2] not in ("mo", "pi", "sp", "tx", "ty"):
            if name[0] == "z":
                lev = levels[int(name[1])]
                src, dst = R[name], R[name[:-3]]
                size = lev.nz if lev.nz % 128 == 0 else lev.lanes
                for s, half in enumerate((0, 0, 1)):
                    for at in range(0, lev.lanes, size):
                        load(
                            src.at[:, half],
                            dst.at[:, pl.ds(s * lev.lanes + at, size), pl.ds(at, size)],
                        )
            else:
                load(R[name], R[name[:-3]])

    for l in edged:
        for n in "xyd":
            clear(f"send{n}{l}")
        clear(f"pend{l}")
    for l in range(len(levels)):
        clear(f"u{l}")
        if levels[l].split:
            clear(f"ub{l}")

    for one in moves[:first_moves]:
        one.wait()
    chebyshev_table(R["spectrum"], R["coef"])
    scale = R["moduli"][...] * (1.0 - R["pinned"][...].astype(F32))
    s0 = R["s0"]
    s0[0 : top.base] = jnp.zeros((top.base, top.lanes), F32)
    for v in range(vecs):
        s0[body_rows, v * nz : (v + 1) * nz] = scale
    put = R["put"]
    put[...] = jnp.zeros_like(put)
    for c in range(3):
        for x in range(top.nx):
            at = top.base + x * top.run
            put[c, x : x + 1, :] = R["r0"][c, at : at + 1, :]
    for x in range(top.nx):
        at = top.base + x * top.run
        put[3, x : x + 1, :] = s0[at : at + 1, :]
    for c in range(4):
        R["putd"][c : c + 1, :] = put[c, 0:1, :]
    R["putd"][4:8, :] = jnp.zeros((4, top.lanes), F32)
    edge = pl.ds(top.base, top.run)

    def first_copies():
        plan = (
            (-1, 0, R["r0"].at[:, edge, :], R["gotx"].at[pl.ds(0, 3)]),
            (-1, 0, s0.at[edge, pl.ds(0, nz)], R["gotx"].at[3, :, pl.ds(0, nz)]),
            (0, -1, put, R["goty"]),
            (-1, -1, R["putd"].at[pl.ds(0, 4)], R["gotd"].at[pl.ds(0, 4)]),
        )
        for i, (dx, dy, src, dst) in enumerate(plan):
            yield dx, dy, pltpu.make_async_remote_copy(
                src_ref=src,
                dst_ref=dst,
                send_sem=R["fsend"].at[i],
                recv_sem=R["frecv"].at[i],
                device_id=device(dx, dy),
                device_id_type=pl.DeviceIdType.MESH,
            )

    around = []
    for me, n, far in ((me_x, gx_n, wide.far[0]), (me_y, gy_n, wide.far[1])):
        around.append(1 + jnp.minimum(me, far) + jnp.minimum(n - 1 - me, far))
    pl.semaphore_wait(barrier, around[0] * around[1] - 1)
    for dx, dy, copy in first_copies():
        pl.when(reach(dx, dy))(copy.start)
    for one in moves[first_moves:]:
        one.wait()

    def copies(l, slot, only):
        for i in only:
            dx, dy = DIRS[i]
            kind, at = ("d", i - 4) if dx and dy else ("x", i) if dx else ("y", i - 2)
            src, dst = R[f"send{kind}{l}"].at[at], R[f"recv{kind}{l}"].at[slot, at]
            if kind == "d":
                src, dst = src.at[pl.ds(0, 3)], dst.at[pl.ds(0, 3)]
            yield i, dx, dy, pltpu.make_async_remote_copy(
                src_ref=src,
                dst_ref=dst,
                send_sem=R[f"ssem{l}"].at[i],
                recv_sem=R[f"rsem{l}"].at[slot, i],
                device_id=device(dx, dy),
                device_id_type=pl.DeviceIdType.MESH,
            )

    def send(l, slot, part, only=range(8)):
        lev = levels[l]
        ys, run, nx = lev.ys, lev.run, lev.nx
        sx, sy, sd = (R[f"send{n}{l}"] for n in "xyd")
        tile = 3 * run
        order = {i: rest for i, *rest in copies(l, slot, only)}
        lows, highs = [v[0:ys] for v in part], [v[ys : 2 * ys] for v in part]
        def launch(which):
            for i in which:
                if i in only:
                    dx, dy, copy = order[i]
                    pl.when(reach(dx, dy))(copy.start)

        for i, start, at in ((0, lev.base, 0), (1, 2 * ys, nx)):
            if i in only:
                for c in range(3):
                    sx[i, c * run : (c + 1) * run] = part[c][start : start + run]
                    sx[i, tile + c : tile + c + 1] = lows[c][at : at + 1]
                    sx[i, tile + 3 + c : tile + 4 + c] = highs[c][at : at + 1]
        launch((0, 1))
        for i, (src, at) in enumerate(((lows, 0), (highs, 0), (lows, nx), (highs, nx))):
            if 4 + i in only:
                for c in range(3):
                    sd[i, c : c + 1] = src[c][at : at + 1]
        launch((4, 5, 6, 7))
        for i, src in enumerate((lows, highs)):
            if 2 + i in only:
                for c in range(3):
                    sy[i, c * ys : (c + 1) * ys] = src[c]
        launch((2, 3))

    def arrive(l, slot, only=range(8)):
        lev = levels[l]
        ys, run, nx = lev.ys, lev.run, lev.nx
        for _, dx, dy, copy in copies(l, slot, only):
            pl.when(reach(-dx, -dy))(copy.wait_recv)
        rx, ry, rd = (R[f"recv{n}{l}"] for n in "xyd")
        tile = pl.ds(3 * run, 8)
        left, right = rx[slot, 1, tile, :], rx[slot, 0, tile, :]
        at = lax.broadcasted_iota(jnp.int32, (ys, lev.lanes), 0)
        out = []
        for c in range(3):
            pieces = []
            for k, src in ((0, 1), (1, 0)):
                val = ry[slot, src, c * ys : (c + 1) * ys, :]
                row = slice(3 * k + c, 3 * k + c + 1)
                low = left[row] + rd[slot, 3 - k, c : c + 1, :]
                high = right[row] + rd[slot, 1 - k, c : c + 1, :]
                val = val + jnp.where(at == 0, low, 0.0) + jnp.where(at == nx, high, 0.0)
                pieces.append(val)
            pieces.append(rx[slot, 0, c * run : (c + 1) * run, :])
            pieces.append(rx[slot, 1, c * run : (c + 1) * run, :])
            out.append(jnp.concatenate(pieces, axis=0))
        return out

    def settle(l, slot, only=range(8)):
        for _, dx, dy, copy in copies(l, slot, only):
            pl.when(reach(dx, dy))(copy.wait_send)

    def wide_copies(kind):
        index = 0
        for dx, dy, start, size, at, nodes in wide.sends:
            if dx == 0 and dy == 0:
                continue
            count = up(len(nodes), 8) if kind == "s" else size
            yield dx, dy, pltpu.make_async_remote_copy(
                src_ref=R[f"pack{kind}"].at[pl.ds(start, count)],
                dst_ref=R[f"get{kind}"].at[pl.ds(at, count)],
                send_sem=R[f"wsend{kind}"].at[index],
                recv_sem=R[f"wrecv{kind}"].at[index],
                device_id=device(dx, dy),
                device_id_type=pl.DeviceIdType.MESH,
            )
            index += 1

    def wide_send(kind, value):
        R[f"pack{kind}"][...] = value
        for dx, dy, copy in wide_copies(kind):
            pl.when(reach(dx, dy))(copy.start)
        for dx, dy, start, size, at, nodes in wide.sends:
            if dx == 0 and dy == 0:
                R[f"get{kind}"][at : at + size] = value[start : start + size]

    def wide_wait(kind):
        for dx, dy, copy in wide_copies(kind):
            pl.when(reach(-dx, -dy))(copy.wait_recv)

    def wide_settle(kind):
        for dx, dy, copy in wide_copies(kind):
            pl.when(reach(dx, dy))(copy.wait_send)

    def thirds(value):
        parts = []
        for _ in range(3):
            parts.append(value.astype(BF16))
            value = value - parts[-1].astype(F32)
        return parts

    def wide_scale_send():
        sel = R["gs"][...]
        picked = [mm(sel, part).astype(BF16) for part in thirds(s0[...])]
        wide_send("s", sum(mm(part, R["sz"][...]) for part in picked))

    def wide_scale_take():
        wide_wait("s")
        wide_settle("s")
        place = R["place"][0 : wide.rows]
        R[f"s{len(levels) - 1}"][...] = sum(mm(place, part) for part in thirds(R["gets"][...]))
        prepare(len(levels) - 1, 0, wide.rows)

    def set_u(l, c, a, b, value):
        lev = levels[l]
        hi, lo = halves(value)
        at = c * lev.kb + a
        R[f"u{l}"][at : at + b - a] = hi
        R[f"u{l}"][at + lev.kp : at + lev.kp + b - a] = hi
        R[f"u{l}"][at + 2 * lev.kp : at + 2 * lev.kp + b - a] = lo
        if lev.split and a < lev.nb:
            n = min(b, lev.nb) - a
            for i, half in enumerate((hi, hi, lo)):
                at = 256 * c + i * lev.nb + a
                R[f"ub{l}"][at : at + n] = half[0:n]

    def span(l, blk):
        lev = levels[l]
        return (0, lev.nb) if blk == "b" else (lev.nb, lev.rows)

    def prepare(l, a, b):
        s = R[f"s{l}"][a:b]
        f = jnp.where(s == 0.0, 1.0, 0.0)
        R[f"f{l}"][a:b] = f
        square = s * s
        m_z, k_z = R[f"kl{l}"][0:1, :], R[f"kl{l}"][1:2, :]
        for c in range(3):
            kd = R[f"kr{l}"][a:b, c : c + 1] * m_z + R[f"kr{l}"][a:b, 3 + c : 4 + c] * k_z
            R[f"dinv{l}"][c, a:b] = 1.0 / (square * kd + f)

    def begin(l, a, b, source):
        scale = R["coef"][l, 12]
        s = R[f"s{l}"][a:b]
        for c in range(3):
            first = scale * (R[f"dinv{l}"][c, a:b] * source[c])
            R[f"r{l}"][c, a:b] = source[c]
            R[f"d{l}"][c, a:b] = first
            R[f"x{l}"][c, a:b] = first
            set_u(l, c, a, b, s * first)

    def ahead(l):
        lev = levels[l]
        if lev.split:
            for c in range(3):
                u = R[f"u{l}"][c * lev.kb : (c + 1) * lev.kb]
                R[f"pre{l}"][c] = mm(R[f"wi{l}"][c], u)

    def ahead_inner():
        n = top.rows - top.nb
        u = R["u0"]
        for at in range(0, 3 * top.kb, top.kp):
            u[at : at + top.nb] = jnp.zeros((top.nb, top.lanes), BF16)
        w1, w2, kb = R["w1i0"], R["w2i0"], top.kb
        R["inner"][0 : 3 * n] = mm(w1[...], u[0 : 2 * kb])
        R["inner"][3 * n : 7 * n] = mm(w2[...], u[2 * kb : 3 * kb])
        for c in range(2):
            at = (7 + c) * n
            R["inner"][at : at + n] = mm(w2[3 * n : 4 * n], u[c * kb : (c + 1) * kb])

    def plane_sums(l, blk, n, step, early):
        lev = levels[l]
        kb = lev.kb
        if blk == "b" and lev.split:
            q = [
                R[f"pre{l}"][c] + mm(R[f"wb{l}"][c], R[f"ub{l}"][256 * c : 256 * (c + 1)])
                for c in range(3)
            ]
            q = [[v[i * n : (i + 1) * n] for i in range(4)] for v in q]
            both = [q[0][i] + q[1][i] for i in range(3)]
            last, plain = q[2], [q[0][3], q[1][3], q[2][3]]
        elif early and lev.split:
            q = [mm(R[f"wj{l}"][c], R[f"ub{l}"][256 * c : 256 * (c + 1)]) for c in range(3)]
            q = [[v[i * n : (i + 1) * n] for i in range(4)] for v in q]
            done = [R["inner"][i * n : (i + 1) * n] for i in range(9)]
            both = [done[i] + q[0][i] + q[1][i] for i in range(3)]
            last = [done[3 + i] + q[2][i] for i in range(4)]
            plain = [done[7] + q[0][3], done[8] + q[1][3], last[3]]
        else:
            u, w1, w2 = R[f"u{l}"], R[f"w1{blk}{l}"], R[f"w2{blk}{l}"]
            tall = [
                w[...] if n == step
                else jnp.concatenate([w[i * step : i * step + n] for i in range(g)], axis=0)
                for w, g in ((w1, 3), (w2, 4))
            ]
            both = mm(tall[0], u[0 : 2 * kb])
            last = mm(tall[1], u[2 * kb : 3 * kb])
            both = [both[i * n : (i + 1) * n] for i in range(3)]
            last = [last[i * n : (i + 1) * n] for i in range(4)]
            mass = w2[3 * step : 3 * step + n]
            plain = [mm(mass, u[0:kb]), mm(mass, u[kb : 2 * kb]), last[3]]
        stretch = (2.0 * MU_SHEAR + LAMBDA_BULK) / MU_SHEAR
        plain[2] = stretch * plain[2]
        return [both[0], both[1], last[2]], plain, [last[0], last[1]], [both[2]]

    def local_sums(l, blk, rows=None, early=False):
        lev = levels[l]
        a, b = span(l, blk)
        n = rows or b - a

        def along(which, parts):
            z = R[f"z{l}"]
            if blk == "b" and lev.split:
                pairs = [halves(v) for v in parts]
                high = [v for v, _ in pairs]
                tall = jnp.concatenate(high + [v for _, v in pairs], axis=0)
                first = mm(tall, z[which, 0 : lev.lanes])
                m = len(parts) * n
                low = mm(jnp.concatenate(high, axis=0), z[which, 2 * lev.lanes : 3 * lev.lanes])
                return first[0:m] + first[m : 2 * m] + low
            return mm(jnp.concatenate([wide3(v) for v in parts], axis=0), z[which])

        mass, stiff, trans, mixed = plane_sums(l, blk, n, b - a, early)
        zm = along(M_, mass)
        zk = along(K_, stiff)
        zt = along(T_, trans)
        zg = along(G_, mixed)
        return [
            zm[0:n] + zk[0:n] + zt[0:n],
            zm[n : 2 * n] + zk[n : 2 * n] + zt[n : 2 * n],
            zm[2 * n : 3 * n] + zk[2 * n : 3 * n] + zg,
        ]

    def advance(l, k, a, b, sums):
        c1, c2 = R["coef"][l, 2 * k], R["coef"][l, 2 * k + 1]
        s, f = R[f"s{l}"][a:b], R[f"f{l}"][a:b]
        for c in range(3):
            d = R[f"d{l}"][c, a:b]
            res = R[f"r{l}"][c, a:b] - (s * sums[c] + f * d)
            new = c1 * d + c2 * (R[f"dinv{l}"][c, a:b] * res)
            R[f"r{l}"][c, a:b] = res
            R[f"d{l}"][c, a:b] = new
            R[f"x{l}"][c, a:b] += new
            set_u(l, c, a, b, s * new)

    def smooth(l, k, slot, beside=None):
        lev = levels[l]
        own, pend = R[f"own{l}"], R[f"pend{l}"]
        part = local_sums(l, "b")
        for c in range(3):
            part[c] = part[c] + pend[c]
            own[c] = part[c]
            pend[c] = jnp.zeros_like(pend[c])
        send(l, slot, part)
        inner = local_sums(l, "i")
        advance(l, k, lev.nb, lev.rows, inner)
        ahead(l)
        if beside is not None:
            beside()
        got = arrive(l, slot)
        advance(l, k, 0, lev.nb, [own[c] + got[c] for c in range(3)])
        settle(l, slot)

    def finish(k, slot):
        only = [i for i, (dx, dy) in enumerate(DIRS) if dx >= 0 and dy >= 0]
        c1, c2 = R["coef"][0, 2 * k], R["coef"][0, 2 * k + 1]

        def result(c, a, b, sums):
            s, f, d = R["s0"][a:b], R["f0"][a:b], R["d0"][c, a:b]
            res = R["r0"][c, a:b] - (s * sums + f * d)
            return R["x0"][c, a:b] + (c1 * d + c2 * (R["dinv0"][c, a:b] * res))

        def put_out(c, start, value):
            for v in range(vecs):
                size = value.shape[0]
                R["out"][v, c, start : start + size] = value[:, v * nz : (v + 1) * nz]

        own = R["own0"]
        part = local_sums(0, "b")
        for c in range(3):
            part[c] = part[c] + R["pend0"][c]
            own[c] = part[c]
        send(0, slot, part, only)
        inner = local_sums(0, "i")
        for c in range(3):
            put_out(c, top.run, result(c, top.nb, top.rows, inner[c]))
        got = arrive(0, slot, only)
        for c in range(3):
            value = result(c, 0, top.nb, own[c] + got[c])
            put_out(c, 0, value[top.base : top.nb])
            for x in range(top.nx):
                put_out(c, x * top.run, value[x : x + 1])
        settle(0, slot, only)

    def restrict(l):
        lev = levels[l]
        masked = []
        for blk in "bi":
            a, b = span(l, blk)
            sums = local_sums(l, blk, early=True)
            s, f = R[f"s{l}"][a:b], R[f"f{l}"][a:b]
            free = 1.0 - f
            if blk == "b":
                row = lax.broadcasted_iota(jnp.int32, (b - a, lev.lanes), 0)
                mine = jnp.logical_or(row < lev.nx, row >= lev.base)
                free = jnp.where(mine, free, 0.0)
            piece = []
            for c in range(3):
                r, d = R[f"r{l}"][c, a:b], R[f"d{l}"][c, a:b]
                piece.append(free * r - s * sums[c])
                if blk == "b":
                    R[f"pend{l}"][c] = sums[c]
                    R[f"r{l}"][c, a:b] = r - f * d
                else:
                    R[f"r{l}"][c, a:b] = r - (s * sums[c] + f * d)
            masked.append(piece)
        fields = [
            tall2(jnp.concatenate([masked[0][c], masked[1][c]], axis=0)) for c in range(3)
        ]
        if l + 1 == len(levels) - 1:
            n = wide.pack_rows
            flat = []
            for side in range(2):
                mat = R["gp"][side * n : (side + 1) * n]
                field = jnp.concatenate([fields[side], fields[2]], axis=0)
                flat.append(wide2(mm(mat, field)))
            return mm(jnp.concatenate(flat, axis=1), R["gz"][...])
        flat = [wide2(mm(R[f"dp{l}"][...], field)) for field in fields]
        down = mm(jnp.concatenate(flat, axis=0), R[f"dz{l}"][...])
        n = levels[l + 1].rows
        return [down[c * n : (c + 1) * n] for c in range(3)]

    def descend(l, slot, sums):
        lev = levels[l]
        own = R[f"own{l}"]
        for c in range(3):
            own[c] = sums[c][0 : lev.nb]
        send(l, slot, [sums[c][0 : lev.nb] for c in range(3)])
        free = 1.0 - R[f"f{l}"][lev.nb : lev.rows]
        begin(l, lev.nb, lev.rows, [free * sums[c][lev.nb : lev.rows] for c in range(3)])
        if l + 1 == len(levels) - 1:
            wide_scale_take()
        got = arrive(l, slot)
        free = 1.0 - R[f"f{l}"][0 : lev.nb]
        begin(l, 0, lev.nb, [free * (own[c] + got[c]) for c in range(3)])
        settle(l, slot)

    def solve_wide(packed):
        l, n, half = len(levels) - 1, wide.rows, wide.half
        wide_send("b", packed)
        wide_wait("b")
        hi, lo = halves(R["getb"][...])
        spread = mm(R["place"][...], hi) + mm(R["place"][...], lo)
        lane = lax.broadcasted_iota(jnp.int32, (n, wide.lanes), 1)
        keep = jnp.where(lane < half, 1.0 - R[f"f{l}"][...], 0.0)
        both, one, two = (spread[i * n : (i + 1) * n] for i in range(3))
        right = [both, pltpu.roll(both, half, 1), one + pltpu.roll(two, half, 1)]
        begin(l, 0, n, [keep * v for v in right])
        wide_settle("b")

        for k, rows in enumerate(wide.needed):
            advance(l, k, 0, rows, local_sums(l, "i", rows))

    def ascend(l):
        lev, n = levels[l], levels[l + 1].rows
        field = jnp.concatenate([wide2(R[f"x{l + 1}"][c]) for c in range(3)], axis=0)
        fine = mm(field, R[f"uz{l}"][...])
        free, s = 1.0 - R[f"f{l}"][...], R[f"s{l}"][...]
        for c in range(3):
            step = free * mm(R[f"up{l}"][...], tall2(fine[c * n : (c + 1) * n]))
            R[f"d{l}"][c] = step
            R[f"x{l}"][c] += step
            set_u(l, c, 0, lev.rows, s * step)
        ahead(l)

    def build(l):
        lev = levels[l]
        lines = []
        for axis in "xy":
            tall = mm(R[f"e{axis}{l}"][...], R[f"t{axis}{l}"][...])
            lines.append(
                [
                    mm(tall[:, 128 * i : 128 * (i + 1)].astype(BF16), R[f"c{axis}{l}"][...])
                    for i in range(4)
                ]
            )
        X, Y = lines
        cc = LAMBDA_BULK + MU_SHEAR
        big = MU_SHEAR + cc
        kxmy, mxky = X[K_] * Y[M_], X[M_] * Y[K_]
        first = (
            (0, 0, big * kxmy + MU_SHEAR * mxky),
            (0, 1, cc * (X[G_] * Y[T_])),
            (1, 0, cc * (X[T_] * Y[G_])),
            (1, 1, MU_SHEAR * kxmy + big * mxky),
            (2, 0, cc * (X[T_] * Y[M_])),
            (2, 1, cc * (X[M_] * Y[T_])),
        )
        second = (
            cc * (X[G_] * Y[M_]),
            cc * (X[M_] * Y[G_]),
            MU_SHEAR * (kxmy + mxky),
            X[M_] * Y[M_],
        )
        lane = lax.broadcasted_iota(jnp.int32, (lev.rows, lev.seg), 1)
        middle = jnp.logical_and(lane >= lev.kp, lane < 2 * lev.kp)

        def store(kind, group, at, value):
            hi, lo = halves(value)
            for blk in "bi" if lev.nb and not lev.split else "i":
                a, b = span(l, blk)
                ref, row = R[f"{kind}{blk}{l}"], group * (b - a)
                row = slice(row, row + b - a)
                if lev.packed:
                    mixed = jnp.where(middle, lo.astype(F32), hi.astype(F32)).astype(BF16)
                    ref[row, at : at + 256] = mixed[a:b]
                else:
                    for s, half in enumerate((hi, lo, hi)):
                        start = at + s * lev.kp
                        ref[row, start : start + lev.kp] = half[a:b]

        for group, side, value in first:
            store("w1", group, side * lev.kb, value)
        for group, value in enumerate(second):
            store("w2", group, 0, value)
        if lev.split:
            n, kp = lev.nb, lev.kp
            lane = lax.broadcasted_iota(jnp.int32, (lev.rows, kp), 1)
            parts = [(side, group, value) for group, side, value in first]
            parts += [(2, group, value) for group, value in enumerate(second)]
            parts += [(0, 3, second[3]), (1, 3, second[3])]
            for side, group, value in parts:
                hi, lo = (v.astype(F32) for v in halves(value))
                rows = slice(group * n, (group + 1) * n)
                inner = [jnp.where(lane[0:n] >= n, v[0:n], 0.0).astype(BF16) for v in (hi, lo)]
                for i, half in enumerate((inner[0], inner[1], inner[0])):
                    R[f"wi{l}"][side, rows, i * kp : (i + 1) * kp] = half
                hi, lo = (jnp.where(lane < n, v, 0.0) for v in (hi, lo))
                mixed = hi + pltpu.roll(lo, n, 1) + pltpu.roll(hi, 2 * n, 1)
                mixed = mixed.astype(BF16)
                R[f"wb{l}"][side, rows] = mixed[0:n]
                rest = lev.rows - n
                R[f"wj{l}"][side, group * rest : (group + 1) * rest] = mixed[n : lev.rows]

    build(0)

    def clear_spare(a, b):
        lead = lax.broadcasted_iota(jnp.int32, (b - a, top.lanes), 0) % top.run == 0
        s0[a:b] = jnp.where(lead, 0.0, s0[a:b])

    clear_spare(top.nb, top.rows)
    prepare(0, top.nb, top.rows)
    begin(0, top.nb, top.rows, [R["r0"][c, top.nb : top.rows] for c in range(3)])
    ahead(0)
    for dx, dy, copy in first_copies():
        pl.when(reach(dx, dy))(copy.wait_send)
        pl.when(reach(-dx, -dy))(copy.wait_recv)
    clear_spare(top.base, top.nb)
    for v in range(1, vecs):
        R["gotx"][3, :, v * nz : (v + 1) * nz] = R["gotx"][3, :, 0:nz]
    ys, run, nx = top.ys, top.run, top.nx
    at = lax.broadcasted_iota(jnp.int32, (ys, top.lanes), 0)
    for c in range(4):
        dst = s0 if c == 3 else R["r0"].at[c]
        low = jnp.where(at == nx, R["gotx"][c, 0:1, :], put[c])
        high = jnp.where(at == nx, R["gotd"][c : c + 1, :], R["goty"][c])
        dst[0:ys] = low
        dst[ys : 2 * ys] = high
        side = R["gotx"][c]
        if c == 3:
            row = lax.broadcasted_iota(jnp.int32, (run, top.lanes), 0)
            side = jnp.where(row == 0, 0.0, side)
        dst[2 * ys : 2 * ys + run] = side
    prepare(0, 0, top.nb)
    begin(0, 0, top.nb, [R["r0"][c, 0 : top.nb] for c in range(3)])

    def coarse_setup():
        parts = thirds(s0[...])
        build(len(levels) - 1)
        for l in range(1, len(levels) - 1):
            sel_x, sel_z = R[f"sx{l}"][...], R[f"sz{l}"][...]
            picked = [mm(sel_x, part).astype(BF16) for part in parts]
            R[f"s{l}"][...] = sum(mm(part, sel_z) for part in picked)
            prepare(l, 0, levels[l].rows)
            build(l)

    def pre(k, _):
        def beside():
            pl.when(k == 0)(coarse_setup)
            pl.when(k == DEG - 2)(ahead_inner)

        smooth(0, k, k % 2, beside)
        return 0

    def cycle(l):
        skip = 0 if l == 0 else 1

        def body(k, _):
            smooth(l, k, (k + skip) % 2)
            return 0

        def tail(k, _):
            smooth(l, k, (k + skip + 1) % 2)
            return 0

        lax.fori_loop(0, DEG - 1, pre if l == 0 else body, 0)
        if l == 0:
            wide_scale_send()
        if l + 1 == len(levels) - 1:
            solve_wide(restrict(l))
        else:
            descend(l + 1, 0, restrict(l))
            cycle(l + 1)
        ascend(l)
        if l:
            lax.fori_loop(DEG, 2 * DEG, tail, 0)
        else:
            lax.fori_loop(DEG, 2 * DEG - 1, tail, 0)
            finish(2 * DEG - 1, (2 * DEG + skip) % 2)

    cycle(0)


def chebyshev_table(spectrum, coef):
    for l in range(3):
        low, top = spectrum[0, l], spectrum[1, l]
        center = 0.5 * (top + low)
        radius = 0.5 * (top - low)
        ratio = center / radius
        rho = 1.0 / ratio
        steps = []
        for _ in range(COARSE_DEG - 1):
            rho_next = 1.0 / (2.0 * ratio - rho)
            steps.append((rho_next * rho, 2.0 * rho_next / radius))
            rho = rho_next
        smooth = steps[: DEG - 1]
        flat = [(0.0, 0.0), (0.0, 1.0 / center)]
        picked = steps if l == 2 else smooth + flat + smooth
        for k, two in enumerate(picked):
            coef[l, 2 * k] = jnp.asarray(two[0], F32)
            coef[l, 2 * k + 1] = jnp.asarray(two[1], F32)
        coef[l, 12] = 1.0 / center


def local(modes, moduli, pinned, spectrum):
    vecs, _, nx, ny, nz = modes.shape
    levels = []
    names, args = [], []

    def add(name, value):
        names.append(name)
        args.append(value)

    for degree in DEGREES:
        step = DEGREES[0] // degree
        size = (degree, nx // step, ny // step, nz // step, vecs)
        levels.append(Level(*size) if step < DEGREES[0] else Wide(*size, COARSE_DEG - 1))
    top = levels[0]
    assert ny == top.run and nz % 128 == 0 and top.rows == top.base + nx * ny
    add("spectrum_in", spectrum.T)
    add("modes", modes.reshape(vecs, 3, nx * ny, nz))
    add("moduli_in", moduli.reshape(nx * ny, nz))
    add("pinned_in", pinned.reshape(nx * ny, nz))
    for l, lev in enumerate(levels):
        for axis, mats in zip("xy", lev.factors()):
            for key, mat in zip("etc", mats):
                add(f"{key}{axis}{l}_in", jnp.asarray(mat))
        add(f"z{l}_in", jnp.asarray(lev.lines()))
        for key, mat in zip(("kr", "kl"), lev.diagonal()):
            add(f"{key}{l}_in", jnp.asarray(mat))
        if l + 1 < len(levels):
            coarsest = l + 2 == len(levels)
            for key, mat in zip(("dp", "dz", "up", "uz"), transfer(lev, levels[l + 1])):
                if key[0] == "u" or not coarsest:
                    add(f"{key}{l}_in", jnp.asarray(mat))
        if 0 < l < len(levels) - 1:
            for key, mat in zip(("sx", "sz"), lev.sample(top)):
                add(f"{key}{l}_in", jnp.asarray(mat))
    wide = levels[-1]
    for key, mat in zip(("gp", "gs", "place", "gz"), wide.gather(levels[-2], top)):
        add(f"{key}_in", jnp.asarray(mat))
    add("sz_in", jnp.asarray(wide.sample(top)[1]))

    specs = [pl.BlockSpec(memory_space=pl.ANY) for n in names]
    scratch = []
    all_names = names + ["out"]

    def temp(name, what):
        all_names.append(name)
        scratch.append(what)

    temp("coef", pltpu.SMEM((3, 13), F32))
    temp("lsem", pltpu.SemaphoreType.DMA((len(names) + 24,)))
    for name, value in zip(names, args):
        if name == "spectrum_in":
            temp("spectrum", pltpu.SMEM(value.shape, F32))
        elif name.endswith("_in"):
            shape = value.shape
            if name[0] == "z":
                lanes = levels[int(name[1])].lanes
                shape = (4, 3 * lanes, lanes)
            elif name[0] == "t":
                shape = shape[1:]
            temp(name[:-3], pltpu.VMEM(shape, value.dtype))
    for l, lev in enumerate(levels):
        field = (3, lev.rows, lev.lanes)
        for n in ("s", "f"):
            temp(f"{n}{l}", pltpu.VMEM(field[1:], F32))
        for n in ("r", "d", "x", "dinv"):
            temp(f"{n}{l}", pltpu.VMEM(field, F32))
        temp(f"u{l}", pltpu.VMEM((3 * lev.kb, lev.lanes), BF16))
        for blk, n in (("b", lev.nb), ("i", lev.rows - lev.nb)):
            if n and not (blk == "b" and lev.split):
                temp(f"w1{blk}{l}", pltpu.VMEM((3 * n, 2 * lev.kb), BF16))
                temp(f"w2{blk}{l}", pltpu.VMEM((4 * n, lev.kb), BF16))
        if lev.split:
            temp(f"ub{l}", pltpu.VMEM((3 * 256, lev.lanes), BF16))
            temp(f"pre{l}", pltpu.VMEM((3, 4 * lev.nb, lev.lanes), F32))
            temp(f"wi{l}", pltpu.VMEM((3, 4 * lev.nb, lev.kb), BF16))
            temp(f"wb{l}", pltpu.VMEM((3, 4 * lev.nb, 256), BF16))
            rest = lev.rows - lev.nb
            temp(f"wj{l}", pltpu.VMEM((3, 4 * rest, 256), BF16))
            temp("inner", pltpu.VMEM((9 * rest, lev.lanes), F32))
        if lev is wide:
            continue
        for n in ("own", "pend"):
            temp(f"{n}{l}", pltpu.VMEM((3, lev.nb, lev.lanes), F32))
        for n, shape in (
            ("x", (2, 3 * lev.run + 8, lev.lanes)),
            ("y", (2, 3 * lev.ys, lev.lanes)),
            ("d", (4, 8, lev.lanes)),
        ):
            temp(f"send{n}{l}", pltpu.VMEM(shape, F32))
            temp(f"recv{n}{l}", pltpu.VMEM((2,) + shape, F32))
        temp(f"ssem{l}", pltpu.SemaphoreType.DMA((len(DIRS),)))
        temp(f"rsem{l}", pltpu.SemaphoreType.DMA((2, len(DIRS))))
    for kind in "sb":
        temp(f"pack{kind}", pltpu.VMEM((wide.pack_rows, wide.lanes), F32))
        temp(f"get{kind}", pltpu.VMEM((wide.got_rows, wide.lanes), F32))
        temp(f"wsend{kind}", pltpu.SemaphoreType.DMA((len(wide.sends) - 1,)))
        temp(f"wrecv{kind}", pltpu.SemaphoreType.DMA((len(wide.sends) - 1,)))
    temp("put", pltpu.VMEM((4, top.ys, top.lanes), F32))
    temp("putd", pltpu.VMEM((8, top.lanes), F32))
    temp("gotx", pltpu.VMEM((4, top.run, top.lanes), F32))
    temp("goty", pltpu.VMEM((4, top.ys, top.lanes), F32))
    temp("gotd", pltpu.VMEM((8, top.lanes), F32))
    temp("fsend", pltpu.SemaphoreType.DMA((4,)))
    temp("frecv", pltpu.SemaphoreType.DMA((4,)))
    out = pl.pallas_call(
        functools.partial(kernel, levels, all_names),
        out_shape=pltpu.VMEM((vecs, 3, nx * ny, nz), F32),
        in_specs=specs,
        out_specs=pl.BlockSpec(memory_space=pltpu.VMEM),
        scratch_shapes=scratch,
        compiler_params=pltpu.CompilerParams(
            collective_id=0, has_side_effects=True, vmem_limit_bytes=62 * 1024 * 1024
        ),
    )(*args)
    return out.reshape(modes.shape)


def solution(mesh):
    placed = (P(None, None, "gx", "gy", None), P("gx", "gy", None), P("gx", "gy", None), P())
    return jax.shard_map(
        local,
        mesh=mesh,
        in_specs=placed,
        out_specs=P(None, None, "gx", "gy", None),
        check_vma=False,
    )
```
